1024 devices in a mesh: gx: 32 (over z, x_lo, core), gz: 32 (over x_hi, y).
Axes of the slice: x: 8 (x_hi: 4, x_lo: 2; x = x_hi * 2 + x_lo), y: 8, z: 8, core: 2. Of those that a mesh axis runs over, the one named last changes fastest.
Arguments:
- populations: float32 [19, 8, 256, 4096], P(None, None, 'gz', 'gx'), may hold values from 0.001 to 0.6, as said below
- solid: int32 [8, 256, 4096], P(None, 'gz', 'gx'), may hold values from 0 to 1, as said below
- top_inflow: float32 [5, 256, 4096], P(None, 'gz', 'gx'), may hold values from 0.005 to 0.1
Outputs:
- advanced: float32 [19, 8, 256, 4096], P(None, None, 'gz', 'gx')
The draws below stay inside these ranges and needn't reach their ends.
Inputs may be any that keep to these rules, and one draw needn't show every extreme that they name: Positive populations near equilibrium. Only the two planes nearest the wall hold solid nodes.
All inputs are finite; a program needn't handle non-finite values.
Results may differ from the reference program's by a relative error of at most 0.0003.
Values sent between devices are 32-bit elements; how exact they have to be, the bound alone decides.
No kernel may reach another device: no remote copies, remote signals or barrier semaphores. Data moves between devices by JAX's collectives and lax.ppermute only.
A program may use at most 32 MiB of HBM per device.

```python
from functools import reduce
import jax
import jax.numpy as jnp
import numpy as np
from jax import lax

NY = 8
STEPS = 2
NX = 4096
NZ = 256


draw_lattice = np.array([[0, 0, 0], [1, 0, 0], [-1, 0, 0], [0, 1, 0], [0, -1, 0], [0, 0, 1], [0, 0, -1], [1, 1, 0], [-1, -1, 0], [1, -1, 0], [-1, 1, 0], [1, 0, 1], [-1, 0, -1], [1, 0, -1], [-1, 0, 1], [0, 1, 1], [0, -1, -1], [0, 1, -1], [0, -1, 1]])


draw_weights = [1.0 / 3.0] + [1.0 / 18.0] * 6 + [1.0 / 36.0] * 12


draw_modes = [(1, 0), (2, 0), (3, 0), (0, 1), (1, 1), (2, 1), (1, 2)]


def draw_equilibrium(density, velocity):
    speed_square = velocity[0] * velocity[0] + velocity[1] * velocity[1] + velocity[2] * velocity[2]
    terms = []
    for index in range(19):
        along = float(draw_lattice[index, 0]) * velocity[0] + float(draw_lattice[index, 1]) * velocity[1] + float(draw_lattice[index, 2]) * velocity[2]
        terms.append(draw_weights[index] * density * (1.0 + 3.0 * along + 4.5 * along * along - 1.5 * speed_square))
    return jnp.stack(terms)


def draw_populations(key, part):
    subkeys = jax.random.split(jax.random.fold_in(key, 11), 8)
    grid_shape = (NY, NZ, NX)
    position = lax.broadcasted_iota(jnp.float32, grid_shape, 2) / float(NX)
    across = lax.broadcasted_iota(jnp.float32, grid_shape, 1) / float(NZ)
    phases = jax.random.uniform(subkeys[6], (len(draw_modes),), jnp.float32, 0.0, 2.0 * np.pi)
    offset = jax.random.uniform(subkeys[7], (), jnp.float32, 0.02, 0.05)
    amplitudes = 0.012 * jax.random.normal(subkeys[5], (len(draw_modes),), jnp.float32)
    regional = jnp.zeros(grid_shape, jnp.float32)
    for mode_index in range(len(draw_modes)):
        wave_x, wave_z = draw_modes[mode_index]
        angle_field = 2.0 * np.pi * (float(wave_x) * position + float(wave_z) * across) + phases[mode_index]
        regional = regional + amplitudes[mode_index] * jnp.cos(angle_field)
    density = 1.0 + 0.04 * jax.random.normal(subkeys[0], grid_shape, jnp.float32)
    speed_x = offset * (1.0 + 2.0 * position) + regional + 0.02 * jax.random.normal(subkeys[1], grid_shape, jnp.float32)
    speed_y = 0.01 * jax.random.normal(subkeys[2], grid_shape, jnp.float32)
    speed_z = 0.02 * jax.random.normal(subkeys[3], grid_shape, jnp.float32)
    fluctuation = 0.05 * jax.random.normal(subkeys[4], (19,) + grid_shape, jnp.float32)
    base_state = draw_equilibrium(density, (speed_x, speed_y, speed_z))
    scaled = jnp.asarray(np.array(draw_weights, dtype=np.float32))[:, None, None, None]
    return jnp.clip(base_state + scaled * fluctuation, 0.001, 0.6).astype(jnp.float32)


def draw_solid(key, part):
    grid_shape = (NY, NZ, NX)
    drawn = jax.random.randint(jax.random.fold_in(key, 23), grid_shape, 0, 100)
    plane = lax.broadcasted_iota(jnp.int32, grid_shape, 0)
    limit = jnp.where(plane == 0, 35, jnp.where(plane == 1, 12, 0))
    return (drawn < limit).astype(jnp.int32)


def draw_top_inflow(key, part):
    chosen = [4, 8, 9, 16, 18]
    grid_shape = (5, NZ, NX)
    inflow_speed = 0.1
    factor = 1.0 + 0.1 * jax.random.normal(jax.random.fold_in(key, 31), grid_shape, jnp.float32)
    levels = []
    for index in chosen:
        along = float(draw_lattice[index, 0]) * inflow_speed
        levels.append(draw_weights[index] * (1.0 + 3.0 * along + 4.5 * along * along - 1.5 * inflow_speed * inflow_speed))
    table = jnp.asarray(np.array(levels, dtype=np.float32))[:, None, None]
    return jnp.clip(table * factor, 0.005, 0.1).astype(jnp.float32)


def setup_inputs(seed: int = 0) -> dict:
    arg_keys = jax.random.split(jax.random.key(seed), 4)
    populations = draw_populations(jax.random.fold_in(arg_keys[3], 71), 0)
    solid = draw_solid(jax.random.fold_in(arg_keys[3], 71), 0)
    top_inflow = draw_top_inflow(jax.random.fold_in(arg_keys[3], 71), 0)
    return dict(populations=populations, solid=solid, top_inflow=top_inflow)


lattice = np.array([[0, 0, 0], [1, 0, 0], [-1, 0, 0], [0, 1, 0], [0, -1, 0], [0, 0, 1], [0, 0, -1],
                    [1, 1, 0], [-1, -1, 0], [1, -1, 0], [-1, 1, 0], [1, 0, 1], [-1, 0, -1],
                    [1, 0, -1], [-1, 0, 1], [0, 1, 1], [0, -1, -1], [0, 1, -1], [0, -1, 1]])
lattice_weights = [1.0 / 3.0] + [1.0 / 18.0] * 6 + [1.0 / 36.0] * 12
opposite = [0, 2, 1, 4, 3, 6, 5, 8, 7, 10, 9, 12, 11, 14, 13, 16, 15, 18, 17]
incoming = [4, 8, 9, 16, 18]
base_drive = 0.0001
drive_gain = 1.0
target_flow = 0.1


def invert_rows(matrix):
    order = len(matrix)
    work = [list(matrix[row]) + [1.0 if col == row else 0.0 for col in range(order)] for row in range(order)]
    for col in range(order):
        pivot = max(range(col, order), key=lambda row: abs(work[row][col]))
        work[col], work[pivot] = work[pivot], work[col]
        lead = work[col][col]
        work[col] = [value / lead for value in work[col]]
        for row in range(order):
            if row != col:
                factor = work[row][col]
                if factor != 0.0:
                    work[row] = [value - factor * other for value, other in zip(work[row], work[col])]
    return [line[order:] for line in work]


def collide_matrix():
    moment_rows = []
    for power in [(0, 0, 0), (1, 0, 0), (0, 1, 0), (0, 0, 1), (1, 1, 0), (1, 0, 1), (0, 1, 1),
                  (2, 0, 0), (0, 2, 0), (0, 0, 2), (1, 2, 0), (1, 0, 2), (2, 1, 0), (0, 1, 2),
                  (2, 0, 1), (0, 2, 1), (2, 2, 0), (2, 0, 2), (0, 2, 2)]:
        moment_rows.append([float(int(lattice[q, 0]) ** power[0] * int(lattice[q, 1]) ** power[1]
                                  * int(lattice[q, 2]) ** power[2]) for q in range(19)])
    rates = [0.0] * 4 + [1.8] * 6 + [1.2] * 6 + [1.1] * 3
    inverse = invert_rows(moment_rows)
    result = [[sum(inverse[row][mid] * rates[mid] * moment_rows[mid][col] for mid in range(19))
               for col in range(19)] for row in range(19)]
    return np.array(result, dtype=np.float32)


def signed_sum(populations, component):
    plus_terms = [populations[index] for index in range(19) if lattice[index, component] == 1]
    minus_terms = [populations[index] for index in range(19) if lattice[index, component] == -1]
    return reduce(lambda left, right: left + right, plus_terms) - reduce(lambda left, right: left + right, minus_terms)


def moments(populations):
    density = jnp.sum(populations, axis=0)
    momentum = (signed_sum(populations, 0), signed_sum(populations, 1), signed_sum(populations, 2))
    return density, momentum


def project(index, velocity):
    result = jnp.zeros_like(velocity[0])
    for component in range(3):
        factor = int(lattice[index, component])
        if factor == 1:
            result = result + velocity[component]
        elif factor == -1:
            result = result - velocity[component]
    return result


def equilibrium(density, velocity):
    speed_square = velocity[0] * velocity[0] + velocity[1] * velocity[1] + velocity[2] * velocity[2]
    terms = []
    for index in range(19):
        along = project(index, velocity)
        terms.append(lattice_weights[index] * density * (1.0 + 3.0 * along + 4.5 * along * along - 1.5 * speed_square))
    return jnp.stack(terms)


def collide(current, density, momentum, driving):
    velocity = tuple(part_value / density for part_value in momentum)
    base_state = equilibrium(density, velocity)
    pushed = equilibrium(density, (velocity[0] + driving / density, velocity[1], velocity[2]))
    relaxed = jnp.tensordot(jnp.asarray(collide_matrix()), current - base_state, axes=1,
                            precision=lax.Precision.HIGHEST)
    return current - relaxed + pushed - base_state


def shift_planes(carried, blocked, step_y):
    if step_y == 1:
        carried = jnp.concatenate([jnp.zeros_like(carried[:1]), carried[:-1]], axis=0)
        blocked = jnp.concatenate([jnp.ones_like(blocked[:1]), blocked[:-1]], axis=0)
    elif step_y == -1:
        carried = jnp.concatenate([carried[1:], jnp.zeros_like(carried[:1])], axis=0)
        blocked = jnp.concatenate([blocked[1:], jnp.zeros_like(blocked[:1])], axis=0)
    return carried, blocked


def stream_whole(collided, solid, top_inflow, before):
    planes = collided.shape[1]
    results = []
    for index in range(19):
        step_x = int(lattice[index, 0])
        step_y = int(lattice[index, 1])
        step_z = int(lattice[index, 2])
        carried = jnp.roll(collided[index], (step_z, step_x), axis=(1, 2))
        blocked = jnp.roll(solid, (step_z, step_x), axis=(1, 2))
        carried, blocked = shift_planes(carried, blocked, step_y)
        arrived = jnp.where(blocked == 1, collided[opposite[index]], carried)
        if step_y == -1:
            arrived = arrived.at[planes - 1].set(top_inflow[incoming.index(index)])
        results.append(arrived)
    return jnp.where(solid[None] == 1, before, jnp.stack(results))


def reference(populations, solid, top_inflow):
    fluid_nodes = (1 - solid).astype(jnp.float32)
    node_total = float(NX * NY * NZ)
    current = populations
    for step_index in range(STEPS):
        density, momentum = moments(current)
        bulk_flow = jnp.sum(momentum[0] * fluid_nodes) / node_total
        driving = base_drive + drive_gain * (target_flow - bulk_flow)
        collided = collide(current, density, momentum, driving)
        current = stream_whole(collided, solid, top_inflow, current)
    return current
```

```python
import jax
import jax.numpy as jnp
from jax import lax
from jax.experimental import pallas as pl
from jax.experimental.pallas import tpu as pltpu
from jax.sharding import PartitionSpec as P

Q = 19
PLANES = 8
LATTICE = (
    (0, 0, 0),
    (1, 0, 0),
    (-1, 0, 0),
    (0, 1, 0),
    (0, -1, 0),
    (0, 0, 1),
    (0, 0, -1),
    (1, 1, 0),
    (-1, -1, 0),
    (1, -1, 0),
    (-1, 1, 0),
    (1, 0, 1),
    (-1, 0, -1),
    (1, 0, -1),
    (-1, 0, 1),
    (0, 1, 1),
    (0, -1, -1),
    (0, 1, -1),
    (0, -1, 1),
)
OPPOSITE = (0, 2, 1, 4, 3, 6, 5, 8, 7, 10, 9, 12, 11, 14, 13, 16, 15, 18, 17)
INCOMING = (4, 8, 9, 16, 18)
SECOND, THIRD, FOURTH = 1.8, 1.2, 1.1
BASE_DRIVE = 0.0001
DRIVE_GAIN = 1.0
TARGET_FLOW = 0.1

FLAG_SLOT = Q * PLANES
INFLOW_SLOT = FLAG_SLOT + 2
SLOTS = INFLOW_SLOT + len(INCOMING)
TILES = 5
ZROWS = SLOTS + TILES


def relax(f):
    along = []
    for p in (1, 3, 5):
        along.append((f[p] + f[p + 1], f[p] - f[p + 1]))
    diagonal = []
    for p in (7, 11, 15):
        a, b = f[p] + f[p + 1], f[p + 2] + f[p + 3]
        c, d = f[p] - f[p + 1], f[p + 2] - f[p + 3]
        diagonal.append((a + b, a - b, c + d, c - d))
    (xxyy, xy, xyy, xxy), (xxzz, xz, xzz, xxz), (yyzz, yz, yzz, yyz) = diagonal
    density = f[0] + (along[0][0] + along[1][0] + along[2][0]) + (xxyy + xxzz + yyzz)
    jx = along[0][1] + xyy + xzz
    jy = along[1][1] + xxy + yzz
    jz = along[2][1] + xxz + yyz
    inv = 1.0 / density
    ux, uy, uz = jx * inv, jy * inv, jz * inv
    exx, eyy, ezz = jx * ux, jy * uy, jz * uz
    third = density * (1.0 / 3.0)
    ninth = density * (1.0 / 9.0)
    xx = along[0][0] + xxyy + xxzz
    yy = along[1][0] + xxyy + yyzz
    zz = along[2][0] + xxzz + yyzz
    dxx = SECOND * (xx - third - exx)
    dyy = SECOND * (yy - third - eyy)
    dzz = SECOND * (zz - third - ezz)
    dxy = SECOND * (xy - jx * uy)
    dxz = SECOND * (xz - jx * uz)
    dyz = SECOND * (yz - jy * uz)
    x3, y3, z3 = jx * (1.0 / 3.0), jy * (1.0 / 3.0), jz * (1.0 / 3.0)
    dxyy, dxzz = THIRD * (xyy - x3), THIRD * (xzz - x3)
    dxxy, dyzz = THIRD * (xxy - y3), THIRD * (yzz - y3)
    dxxz, dyyz = THIRD * (xxz - z3), THIRD * (yyz - z3)
    half = 0.5 * (exx + eyy + ezz)
    dxxyy = FOURTH * (xxyy - ninth - (half - 0.5 * ezz) * (2.0 / 3.0) + ezz * (1.0 / 6.0))
    dxxzz = FOURTH * (xxzz - ninth - (half - 0.5 * eyy) * (2.0 / 3.0) + eyy * (1.0 / 6.0))
    dyyzz = FOURTH * (yyzz - ninth - (half - 0.5 * exx) * (2.0 / 3.0) + exx * (1.0 / 6.0))
    out = [None] * Q
    out[0] = f[0] + (dxx + dyy + dzz) - (dxxyy + dxxzz + dyyzz)
    for p, even, odd in (
        (1, dxx - dxxyy - dxxzz, dxyy + dxzz),
        (3, dyy - dxxyy - dyyzz, dxxy + dyzz),
        (5, dzz - dxxzz - dyyzz, dxxz + dyyz),
    ):
        out[p] = f[p] - 0.5 * (even - odd)
        out[p + 1] = f[p + 1] - 0.5 * (even + odd)
    for p, four, cross, first, second in (
        (7, dxxyy, dxy, dxyy, dxxy),
        (11, dxxzz, dxz, dxzz, dxxz),
        (15, dyyzz, dyz, dyzz, dyyz),
    ):
        same, other = 0.25 * (four + cross), 0.25 * (four - cross)
        total, rest = 0.25 * (first + second), 0.25 * (first - second)
        out[p] = f[p] - (same + total)
        out[p + 1] = f[p + 1] - (same - total)
        out[p + 2] = f[p + 2] - (other + rest)
        out[p + 3] = f[p + 3] - (other - rest)
    return out, (ux, uy, uz), inv


def weight(index):
    return 1.0 / 3.0 if index == 0 else (1.0 / 18.0 if index < 7 else 1.0 / 36.0)


def push_parts(index, velocity, inv):
    cx, cy, cz = LATTICE[index]
    along = 9.0 * velocity[0] - 3.0 * velocity[0] + 3.0 * cx
    if cy:
        along = along + (9.0 * cx * cy) * velocity[1]
    if cz:
        along = along + (9.0 * cx * cz) * velocity[2]
    return weight(index) * along, (3.0 * weight(index)) * inv


def driven(relaxed, velocity, inv, drive):
    ux, uy, uz = velocity
    square = drive * drive * inv
    still = -3.0 * drive * ux - 1.5 * square
    moved = still + 9.0 * drive * ux + 4.5 * square
    three = 3.0 * drive
    up, down = moved + three, moved - three
    hy, hz = 9.0 * drive * uy, 9.0 * drive * uz
    calm = still * (1.0 / 36.0)
    out = list(relaxed)
    out[0] = out[0] + still * (1.0 / 3.0)
    out[1] = out[1] + up * (1.0 / 18.0)
    out[2] = out[2] + down * (1.0 / 18.0)
    for index in (3, 4, 5, 6):
        out[index] = out[index] + (calm + calm)
    for p, side in ((7, hy), (11, hz)):
        out[p] = out[p] + (up + side) * (1.0 / 36.0)
        out[p + 1] = out[p + 1] + (down + side) * (1.0 / 36.0)
        out[p + 2] = out[p + 2] + (up - side) * (1.0 / 36.0)
        out[p + 3] = out[p + 3] + (down - side) * (1.0 / 36.0)
    for index in (15, 16, 17, 18):
        out[index] = out[index] + calm
    return out


def rolled(value, step_z, step_x):
    if step_z:
        value = pltpu.roll(value, step_z % value.shape[0], 0)
    if step_x:
        value = pltpu.roll(value, step_x % value.shape[1], 1)
    return value


def slot_values(pops, solid, inflow):
    values = [lambda q=q, y=y: pops[q, y] for q in range(Q) for y in range(PLANES)]
    values += [lambda y=y: solid[y].astype(jnp.float32) for y in range(2)]
    values += [lambda i=i: inflow[i] for i in range(len(INCOMING))]
    return values


def pack_columns(pops, solid, inflow, edges):
    lane = lax.broadcasted_iota(jnp.int32, (8, 128), 1)
    values = slot_values(pops, solid, inflow)
    for tile in range(TILES):
        first = jnp.zeros((8, 128), jnp.float32)
        for slot in range(32):
            if tile * 32 + slot < SLOTS:
                offset = 4 * slot
                moved = rolled(values[tile * 32 + slot](), 0, offset)
                place = ((lane + (128 - offset + 2)) & 127) < 4
                first = jnp.where(place, moved, first)
        edges[tile] = first


def pack_rows(pops, solid, inflow, left, right, below, above, sides):
    lane = lax.broadcasted_iota(jnp.int32, (8, 128), 1)
    for index, value in enumerate(slot_values(pops, solid, inflow)):
        tile = value()
        below[index] = tile[0:2]
        above[index] = tile[6:8]
    for tile in range(TILES):
        both = jnp.where((lane & 3) < 2, right[tile], left[tile])
        sides[tile] = both
        below[SLOTS + tile] = both[0:2]
        above[SLOTS + tile] = both[6:8]


def lay_sides(sides, below, above, ring):
    for tile in range(TILES):
        ring[tile, 0:8] = sides[tile]
        ring[tile, 8:10] = above[SLOTS + tile]
        ring[tile, 14:16] = below[SLOTS + tile]


def lay_out(target, main, slot, ring, below, above):
    target[0:8, 0:128] = main
    target[8:10, 0:128] = above[slot]
    target[14:16, 0:128] = below[slot]
    target[:, 128:256] = rolled(ring[slot // 32], 0, -4 * (slot % 32))


def tally(pops, solid, inflow, sides, below, above, out, ring, flags):
    lay_sides(sides, below, above, ring)
    for y in range(2):
        lay_out(flags.at[y], solid[y].astype(jnp.float32), FLAG_SLOT + y, ring, below, above)
    flow = jnp.zeros((8, 128), jnp.float32)
    count = jnp.full((8, 128), float(PLANES - 2), jnp.float32)
    fluid = [1.0 - flags[y, 0:8, 0:128] for y in range(2)]
    for y in range(PLANES):
        f = pops
        jx = (
            (f[1, y] - f[2, y])
            + (f[7, y] - f[8, y])
            + (f[9, y] - f[10, y])
            + (f[11, y] - f[12, y])
            + (f[13, y] - f[14, y])
        )
        flow = flow + (jx * fluid[y] if y < 2 else jx)
    count = count + fluid[0] + fluid[1]
    one = flow
    two = jnp.zeros((8, 128), jnp.float32)
    for y in (0, 1, 2, PLANES - 1):
        relaxed, velocity, inv = relax([pops[q, y] for q in range(Q)])
        for index in range(Q):
            cx, cy, cz = LATTICE[index]
            target = y + cy
            if not cx or 1 < target < PLANES:
                continue
            linear, square = push_parts(index, velocity, inv)
            if target >= PLANES:
                factor = -float(cx)
            elif target < 0:
                factor = (-2.0 * cx) * fluid[y]
            else:
                hit = rolled(flags[target], -cz, -cx)[0:8, 0:128]
                factor = (-2.0 * cx) * hit
                if y < 2:
                    factor = factor * fluid[y]
            one = one + factor * relaxed[index]
            count = count + factor * linear
            two = two + factor * square
    one = one + (inflow[INCOMING.index(9)] - inflow[INCOMING.index(8)])
    lane = lax.broadcasted_iota(jnp.int32, (1, 128), 1)
    packed = jnp.zeros((1, 128), jnp.float32)
    for place, part in enumerate((flow, one, count, two)):
        total = jnp.sum(jnp.sum(part, axis=0, keepdims=True), axis=1, keepdims=True)
        packed = jnp.where(lane == place, total, packed)
    out[...] = jnp.broadcast_to(packed[None], out.shape)


def advance(node_total, pops, solid, inflow, sides, below, above, sums, out, ring, flags, entry, hits, now, moved):
    total = jnp.sum(sums[...], axis=0)
    flow, one, count, two = (total[:, i : i + 1] for i in range(4))
    first = BASE_DRIVE + DRIVE_GAIN * (TARGET_FLOW - flow / node_total)
    later = (one + count * first + two * (first * first)) / node_total
    second = BASE_DRIVE + DRIVE_GAIN * (TARGET_FLOW - later)

    lay_sides(sides, below, above, ring)
    for y in range(2):
        lay_out(flags.at[y], solid[y].astype(jnp.float32), FLAG_SLOT + y, ring, below, above)
        for step_z in (-1, 0, 1):
            for step_x in (-1, 0, 1):
                hits[y, 3 * step_z + step_x + 4] = rolled(flags[y], step_z, step_x)
    for i in range(len(INCOMING)):
        lay_out(entry.at[i], inflow[i], INFLOW_SLOT + i, ring, below, above)
    for y in range(PLANES):
        for q in range(Q):
            lay_out(now.at[y, q], pops[q, y], q * PLANES + y, ring, below, above)

    for step in range(2):
        drive = jnp.broadcast_to(first if step == 0 else second, (8, 128))

        def collide(y, carry):
            for rows in (slice(0, 8), slice(8, 16)):
                for cols in (slice(0, 128), slice(128, 256)):
                    result = relax([now[y, q, rows, cols] for q in range(Q)])
                    for q, value in enumerate(driven(*result, drive)):
                        moved[y, q, rows, cols] = value
            return carry

        lax.fori_loop(0, PLANES, collide, 0)
        whole = (slice(0, 16), slice(0, 256))
        part = whole if step == 0 else (slice(0, 8), slice(0, 128))
        for y in range(PLANES):
            for q in range(Q):
                cx, cy, cz = LATTICE[q]
                source = y - cy
                if source < 0:
                    arrived = moved[(y, OPPOSITE[q]) + part]
                elif source >= PLANES:
                    arrived = entry[(INCOMING.index(q),) + part]
                else:
                    arrived = rolled(moved[source, q], cz, cx)[part]
                    if source < 2:
                        hit = hits[(source, 3 * cz + cx + 4) + part]
                        arrived = jnp.where(hit > 0.5, moved[(y, OPPOSITE[q]) + part], arrived)
                if y < 2:
                    arrived = jnp.where(flags[(y,) + part] > 0.5, now[(y, q) + part], arrived)
                if step == 0:
                    now[y, q] = arrived
                else:
                    out[q, y] = arrived


def kernel_call(body, shapes, scratch, *operands):
    vmem = pl.BlockSpec(memory_space=pltpu.VMEM)
    return pl.pallas_call(
        body,
        in_specs=[vmem] * len(operands),
        out_specs=[vmem] * len(shapes),
        out_shape=[jax.ShapeDtypeStruct(shape, jnp.float32) for shape in shapes],
        scratch_shapes=[pltpu.VMEM(shape, jnp.float32) for shape in scratch],
        compiler_params=pltpu.CompilerParams(vmem_limit_bytes=48 * 1024 * 1024),
    )(*operands)


def neighbours(axis, low, high):
    count = lax.axis_size(axis)
    up = [(i, (i + 1) % count) for i in range(count)]
    down = [(target, source) for source, target in up]
    return lax.ppermute(high, axis, up), lax.ppermute(low, axis, down)


def local(populations, solid, top_inflow):
    along_x, along_z = lax.axis_size("gx"), lax.axis_size("gz")
    node_total = float(PLANES * 8 * 128 * along_x * along_z)
    fields = (populations, solid, top_inflow)
    (edges,) = kernel_call(pack_columns, [(TILES, 8, 128)], [], *fields)
    left, right = neighbours("gx", edges, edges)
    below, above, sides = kernel_call(
        pack_rows, [(ZROWS, 2, 128)] * 2 + [(TILES, 8, 128)], [], *fields, left, right
    )
    below, above = neighbours("gz", below, above)
    ring = [(TILES, 16, 128), (2, 16, 256)]
    halo = (sides, below, above)
    (sums,) = kernel_call(tally, [(along_x, 1, 128)], ring, *fields, *halo)
    sums = lax.all_to_all(sums, "gx", 0, 0, tiled=True)
    sums = jnp.broadcast_to(jnp.sum(sums, axis=0, keepdims=True), (along_z, 1, 128))
    sums = lax.all_to_all(sums, "gz", 0, 0, tiled=True)
    state = [(PLANES, Q, 16, 256)] * 2
    (advanced,) = kernel_call(
        lambda *refs: advance(node_total, *refs),
        [(Q, PLANES, 8, 128)],
        ring + [(len(INCOMING), 16, 256), (2, 9, 16, 256)] + state,
        *fields,
        *halo,
        sums,
    )
    return advanced


def solution(mesh):
    placed = (P(None, None, "gz", "gx"), P(None, "gz", "gx"), P(None, "gz", "gx"))
    return jax.shard_map(
        local, mesh=mesh, in_specs=placed, out_specs=P(None, None, "gz", "gx"), check_vma=False
    )
```

```python
import jax
import jax.numpy as jnp
from jax import lax
from jax.experimental import pallas as pl
from jax.experimental.pallas import tpu as pltpu
from jax.sharding import PartitionSpec as P

Q = 19
PLANES = 8
LATTICE = (
    (0, 0, 0),
    (1, 0, 0),
    (-1, 0, 0),
    (0, 1, 0),
    (0, -1, 0),
    (0, 0, 1),
    (0, 0, -1),
    (1, 1, 0),
    (-1, -1, 0),
    (1, -1, 0),
    (-1, 1, 0),
    (1, 0, 1),
    (-1, 0, -1),
    (1, 0, -1),
    (-1, 0, 1),
    (0, 1, 1),
    (0, -1, -1),
    (0, 1, -1),
    (0, -1, 1),
)
OPPOSITE = (0, 2, 1, 4, 3, 6, 5, 8, 7, 10, 9, 12, 11, 14, 13, 16, 15, 18, 17)
INCOMING = (4, 8, 9, 16, 18)
SECOND, THIRD, FOURTH = 1.8, 1.2, 1.1
BASE_DRIVE = 0.0001
DRIVE_GAIN = 1.0
TARGET_FLOW = 0.1

FLAG_SLOT = Q * PLANES
INFLOW_SLOT = FLAG_SLOT + 2
SLOTS = INFLOW_SLOT + len(INCOMING)
TILES = 5
GROUP = 24
SUMS_LANE = 10 * GROUP


def relax(f):
    along = []
    for p in (1, 3, 5):
        along.append((f[p] + f[p + 1], f[p] - f[p + 1]))
    diagonal = []
    for p in (7, 11, 15):
        a, b = f[p] + f[p + 1], f[p + 2] + f[p + 3]
        c, d = f[p] - f[p + 1], f[p + 2] - f[p + 3]
        diagonal.append((a + b, a - b, c + d, c - d))
    (xxyy, xy, xyy, xxy), (xxzz, xz, xzz, xxz), (yyzz, yz, yzz, yyz) = diagonal
    density = f[0] + (along[0][0] + along[1][0] + along[2][0]) + (xxyy + xxzz + yyzz)
    jx = along[0][1] + xyy + xzz
    jy = along[1][1] + xxy + yzz
    jz = along[2][1] + xxz + yyz
    inv = 1.0 / density
    ux, uy, uz = jx * inv, jy * inv, jz * inv
    exx, eyy, ezz = jx * ux, jy * uy, jz * uz
    third = density * (1.0 / 3.0)
    ninth = density * (1.0 / 9.0)
    xx = along[0][0] + xxyy + xxzz
    yy = along[1][0] + xxyy + yyzz
    zz = along[2][0] + xxzz + yyzz
    dxx = SECOND * (xx - third - exx)
    dyy = SECOND * (yy - third - eyy)
    dzz = SECOND * (zz - third - ezz)
    dxy = SECOND * (xy - jx * uy)
    dxz = SECOND * (xz - jx * uz)
    dyz = SECOND * (yz - jy * uz)
    x3, y3, z3 = jx * (1.0 / 3.0), jy * (1.0 / 3.0), jz * (1.0 / 3.0)
    dxyy, dxzz = THIRD * (xyy - x3), THIRD * (xzz - x3)
    dxxy, dyzz = THIRD * (xxy - y3), THIRD * (yzz - y3)
    dxxz, dyyz = THIRD * (xxz - z3), THIRD * (yyz - z3)
    half = 0.5 * (exx + eyy + ezz)
    dxxyy = FOURTH * (xxyy - ninth - (half - 0.5 * ezz) * (2.0 / 3.0) + ezz * (1.0 / 6.0))
    dxxzz = FOURTH * (xxzz - ninth - (half - 0.5 * eyy) * (2.0 / 3.0) + eyy * (1.0 / 6.0))
    dyyzz = FOURTH * (yyzz - ninth - (half - 0.5 * exx) * (2.0 / 3.0) + exx * (1.0 / 6.0))
    out = [None] * Q
    out[0] = f[0] + (dxx + dyy + dzz) - (dxxyy + dxxzz + dyyzz)
    for p, even, odd in (
        (1, dxx - dxxyy - dxxzz, dxyy + dxzz),
        (3, dyy - dxxyy - dyyzz, dxxy + dyzz),
        (5, dzz - dxxzz - dyyzz, dxxz + dyyz),
    ):
        out[p] = f[p] - 0.5 * (even - odd)
        out[p + 1] = f[p + 1] - 0.5 * (even + odd)
    for p, four, cross, first, second in (
        (7, dxxyy, dxy, dxyy, dxxy),
        (11, dxxzz, dxz, dxzz, dxxz),
        (15, dyyzz, dyz, dyzz, dyyz),
    ):
        same, other = 0.25 * (four + cross), 0.25 * (four - cross)
        total, rest = 0.25 * (first + second), 0.25 * (first - second)
        out[p] = f[p] - (same + total)
        out[p + 1] = f[p + 1] - (same - total)
        out[p + 2] = f[p + 2] - (other + rest)
        out[p + 3] = f[p + 3] - (other - rest)
    return out, (ux, uy, uz), inv


def weight(index):
    return 1.0 / 3.0 if index == 0 else (1.0 / 18.0 if index < 7 else 1.0 / 36.0)


def push_parts(index, velocity, inv):
    cx, cy, cz = LATTICE[index]
    along = 9.0 * velocity[0] - 3.0 * velocity[0] + 3.0 * cx
    if cy:
        along = along + (9.0 * cx * cy) * velocity[1]
    if cz:
        along = along + (9.0 * cx * cz) * velocity[2]
    return weight(index) * along, (3.0 * weight(index)) * inv


def driven(relaxed, velocity, inv, drive):
    ux, uy, uz = velocity
    square = drive * drive * inv
    still = -3.0 * drive * ux - 1.5 * square
    moved = still + 9.0 * drive * ux + 4.5 * square
    three = 3.0 * drive
    up, down = moved + three, moved - three
    hy, hz = 9.0 * drive * uy, 9.0 * drive * uz
    calm = still * (1.0 / 36.0)
    out = list(relaxed)
    out[0] = out[0] + still * (1.0 / 3.0)
    out[1] = out[1] + up * (1.0 / 18.0)
    out[2] = out[2] + down * (1.0 / 18.0)
    for index in (3, 4, 5, 6):
        out[index] = out[index] + (calm + calm)
    for p, side in ((7, hy), (11, hz)):
        out[p] = out[p] + (up + side) * (1.0 / 36.0)
        out[p + 1] = out[p + 1] + (down + side) * (1.0 / 36.0)
        out[p + 2] = out[p + 2] + (up - side) * (1.0 / 36.0)
        out[p + 3] = out[p + 3] + (down - side) * (1.0 / 36.0)
    for index in (15, 16, 17, 18):
        out[index] = out[index] + calm
    return out


def rolled(value, step_z, step_x):
    if step_z:
        value = pltpu.roll(value, step_z % value.shape[0], 0)
    if step_x:
        value = pltpu.roll(value, step_x % value.shape[1], 1)
    return value


def slot_values(pops, solid, inflow):
    values = [lambda q=q, y=y: pops[q, y] for q in range(Q) for y in range(PLANES)]
    values += [lambda y=y: solid[y].astype(jnp.float32) for y in range(2)]
    values += [lambda i=i: inflow[i] for i in range(len(INCOMING))]
    return values


def pack_rows(pops_hbm, solid_hbm, inflow_hbm, below, above, pops, solid, inflow, done):
    copies = [
        pltpu.make_async_copy(source, target, done.at[i])
        for i, (source, target) in enumerate(((pops_hbm, pops), (solid_hbm, solid), (inflow_hbm, inflow)))
    ]
    for copy in copies:
        copy.start()
    for copy in copies:
        copy.wait()
    for index, value in enumerate(slot_values(pops, solid, inflow)):
        tile = value()
        below[index] = tile[0:2]
        above[index] = tile[6:8]


def lay_rows(target, main, slot, below, above):
    target[0:8] = main
    target[8:10] = above[slot]
    target[14:16] = below[slot]


def pack_columns(pops, solid, inflow, below, above, edges, rows):
    lane = lax.broadcasted_iota(jnp.int32, (16, 128), 1)
    values = slot_values(pops, solid, inflow)
    rows[8:16] = jnp.zeros((8, 128), jnp.float32)
    for tile in range(TILES):
        packed = jnp.zeros((16, 128), jnp.float32)
        for slot in range(tile * 32, min(tile * 32 + 32, SLOTS)):
            offset = 4 * (slot % 32)
            lay_rows(rows, values[slot](), slot, below, above)
            place = ((lane + (128 - offset + 2)) & 127) < 4
            packed = jnp.where(place, rolled(rows[...], 0, offset), packed)
        edges[tile] = packed


def tally(pops, solid, inflow, below, above, out, flags, weights):
    lane = lax.broadcasted_iota(jnp.int32, (8, 128), 1)
    flags[...] = jnp.zeros(flags.shape, jnp.float32)
    weights[...] = jnp.zeros(weights.shape, jnp.float32)
    for y in range(2):
        lay_rows(flags.at[y], solid[y].astype(jnp.float32), FLAG_SLOT + y, below, above)
    fluid = [1.0 - flags[y, 0:8] for y in range(2)]
    flow = jnp.zeros((8, 128), jnp.float32)
    for y in range(PLANES):
        f = pops
        jx = (
            (f[1, y] - f[2, y])
            + (f[7, y] - f[8, y])
            + (f[9, y] - f[10, y])
            + (f[11, y] - f[12, y])
            + (f[13, y] - f[14, y])
        )
        flow = flow + (jx * fluid[y] if y < 2 else jx)
    one = flow
    count = float(PLANES - 2) + fluid[0] + fluid[1]
    two = jnp.zeros((8, 128), jnp.float32)
    nothing = jnp.zeros((8, 128), jnp.float32)
    for y in (0, 1, 2, PLANES - 1):
        relaxed, velocity, inv = relax([pops[q, y] for q in range(Q)])
        for index in range(Q):
            cx, cy, cz = LATTICE[index]
            target = y + cy
            if not cx or 1 < target < PLANES:
                continue
            linear, square = push_parts(index, velocity, inv)
            factor = -float(cx) if target >= PLANES else -2.0 * cx
            parts = [relaxed[index] * factor, linear * factor, square * factor]
            if y < 2:
                parts = [part * fluid[y] for part in parts]
            if 0 <= target < PLANES:
                beyond = 0 if cx > 0 else 6
                for i, part in enumerate(parts):
                    wide = jnp.concatenate([part, nothing], axis=0)
                    place = beyond + 3 * target + i
                    weights[place] = weights[place] + rolled(wide, cz, 0)
                hit = rolled(flags[target], -cz, -cx)[0:8]
                hit = jnp.where(lane == (127 if cx > 0 else 0), 0.0, hit)
                parts = [part * hit for part in parts]
            one, count, two = one + parts[0], count + parts[1], two + parts[2]
    one = one + (inflow[INCOMING.index(9)] - inflow[INCOMING.index(8)])

    lanes = lax.broadcasted_iota(jnp.int32, (16, 128), 1)
    table = jnp.zeros((16, 128), jnp.float32)
    for place in range(12):
        source = 127 if place < 6 else 0
        table = jnp.where(lanes == place, rolled(weights[place], 0, place - source), table)
    for y in range(2):
        for i in range(3):
            place = 12 + 3 * y + i
            table = jnp.where(lanes == place, rolled(flags[y], 0, place), table)
            table = jnp.where(lanes == place + 6, rolled(flags[y], 0, place + 6 - 127), table)
    table = jnp.concatenate([table, jnp.zeros((16, 128), jnp.float32)], axis=1)
    packed = jnp.zeros((1, 256), jnp.float32)
    for k in range(10):
        row = k if k < 9 else 15
        packed = packed + rolled(table, -row, GROUP * k)[0:1]
    wide = lax.broadcasted_iota(jnp.int32, (1, 256), 1)
    for i, part in enumerate((flow, one, count, two)):
        total = jnp.sum(jnp.sum(part, axis=0, keepdims=True), axis=1, keepdims=True)
        packed = jnp.where(wide == SUMS_LANE + i, total, packed)
    out[...] = jnp.broadcast_to(packed[None], out.shape)


def cross(messages, out):
    table = messages[...]
    count = table.shape[0]
    place = lax.broadcasted_iota(jnp.int32, table.shape, 1)
    within = lax.rem(place, GROUP)
    following = jnp.where(within < 18, pltpu.roll(table, count - 1, 0), pltpu.roll(table, 1, 0))
    matched = jnp.where((within < 12) & (place < SUMS_LANE), table * rolled(following, 0, -12), 0.0)
    matched = jnp.sum(matched, axis=0, keepdims=True)
    sums = jnp.sum(table, axis=0, keepdims=True)
    place, within = place[0:1], within[0:1]
    lane = lax.broadcasted_iota(jnp.int32, (1, 128), 1)
    packed = jnp.zeros((1, 128), jnp.float32)
    for i in range(4):
        part = jnp.where(place == SUMS_LANE + i, sums, 0.0)
        if i:
            part = part + jnp.where(lax.rem(within, 3) == i - 1, matched, 0.0)
        packed = jnp.where(lane == i, jnp.sum(part, axis=1, keepdims=True), packed)
    out[...] = jnp.broadcast_to(packed[None], out.shape)


QUARTERS = tuple(
    (rows, cols)
    for rows in (slice(0, 8), slice(8, 16))
    for cols in (slice(0, 128), slice(128, 256))
)
MAIN = (slice(0, 8), slice(0, 128))


def advance(
    node_total, pops, solid, inflow, below, above, left, right, sums, out, flags, entry, hits, now, moved, edges
):
    total = jnp.sum(sums[...], axis=0)
    flow, one, count, two = (total[:, i : i + 1] for i in range(4))
    first = BASE_DRIVE + DRIVE_GAIN * (TARGET_FLOW - flow / node_total)
    later = (one + count * first + two * (first * first)) / node_total
    second = BASE_DRIVE + DRIVE_GAIN * (TARGET_FLOW - later)

    lane = lax.broadcasted_iota(jnp.int32, (16, 128), 1)
    for tile in range(TILES):
        edges[tile] = jnp.where((lane & 3) < 2, right[tile], left[tile])

    def lay_out(target, main, slot):
        lay_rows(target.at[:, 0:128], main, slot, below, above)
        target[:, 128:256] = rolled(edges[slot // 32], 0, -4 * (slot % 32))

    for y in range(2):
        lay_out(flags.at[y], solid[y].astype(jnp.float32), FLAG_SLOT + y)
        for step_z in (-1, 0, 1):
            for step_x in (-1, 0, 1):
                hits[y, 3 * step_z + step_x + 4] = rolled(flags[y], step_z, step_x)
    for i in range(len(INCOMING)):
        lay_out(entry.at[i], inflow[i], INFLOW_SLOT + i)
    for y in range(PLANES):
        for q in range(Q):
            lay_out(now.at[y, q], pops[q, y], q * PLANES + y)

    for step in range(2):
        drive = jnp.broadcast_to(first if step == 0 else second, (8, 128))

        def collide(y, carry):
            for rows, cols in QUARTERS:
                result = relax([now[y, q, rows, cols] for q in range(Q)])
                for q, value in enumerate(driven(*result, drive)):
                    moved[y, q, rows, cols] = value
            return carry

        lax.fori_loop(0, PLANES, collide, 0)
        part = (slice(0, 16), slice(0, 256)) if step == 0 else MAIN
        for y in range(PLANES):
            for q in range(Q):
                cx, cy, cz = LATTICE[q]
                source = y - cy
                if source < 0:
                    arrived = moved[(y, OPPOSITE[q]) + part]
                elif source >= PLANES:
                    arrived = entry[(INCOMING.index(q),) + part]
                else:
                    arrived = rolled(moved[source, q], cz, cx)[part]
                    if source < 2:
                        hit = hits[(source, 3 * cz + cx + 4) + part]
                        arrived = jnp.where(hit > 0.5, moved[(y, OPPOSITE[q]) + part], arrived)
                if y < 2:
                    arrived = jnp.where(flags[(y,) + part] > 0.5, now[(y, q) + part], arrived)
                if step == 0:
                    now[y, q] = arrived
                else:
                    out[q, y] = arrived


def kernel_call(body, shapes, scratch, *operands, memory=pltpu.VMEM):
    vmem = pl.BlockSpec(memory_space=pltpu.VMEM)
    return pl.pallas_call(
        body,
        in_specs=[pl.BlockSpec(memory_space=memory)] * len(operands),
        out_specs=[vmem] * len(shapes),
        out_shape=[pltpu.VMEM(item, jnp.float32) if isinstance(item, tuple) else item for item in shapes],
        scratch_shapes=[
            pltpu.VMEM(item, jnp.float32) if isinstance(item, tuple) else item for item in scratch
        ],
        compiler_params=pltpu.CompilerParams(vmem_limit_bytes=20 * 1024 * 1024),
    )(*operands)


def neighbours(axis, low, high):
    count = lax.axis_size(axis)
    up = [(i, (i + 1) % count) for i in range(count)]
    down = [(target, source) for source, target in up]
    return lax.ppermute(high, axis, up), lax.ppermute(low, axis, down)


def local(populations, solid, top_inflow):
    along_x, along_z = lax.axis_size("gx"), lax.axis_size("gz")
    node_total = float(PLANES * 8 * 128 * along_x * along_z)
    fields = (populations, solid, top_inflow)
    below, above, *fields = kernel_call(
        pack_rows,
        [(SLOTS, 2, 128)] * 2 + [pltpu.VMEM(field.shape, field.dtype) for field in fields],
        [pltpu.SemaphoreType.DMA((3,))],
        *(pltpu.with_memory_space_constraint(field, pltpu.HBM) for field in fields),
        memory=pltpu.HBM,
    )
    halo = neighbours("gz", below, above)
    (sums,) = kernel_call(tally, [(along_x, 1, 256)], [(2, 16, 128), (12, 16, 128)], *fields, *halo)
    sums = lax.all_to_all(sums, "gx", 0, 0, tiled=True)
    (edges,) = kernel_call(pack_columns, [(TILES, 16, 128)], [(16, 128)], *fields, *halo)
    left, right = neighbours("gx", edges, edges)
    (sums,) = kernel_call(cross, [(along_z, 1, 128)], [], sums.reshape(along_x, 256))
    sums = lax.all_to_all(sums, "gz", 0, 0, tiled=True)
    lattice = (PLANES, Q, 16, 256)
    (advanced,) = kernel_call(
        lambda *refs: advance(node_total, *refs),
        [jax.ShapeDtypeStruct((Q, PLANES, 8, 128), jnp.float32)],
        [
            (2, 16, 256),
            (len(INCOMING), 16, 256),
            (2, 9, 16, 256),
            lattice,
            lattice,
            (TILES, 16, 128),
        ],
        *fields,
        *halo,
        left,
        right,
        sums,
    )
    return advanced


def solution(mesh):
    placed = (P(None, None, "gz", "gx"), P(None, "gz", "gx"), P(None, "gz", "gx"))
    return jax.shard_map(
        local, mesh=mesh, in_specs=placed, out_specs=P(None, None, "gz", "gx"), check_vma=False
    )
```

```python
import jax
import jax.numpy as jnp
from jax import lax
from jax.experimental import pallas as pl
from jax.experimental.pallas import tpu as pltpu
from jax.sharding import PartitionSpec as P

Q = 19
PLANES = 8
LATTICE = (
    (0, 0, 0),
    (1, 0, 0),
    (-1, 0, 0),
    (0, 1, 0),
    (0, -1, 0),
    (0, 0, 1),
    (0, 0, -1),
    (1, 1, 0),
    (-1, -1, 0),
    (1, -1, 0),
    (-1, 1, 0),
    (1, 0, 1),
    (-1, 0, -1),
    (1, 0, -1),
    (-1, 0, 1),
    (0, 1, 1),
    (0, -1, -1),
    (0, 1, -1),
    (0, -1, 1),
)
OPPOSITE = (0, 2, 1, 4, 3, 6, 5, 8, 7, 10, 9, 12, 11, 14, 13, 16, 15, 18, 17)
INCOMING = (4, 8, 9, 16, 18)
SECOND, THIRD, FOURTH = 1.8, 1.2, 1.1
BASE_DRIVE = 0.0001
DRIVE_GAIN = 1.0
TARGET_FLOW = 0.1

FLAG_SLOT = Q * PLANES
INFLOW_SLOT = FLAG_SLOT + 2
SLOTS = INFLOW_SLOT + len(INCOMING)
TILES = 5
ROW_TILES = 40
GROUP = 24
SUMS_LANE = 10 * GROUP


def relax(f):
    along = []
    for p in (1, 3, 5):
        along.append((f[p] + f[p + 1], f[p] - f[p + 1]))
    diagonal = []
    for p in (7, 11, 15):
        a, b = f[p] + f[p + 1], f[p + 2] + f[p + 3]
        c, d = f[p] - f[p + 1], f[p + 2] - f[p + 3]
        diagonal.append((a + b, a - b, c + d, c - d))
    (xxyy, xy, xyy, xxy), (xxzz, xz, xzz, xxz), (yyzz, yz, yzz, yyz) = diagonal
    density = f[0] + (along[0][0] + along[1][0] + along[2][0]) + (xxyy + xxzz + yyzz)
    jx = along[0][1] + xyy + xzz
    jy = along[1][1] + xxy + yzz
    jz = along[2][1] + xxz + yyz
    inv = 1.0 / density
    ux, uy, uz = jx * inv, jy * inv, jz * inv
    exx, eyy, ezz = jx * ux, jy * uy, jz * uz
    third = density * (1.0 / 3.0)
    ninth = density * (1.0 / 9.0)
    xx = along[0][0] + xxyy + xxzz
    yy = along[1][0] + xxyy + yyzz
    zz = along[2][0] + xxzz + yyzz
    dxx = SECOND * (xx - third - exx)
    dyy = SECOND * (yy - third - eyy)
    dzz = SECOND * (zz - third - ezz)
    dxy = SECOND * (xy - jx * uy)
    dxz = SECOND * (xz - jx * uz)
    dyz = SECOND * (yz - jy * uz)
    x3, y3, z3 = jx * (1.0 / 3.0), jy * (1.0 / 3.0), jz * (1.0 / 3.0)
    dxyy, dxzz = THIRD * (xyy - x3), THIRD * (xzz - x3)
    dxxy, dyzz = THIRD * (xxy - y3), THIRD * (yzz - y3)
    dxxz, dyyz = THIRD * (xxz - z3), THIRD * (yyz - z3)
    half = 0.5 * (exx + eyy + ezz)
    dxxyy = FOURTH * (xxyy - ninth - (half - 0.5 * ezz) * (2.0 / 3.0) + ezz * (1.0 / 6.0))
    dxxzz = FOURTH * (xxzz - ninth - (half - 0.5 * eyy) * (2.0 / 3.0) + eyy * (1.0 / 6.0))
    dyyzz = FOURTH * (yyzz - ninth - (half - 0.5 * exx) * (2.0 / 3.0) + exx * (1.0 / 6.0))
    out = [None] * Q
    out[0] = f[0] + (dxx + dyy + dzz) - (dxxyy + dxxzz + dyyzz)
    for p, even, odd in (
        (1, dxx - dxxyy - dxxzz, dxyy + dxzz),
        (3, dyy - dxxyy - dyyzz, dxxy + dyzz),
        (5, dzz - dxxzz - dyyzz, dxxz + dyyz),
    ):
        out[p] = f[p] - 0.5 * (even - odd)
        out[p + 1] = f[p + 1] - 0.5 * (even + odd)
    for p, four, cross, first, second in (
        (7, dxxyy, dxy, dxyy, dxxy),
        (11, dxxzz, dxz, dxzz, dxxz),
        (15, dyyzz, dyz, dyzz, dyyz),
    ):
        same, other = 0.25 * (four + cross), 0.25 * (four - cross)
        total, rest = 0.25 * (first + second), 0.25 * (first - second)
        out[p] = f[p] - (same + total)
        out[p + 1] = f[p + 1] - (same - total)
        out[p + 2] = f[p + 2] - (other + rest)
        out[p + 3] = f[p + 3] - (other - rest)
    return out, (ux, uy, uz), inv


def weight(index):
    return 1.0 / 3.0 if index == 0 else (1.0 / 18.0 if index < 7 else 1.0 / 36.0)


def push_parts(index, velocity, inv):
    cx, cy, cz = LATTICE[index]
    along = 9.0 * velocity[0] - 3.0 * velocity[0] + 3.0 * cx
    if cy:
        along = along + (9.0 * cx * cy) * velocity[1]
    if cz:
        along = along + (9.0 * cx * cz) * velocity[2]
    return weight(index) * along, (3.0 * weight(index)) * inv


def driven(relaxed, velocity, inv, drive):
    ux, uy, uz = velocity
    square = drive * drive * inv
    still = -3.0 * drive * ux - 1.5 * square
    moved = still + 9.0 * drive * ux + 4.5 * square
    three = 3.0 * drive
    up, down = moved + three, moved - three
    hy, hz = 9.0 * drive * uy, 9.0 * drive * uz
    calm = still * (1.0 / 36.0)
    out = list(relaxed)
    out[0] = out[0] + still * (1.0 / 3.0)
    out[1] = out[1] + up * (1.0 / 18.0)
    out[2] = out[2] + down * (1.0 / 18.0)
    for index in (3, 4, 5, 6):
        out[index] = out[index] + (calm + calm)
    for p, side in ((7, hy), (11, hz)):
        out[p] = out[p] + (up + side) * (1.0 / 36.0)
        out[p + 1] = out[p + 1] + (down + side) * (1.0 / 36.0)
        out[p + 2] = out[p + 2] + (up - side) * (1.0 / 36.0)
        out[p + 3] = out[p + 3] + (down - side) * (1.0 / 36.0)
    for index in (15, 16, 17, 18):
        out[index] = out[index] + calm
    return out


def rolled(value, step_z, step_x):
    if step_z:
        value = pltpu.roll(value, step_z % value.shape[0], 0)
    if step_x:
        value = pltpu.roll(value, step_x % value.shape[1], 1)
    return value


def slot_values(pops, solid, inflow):
    values = [lambda q=q, y=y: pops[q, y] for q in range(Q) for y in range(PLANES)]
    values += [lambda y=y: solid[y].astype(jnp.float32) for y in range(2)]
    values += [lambda i=i: inflow[i] for i in range(len(INCOMING))]
    return values


def is_odd(axis):
    return lax.axis_index(axis) % 2 == 1


def pack_rows(pops_hbm, solid_hbm, inflow_hbm, first, second, pops, solid, inflow, done):
    copies = [
        pltpu.make_async_copy(source, target, done.at[i])
        for i, (source, target) in enumerate(((pops_hbm, pops), (solid_hbm, solid), (inflow_hbm, inflow)))
    ]
    for copy in copies:
        copy.start()
    for copy in copies:
        copy.wait()
    odd = is_odd("gz")
    for slot, value in enumerate(slot_values(pops, solid, inflow)):
        tile = value()
        low, high = tile[0:2], tile[6:8]
        place = (slot // 4, slice(2 * (slot % 4), 2 * (slot % 4) + 2))
        first[place] = jnp.where(odd, low, high)
        second[place] = jnp.where(odd, high, low)


def lay_rows(target, main, slot, odd, first, second):
    place = (slot // 4, slice(2 * (slot % 4), 2 * (slot % 4) + 2))
    one, two = first[place], second[place]
    target[0:8] = main
    target[8:10] = jnp.where(odd, two, one)
    target[14:16] = jnp.where(odd, one, two)


def tally(pops, solid, inflow, first, second, out, flags):
    lane = lax.broadcasted_iota(jnp.int32, (8, 128), 1)
    odd = is_odd("gz")
    flags[...] = jnp.zeros(flags.shape, jnp.float32)
    for y in range(2):
        lay_rows(flags.at[y], solid[y].astype(jnp.float32), FLAG_SLOT + y, odd, first, second)
    fluid = [1.0 - flags[y, 0:8] for y in range(2)]
    flow = jnp.zeros((8, 128), jnp.float32)
    for y in range(PLANES):
        f = pops
        jx = (
            (f[1, y] - f[2, y])
            + (f[7, y] - f[8, y])
            + (f[9, y] - f[10, y])
            + (f[11, y] - f[12, y])
            + (f[13, y] - f[14, y])
        )
        flow = flow + (jx * fluid[y] if y < 2 else jx)
    one = flow
    count = float(PLANES - 2) + fluid[0] + fluid[1]
    two = jnp.zeros((8, 128), jnp.float32)
    weights = {}
    for y in (0, 1, 2, PLANES - 1):
        relaxed, velocity, inv = relax([pops[q, y] for q in range(Q)])
        for index in range(Q):
            cx, cy, cz = LATTICE[index]
            target = y + cy
            if not cx or 1 < target < PLANES:
                continue
            linear, square = push_parts(index, velocity, inv)
            factor = -float(cx) if target >= PLANES else -2.0 * cx
            parts = [relaxed[index] * factor, linear * factor, square * factor]
            if y < 2:
                parts = [part * fluid[y] for part in parts]
            if 0 <= target < PLANES:
                for i, part in enumerate(parts):
                    key = ((0 if cx > 0 else 6) + 3 * target + i, cz)
                    weights[key] = weights[key] + part if key in weights else part
                hit = rolled(flags[target], -cz, -cx)[0:8]
                hit = jnp.where(lane == (127 if cx > 0 else 0), 0.0, hit)
                parts = [part * hit for part in parts]
            one, count, two = one + parts[0], count + parts[1], two + parts[2]
    one = one + (inflow[INCOMING.index(9)] - inflow[INCOMING.index(8)])

    nothing = jnp.zeros((8, 128), jnp.float32)
    by_row = {-1: nothing, 0: nothing, 1: nothing}
    for (place, cz), part in weights.items():
        by_row[cz] = jnp.where(lane == place, rolled(part, 0, place - (127 if place < 6 else 0)), by_row[cz])
    table = jnp.zeros((16, 128), jnp.float32)
    for cz, part in by_row.items():
        table = table + rolled(jnp.concatenate([part, nothing], axis=0), cz, 0)
    lanes = lax.broadcasted_iota(jnp.int32, (16, 128), 1)
    for y in range(2):
        for i in range(3):
            place = 12 + 3 * y + i
            table = jnp.where(lanes == place, rolled(flags[y], 0, place), table)
            table = jnp.where(lanes == place + 6, rolled(flags[y], 0, place + 6 - 127), table)
    halves = [nothing, nothing]
    for k in range(10):
        row = k if k < 9 else 15
        spread = rolled(jnp.broadcast_to(table[row : row + 1], (8, 128)), 0, (GROUP * k) % 128)
        for half in range(2):
            start = GROUP * k - 128 * half
            if -GROUP < start < 128:
                halves[half] = jnp.where((lane >= start) & (lane < start + GROUP), spread, halves[half])
    for i, part in enumerate((flow, one, count, two)):
        total = jnp.sum(jnp.sum(part, axis=0, keepdims=True), axis=1, keepdims=True)
        halves[1] = jnp.where(lane == SUMS_LANE - 128 + i, total, halves[1])
    packed = jnp.concatenate([halves[0][0:1], halves[1][0:1]], axis=1)
    out[...] = jnp.broadcast_to(packed[None], out.shape)


def cross(messages, edges, out, edges_out):
    table = messages[...]
    count = table.shape[0]
    place = lax.broadcasted_iota(jnp.int32, table.shape, 1)
    within = lax.rem(place, GROUP)
    following = jnp.where(within < 18, pltpu.roll(table, count - 1, 0), pltpu.roll(table, 1, 0))
    matched = jnp.where(within < 12, table * rolled(following, 0, -12), 0.0)
    packed = jnp.sum(jnp.where(place < SUMS_LANE, matched, table), axis=0, keepdims=True)
    out[...] = jnp.broadcast_to(packed[None], out.shape)
    edges_out[...] = edges[...]


def drives(sums, node_total):
    packed = jnp.sum(sums, axis=0)
    place = lax.broadcasted_iota(jnp.int32, packed.shape, 1)
    within = lax.rem(place, GROUP)
    totals = []
    for i in range(4):
        keep = place == SUMS_LANE + i
        if i:
            keep = keep | ((place < SUMS_LANE) & (within < 12) & (lax.rem(within, 3) == i - 1))
        totals.append(jnp.sum(jnp.where(keep, packed, 0.0), axis=1, keepdims=True))
    flow, one, count, two = totals
    first = BASE_DRIVE + DRIVE_GAIN * (TARGET_FLOW - flow / node_total)
    later = (one + count * first + two * (first * first)) / node_total
    second = BASE_DRIVE + DRIVE_GAIN * (TARGET_FLOW - later)
    return jnp.broadcast_to(first, (8, 128)), jnp.broadcast_to(second, (8, 128))


HALVES = (slice(0, 8), slice(8, 16))


def prepare(pops, solid, inflow, first, second, edges, kept, relaxed, state, flags, entry, rows):
    odd = is_odd("gz")
    lane = lax.broadcasted_iota(jnp.int32, (8, 128), 1)
    row = lax.broadcasted_iota(jnp.int32, (8, 128), 0)
    values = slot_values(pops, solid, inflow)
    for tile in range(TILES):
        packed = [jnp.zeros((8, 128), jnp.float32)] * 2
        for slot in range(tile * 32, min(tile * 32 + 32, SLOTS)):
            offset = 4 * (slot % 32)
            one, two = first[slot // 4], second[slot // 4]
            above, below = jnp.where(odd, two, one), jnp.where(odd, one, two)
            start = 2 * (slot % 4)
            outer = jnp.where(row < 4, rolled(above, -start, 0), rolled(below, 6 - start, 0))
            place = ((lane + (128 - offset + 2)) & 127) < 4
            for half, value in enumerate((values[slot](), outer)):
                packed[half] = jnp.where(place, rolled(value, 0, offset), packed[half])
        edges[tile, 0:8] = packed[0]
        edges[tile, 8:16] = packed[1]
    for y in range(2):
        lay_rows(flags.at[y], solid[y].astype(jnp.float32), FLAG_SLOT + y, odd, first, second)
    for i in range(len(INCOMING)):
        lay_rows(entry.at[i], inflow[i], INFLOW_SLOT + i, odd, first, second)
    for y in range(PLANES):
        for q in range(Q):
            lay_rows(rows.at[y, q], pops[q, y], q * PLANES + y, odd, first, second)
    kept[...] = rows[0:2]

    def collide(y, carry):
        for half in HALVES:
            result, velocity, inv = relax([rows[y, q, half] for q in range(Q)])
            for q in range(Q):
                relaxed[y, q, half] = result[q]
            for i, value in enumerate(velocity + (inv,)):
                state[y, i, half] = value
        return carry

    lax.fori_loop(0, PLANES, collide, 0)


def advance(
    node_total, kept, relaxed, state, flags, entry, near, far, sums,
    out_hbm, out, moved, now, moved_side, now_side, hits, hits_side, done,
):
    drive, drive_later = drives(sums[...], node_total)
    odd = is_odd("gx")
    lane = lax.broadcasted_iota(jnp.int32, (16, 128), 1)
    edges = []
    for tile in range(TILES):
        one, two = near[tile], far[tile]
        low, high = jnp.where(odd, one, two), jnp.where(odd, two, one)
        edges.append(jnp.where((lane & 3) < 2, high, low))
    for q in range(Q):
        now_side[q] = rolled(edges[q // 4], 0, -32 * (q % 4))
    wall = ((lane + 2) & 127) < 8
    flags_side = jnp.where(wall, rolled(edges[4], 0, -96), 0.0)
    stay_side = flags_side > 0.5

    def sideways(value, q, source):
        cx, _, cz = LATTICE[q]
        lane_to = 0 if cx > 0 else 127
        return lane == lane_to, rolled(value, cz, lane_to - (4 * source - (1 if cx > 0 else 0)))

    def inward(q, source):
        cx, cy, cz = LATTICE[q]
        lane_to = 4 * (source + cy) - (0 if cx > 0 else 1)
        return lane == lane_to % 128, lane_to - (127 if cx > 0 else 0)

    for q in range(Q):
        cx, cy, cz = LATTICE[q]
        for source in range(2):
            hit = rolled(flags[source], cz, cx)
            if cx:
                edge, value = sideways(flags_side, q, source)
                hit = jnp.where(edge, value, hit)
            hits[source, q] = hit
        hit = rolled(flags_side, cz, 4 * cy + cx)
        for source in range(2):
            if cx and 0 <= source + cy:
                edge, shift = inward(q, source)
                hit = jnp.where(edge, rolled(flags[source], cz, shift), hit)
        if cy > 0:
            hit = jnp.where(((lane + 2) & 127) < 4, 1.0, hit)
        hits_side[q] = hit

    def push(y, carry):
        for half in HALVES:
            velocity = tuple(state[y, i, half] for i in range(3))
            result = driven([relaxed[y, q, half] for q in range(Q)], velocity, state[y, 3, half], drive)
            for q in range(Q):
                moved[y, q, half] = result[q]
        return carry

    def collide(y, carry):
        for half in HALVES:
            result = driven(*relax([now[y, q, half] for q in range(Q)]), drive_later)
            for q in range(Q):
                moved[y, q, half] = result[q]
        return carry

    def collide_side(applied):
        for half in HALVES:
            result = driven(*relax([now_side[q, half] for q in range(Q)]), applied)
            for q in range(Q):
                moved_side[q, half] = result[q]

    def arrive(y, q, part):
        cx, cy, cz = LATTICE[q]
        source = y - cy
        if source < 0:
            arrived = moved[y, OPPOSITE[q], part]
        elif source >= PLANES:
            arrived = entry[INCOMING.index(q), part]
        else:
            arrived = rolled(moved[source, q], cz, cx)
            if cx:
                edge, value = sideways(moved_side[q], q, source)
                arrived = jnp.where(edge, value, arrived)
            arrived = arrived[part]
            if source < 2:
                arrived = jnp.where(hits[source, q, part] > 0.5, moved[y, OPPOSITE[q], part], arrived)
        if y < 2:
            before = kept if part == slice(0, 16) else now
            arrived = jnp.where(flags[y, part] > 0.5, before[y, q, part], arrived)
        return arrived

    def arrive_side(q):
        cx, cy, cz = LATTICE[q]
        arrived = rolled(moved_side[q], cz, 4 * cy + cx)
        if cx:
            for source in range(PLANES):
                if 0 <= source + cy < PLANES:
                    edge, shift = inward(q, source)
                    arrived = jnp.where(edge, rolled(moved[source, q], cz, shift), arrived)
        arrived = jnp.where(hits_side[q] > 0.5, moved_side[OPPOSITE[q]], arrived)
        if cy < 0:
            slot = (INFLOW_SLOT + INCOMING.index(q)) % 32
            value = rolled(edges[INFLOW_SLOT // 32], 0, 4 * (PLANES - 1) - 4 * slot)
            arrived = jnp.where(((lane - 26) & 127) < 4, value, arrived)
        return jnp.where(stay_side, now_side[q], arrived)

    lax.fori_loop(0, PLANES, push, 0)
    collide_side(drive)
    for y in range(PLANES):
        for q in range(Q):
            now[y, q] = arrive(y, q, slice(0, 16))
    for q in range(Q):
        now_side[q] = arrive_side(q)
    lax.fori_loop(0, PLANES, collide, 0)
    collide_side(drive_later)
    copies = []
    for y in range(PLANES):
        for q in range(Q):
            out[y, q] = arrive(y, q, slice(0, 8))
        copies.append(pltpu.make_async_copy(out.at[y], out_hbm.at[:, y], done.at[y]))
        copies[-1].start()
    for copy in copies:
        copy.wait()


def kernel_call(body, shapes, scratch, *operands, memory=pltpu.VMEM):
    return pl.pallas_call(
        body,
        in_specs=[pl.BlockSpec(memory_space=memory)] * len(operands),
        out_specs=[pl.BlockSpec(memory_space=pltpu.VMEM)] * len(shapes),
        out_shape=[pltpu.VMEM(item, jnp.float32) if isinstance(item, tuple) else item for item in shapes],
        scratch_shapes=[
            pltpu.VMEM(item, jnp.float32) if isinstance(item, tuple) else item for item in scratch
        ],
        compiler_params=pltpu.CompilerParams(vmem_limit_bytes=20 * 1024 * 1024),
    )(*operands)


def swapped(axis, first, second):
    count = lax.axis_size(axis)
    pairs = [(i, i ^ 1) for i in range(count)]
    others = [(i, (i + 1 if i % 2 else i - 1) % count) for i in range(count)]
    return lax.ppermute(first, axis, pairs), lax.ppermute(second, axis, others)


def local(populations, solid, top_inflow):
    along_x, along_z = lax.axis_size("gx"), lax.axis_size("gz")
    node_total = float(PLANES * 8 * 128 * along_x * along_z)
    fields = (populations, solid, top_inflow)
    first, second, *fields = kernel_call(
        pack_rows,
        [(ROW_TILES, 8, 128)] * 2 + [pltpu.VMEM(field.shape, field.dtype) for field in fields],
        [pltpu.SemaphoreType.DMA((3,))],
        *(pltpu.with_memory_space_constraint(field, pltpu.HBM) for field in fields),
        memory=pltpu.HBM,
    )
    halo = swapped("gz", first, second)
    (sums,) = kernel_call(tally, [(along_x, 1, 256)], [(2, 16, 128)], *fields, *halo)
    sums = lax.all_to_all(sums, "gx", 0, 0, tiled=True)
    edges, *prepared = kernel_call(
        prepare,
        [
            (TILES, 16, 128),
            (2, Q, 16, 128),
            (PLANES, Q, 16, 128),
            (PLANES, 4, 16, 128),
            (2, 16, 128),
            (len(INCOMING), 16, 128),
        ],
        [(PLANES, Q, 16, 128)],
        *fields,
        *halo,
    )
    sums, edges = kernel_call(
        cross,
        [(along_z, 1, 256), (TILES, 16, 128)],
        [],
        sums.reshape(along_x, 256),
        edges,
    )
    sums = lax.all_to_all(sums, "gz", 0, 0, tiled=True)
    near, far = swapped("gx", edges, edges)
    (advanced,) = pl.pallas_call(
        lambda *refs: advance(node_total, *refs),
        in_specs=[pl.BlockSpec(memory_space=pltpu.VMEM)] * 8,
        out_specs=[pl.BlockSpec(memory_space=pltpu.HBM)],
        out_shape=[jax.ShapeDtypeStruct((Q, PLANES, 8, 128), jnp.float32)],
        scratch_shapes=[
            pltpu.VMEM((PLANES, Q, 8, 128), jnp.float32),
            pltpu.VMEM((PLANES, Q, 16, 128), jnp.float32),
            pltpu.VMEM((PLANES, Q, 16, 128), jnp.float32),
            pltpu.VMEM((Q, 16, 128), jnp.float32),
            pltpu.VMEM((Q, 16, 128), jnp.float32),
            pltpu.VMEM((2, Q, 16, 128), jnp.float32),
            pltpu.VMEM((Q, 16, 128), jnp.float32),
            pltpu.SemaphoreType.DMA((PLANES,)),
        ],
        compiler_params=pltpu.CompilerParams(vmem_limit_bytes=20 * 1024 * 1024),
    )(*prepared, near, far, sums)
    return advanced


def solution(mesh):
    placed = (P(None, None, "gz", "gx"), P(None, "gz", "gx"), P(None, "gz", "gx"))
    return jax.shard_map(
        local, mesh=mesh, in_specs=placed, out_specs=P(None, None, "gz", "gx"), check_vma=False
    )
```

```python
import jax
import jax.numpy as jnp
from jax import lax
from jax.experimental import pallas as pl
from jax.experimental.pallas import tpu as pltpu
from jax.sharding import PartitionSpec as P


Q = 19
PLANES = 8
LATTICE = (
    (0, 0, 0),
    (1, 0, 0),
    (-1, 0, 0),
    (0, 1, 0),
    (0, -1, 0),
    (0, 0, 1),
    (0, 0, -1),
    (1, 1, 0),
    (-1, -1, 0),
    (1, -1, 0),
    (-1, 1, 0),
    (1, 0, 1),
    (-1, 0, -1),
    (1, 0, -1),
    (-1, 0, 1),
    (0, 1, 1),
    (0, -1, -1),
    (0, 1, -1),
    (0, -1, 1),
)
OPPOSITE = (0, 2, 1, 4, 3, 6, 5, 8, 7, 10, 9, 12, 11, 14, 13, 16, 15, 18, 17)
INCOMING = (4, 8, 9, 16, 18)
SECOND, THIRD, FOURTH = 1.8, 1.2, 1.1
BASE_DRIVE = 0.0001
DRIVE_GAIN = 1.0
TARGET_FLOW = 0.1

FLAG_SLOT = Q * PLANES
INFLOW_SLOT = FLAG_SLOT + 2
SLOTS = INFLOW_SLOT + len(INCOMING)
TILES = 5
ROW_TILES = 40
PIECES = ((0, 5), (5, 10), (10, 15), (15, 19))
GROUP = 24
SUMS_LANE = 10 * GROUP


def relax(f):
    along = []
    for p in (1, 3, 5):
        along.append((f[p] + f[p + 1], f[p] - f[p + 1]))
    diagonal = []
    for p in (7, 11, 15):
        a, b = f[p] + f[p + 1], f[p + 2] + f[p + 3]
        c, d = f[p] - f[p + 1], f[p + 2] - f[p + 3]
        diagonal.append((a + b, a - b, c + d, c - d))
    (xxyy, xy, xyy, xxy), (xxzz, xz, xzz, xxz), (yyzz, yz, yzz, yyz) = diagonal
    density = f[0] + (along[0][0] + along[1][0] + along[2][0]) + (xxyy + xxzz + yyzz)
    jx = along[0][1] + xyy + xzz
    jy = along[1][1] + xxy + yzz
    jz = along[2][1] + xxz + yyz
    inv = 1.0 / density
    ux, uy, uz = jx * inv, jy * inv, jz * inv
    exx, eyy, ezz = jx * ux, jy * uy, jz * uz
    third = density * (1.0 / 3.0)
    ninth = density * (1.0 / 9.0)
    xx = along[0][0] + xxyy + xxzz
    yy = along[1][0] + xxyy + yyzz
    zz = along[2][0] + xxzz + yyzz
    dxx = SECOND * (xx - third - exx)
    dyy = SECOND * (yy - third - eyy)
    dzz = SECOND * (zz - third - ezz)
    dxy = SECOND * (xy - jx * uy)
    dxz = SECOND * (xz - jx * uz)
    dyz = SECOND * (yz - jy * uz)
    x3, y3, z3 = jx * (1.0 / 3.0), jy * (1.0 / 3.0), jz * (1.0 / 3.0)
    dxyy, dxzz = THIRD * (xyy - x3), THIRD * (xzz - x3)
    dxxy, dyzz = THIRD * (xxy - y3), THIRD * (yzz - y3)
    dxxz, dyyz = THIRD * (xxz - z3), THIRD * (yyz - z3)
    half = 0.5 * (exx + eyy + ezz)
    dxxyy = FOURTH * (xxyy - ninth - (half - 0.5 * ezz) * (2.0 / 3.0) + ezz * (1.0 / 6.0))
    dxxzz = FOURTH * (xxzz - ninth - (half - 0.5 * eyy) * (2.0 / 3.0) + eyy * (1.0 / 6.0))
    dyyzz = FOURTH * (yyzz - ninth - (half - 0.5 * exx) * (2.0 / 3.0) + exx * (1.0 / 6.0))
    out = [None] * Q
    out[0] = f[0] + (dxx + dyy + dzz) - (dxxyy + dxxzz + dyyzz)
    for p, even, odd in (
        (1, dxx - dxxyy - dxxzz, dxyy + dxzz),
        (3, dyy - dxxyy - dyyzz, dxxy + dyzz),
        (5, dzz - dxxzz - dyyzz, dxxz + dyyz),
    ):
        out[p] = f[p] - 0.5 * (even - odd)
        out[p + 1] = f[p + 1] - 0.5 * (even + odd)
    for p, four, cross, first, second in (
        (7, dxxyy, dxy, dxyy, dxxy),
        (11, dxxzz, dxz, dxzz, dxxz),
        (15, dyyzz, dyz, dyzz, dyyz),
    ):
        same, other = 0.25 * (four + cross), 0.25 * (four - cross)
        total, rest = 0.25 * (first + second), 0.25 * (first - second)
        out[p] = f[p] - (same + total)
        out[p + 1] = f[p + 1] - (same - total)
        out[p + 2] = f[p + 2] - (other + rest)
        out[p + 3] = f[p + 3] - (other - rest)
    return out, (ux, uy, uz), inv


def weight(index):
    return 1.0 / 3.0 if index == 0 else (1.0 / 18.0 if index < 7 else 1.0 / 36.0)


def push_parts(index, velocity, inv):
    cx, cy, cz = LATTICE[index]
    along = 9.0 * velocity[0] - 3.0 * velocity[0] + 3.0 * cx
    if cy:
        along = along + (9.0 * cx * cy) * velocity[1]
    if cz:
        along = along + (9.0 * cx * cz) * velocity[2]
    return weight(index) * along, (3.0 * weight(index)) * inv


def driven(relaxed, velocity, inv, drive):
    ux, uy, uz = velocity
    square = drive * drive * inv
    still = -3.0 * drive * ux - 1.5 * square
    moved = still + 9.0 * drive * ux + 4.5 * square
    three = 3.0 * drive
    up, down = moved + three, moved - three
    hy, hz = 9.0 * drive * uy, 9.0 * drive * uz
    calm = still * (1.0 / 36.0)
    out = list(relaxed)
    out[0] = out[0] + still * (1.0 / 3.0)
    out[1] = out[1] + up * (1.0 / 18.0)
    out[2] = out[2] + down * (1.0 / 18.0)
    for index in (3, 4, 5, 6):
        out[index] = out[index] + (calm + calm)
    for p, side in ((7, hy), (11, hz)):
        out[p] = out[p] + (up + side) * (1.0 / 36.0)
        out[p + 1] = out[p + 1] + (down + side) * (1.0 / 36.0)
        out[p + 2] = out[p + 2] + (up - side) * (1.0 / 36.0)
        out[p + 3] = out[p + 3] + (down - side) * (1.0 / 36.0)
    for index in (15, 16, 17, 18):
        out[index] = out[index] + calm
    return out


def rolled(value, step_z, step_x):
    if step_z:
        value = pltpu.roll(value, step_z % value.shape[0], 0)
    if step_x:
        value = pltpu.roll(value, step_x % value.shape[1], 1)
    return value


def slot_values(pops, solid, inflow):
    values = [lambda q=q, y=y: pops[q, y] for q in range(Q) for y in range(PLANES)]
    values += [lambda y=y: solid[y].astype(jnp.float32) for y in range(2)]
    values += [lambda i=i: inflow[i] for i in range(len(INCOMING))]
    return values


def is_odd(axis):
    return lax.axis_index(axis) % 2 == 1


def load(pops_hbm, solid_hbm, inflow_hbm, first, second, pops, solid, inflow, done):
    copies = [(solid_hbm, solid), (inflow_hbm, inflow)]
    copies += [(pops_hbm.at[a:b], pops.at[a:b]) for a, b in PIECES]
    copies = [pltpu.make_async_copy(source, target, done.at[i]) for i, (source, target) in enumerate(copies)]
    for copy in copies:
        copy.start()
    copies[0].wait()
    odd = is_odd("gz")
    first[...] = jnp.zeros(first.shape, jnp.float32)
    second[...] = jnp.zeros(second.shape, jnp.float32)
    for y in range(2):
        tile = solid[y].astype(jnp.float32)
        low, high = tile[0:2], tile[6:8]
        first[2 * y : 2 * y + 2] = jnp.where(odd, low, high)
        second[2 * y : 2 * y + 2] = jnp.where(odd, high, low)
    for copy in copies[1:]:
        copy.wait()


def pack_rows(pops, inflow, after, first, second):
    odd = is_odd("gz")
    values = [(q * PLANES + y, pops[q, y]) for q in range(Q) for y in range(PLANES)]
    values += [(INFLOW_SLOT + i, inflow[i]) for i in range(len(INCOMING))]
    for slot, tile in values:
        low, high = tile[0:2], tile[6:8]
        place = (slot // 4, slice(2 * (slot % 4), 2 * (slot % 4) + 2))
        first[place] = jnp.where(odd, low, high)
        second[place] = jnp.where(odd, high, low)


def lay_rows(target, main, odd, one, two):
    target[0:8] = main
    target[8:10] = jnp.where(odd, two, one)
    target[14:16] = jnp.where(odd, one, two)


def halo_rows(slot, first, second):
    place = (slot // 4, slice(2 * (slot % 4), 2 * (slot % 4) + 2))
    return first[place], second[place]


def tally(pops, solid, inflow, acc, low_rows, high_rows, half_one, half_two):
    lane = lax.broadcasted_iota(jnp.int32, (8, 128), 1)
    row = lax.broadcasted_iota(jnp.int32, (8, 128), 0)
    nothing = jnp.zeros((8, 128), jnp.float32)
    blocked = [solid[y].astype(jnp.float32) for y in range(2)]
    flags = [jnp.concatenate([part, nothing], axis=0) for part in blocked]
    fluid = [1.0 - part for part in blocked]
    flow = nothing
    for y in range(PLANES):
        f = pops
        jx = (
            (f[1, y] - f[2, y])
            + (f[7, y] - f[8, y])
            + (f[9, y] - f[10, y])
            + (f[11, y] - f[12, y])
            + (f[13, y] - f[14, y])
        )
        flow = flow + (jx * fluid[y] if y < 2 else jx)
    one = flow + (inflow[INCOMING.index(9)] - inflow[INCOMING.index(8)])
    count = float(PLANES - 2) + fluid[0] + fluid[1]
    two = nothing
    weights = {}
    outer = {-1: nothing, 1: nothing}
    for y in (0, 1, 2, PLANES - 1):
        relaxed, velocity, inv = relax([pops[q, y] for q in range(Q)])
        for index in range(Q):
            cx, cy, cz = LATTICE[index]
            target = y + cy
            if not cx or 1 < target < PLANES:
                continue
            linear, square = push_parts(index, velocity, inv)
            factor = -float(cx) if target >= PLANES else -2.0 * cx
            parts = [relaxed[index] * factor, linear * factor, square * factor]
            if y < 2:
                parts = [part * fluid[y] for part in parts]
            if 0 <= target < PLANES:
                for i, part in enumerate(parts):
                    key = ((0 if cx > 0 else 6) + 3 * target + i, cz)
                    weights[key] = weights[key] + part if key in weights else part
                    if cz:
                        place = 3 * target + i
                        moved = rolled(part, place - (7 if cz > 0 else 0), cx)
                        keep = (row == place) & (lane != (0 if cx > 0 else 127))
                        outer[cz] = outer[cz] + jnp.where(keep, moved, 0.0)
                hit = rolled(flags[target], -cz, -cx)[0:8]
                hit = jnp.where(lane == (127 if cx > 0 else 0), 0.0, hit)
                parts = [part * hit for part in parts]
            one, count, two = one + parts[0], count + parts[1], two + parts[2]
    low_rows[...] = outer[-1]
    high_rows[...] = outer[1]
    totals = nothing
    for i, part in enumerate((flow, one, count, two)):
        totals = jnp.where(row == i, jnp.sum(part, axis=0, keepdims=True), totals)
    acc[...] = totals

    by_row = {-1: nothing, 0: nothing, 1: nothing}
    for (place, cz), part in weights.items():
        by_row[cz] = jnp.where(lane == place, rolled(part, 0, place - (127 if place < 6 else 0)), by_row[cz])
    table = jnp.zeros((16, 128), jnp.float32)
    for cz, part in by_row.items():
        table = table + rolled(jnp.concatenate([part, nothing], axis=0), cz, 0)
    lanes = lax.broadcasted_iota(jnp.int32, (16, 128), 1)
    for y in range(2):
        for i in range(3):
            place = 12 + 3 * y + i
            table = jnp.where(lanes == place, rolled(flags[y], 0, place), table)
            table = jnp.where(lanes == place + 6, rolled(flags[y], 0, place + 6 - 127), table)
    halves = [nothing, nothing]
    for k in range(10):
        source = k if k < 9 else 15
        spread = rolled(jnp.broadcast_to(table[source : source + 1], (8, 128)), 0, (GROUP * k) % 128)
        for half in range(2):
            start = GROUP * k - 128 * half
            if -GROUP < start < 128:
                halves[half] = jnp.where((lane >= start) & (lane < start + GROUP), spread, halves[half])
    half_one[...] = halves[0]
    half_two[...] = halves[1]


def announce(first, second, acc, low_rows, high_rows, half_one, half_two, out):
    lane = lax.broadcasted_iota(jnp.int32, (8, 128), 1)
    row = lax.broadcasted_iota(jnp.int32, (8, 128), 0)
    odd = is_odd("gz")
    one, two = first[...], second[...]
    below, above = jnp.where(odd, one, two), jnp.where(odd, two, one)
    tail = half_two[...]
    edge = []
    for flags, offset, k in ((below, 1, 9), (above, 0, 8)):
        planes = [jnp.broadcast_to(flags[2 * y + offset : 2 * y + offset + 1], (8, 128)) for y in range(2)]
        edge.append(jnp.where(row < 3, planes[0], jnp.where(row < 6, planes[1], 0.0)))
        for y in range(2):
            start = GROUP * k - 128 + 12 + 3 * y
            for begin, column in ((start, 0), (start + 6, 127)):
                value = jnp.broadcast_to(planes[y][:, column : column + 1], (8, 128))
                tail = jnp.where((lane >= begin) & (lane < begin + 3), value, tail)
    more = low_rows[...] * edge[0] + high_rows[...] * edge[1]
    inside = (row >= 1) & (row < 4)
    total = acc[...] + jnp.where(inside, rolled(more, 1, 0) + rolled(more, -2, 0), 0.0)
    total = jnp.broadcast_to(jnp.sum(total, axis=1, keepdims=True), (8, 128))
    total = jnp.sum(jnp.where(lane == SUMS_LANE - 128 + row, total, 0.0), axis=0, keepdims=True)
    tail = jnp.where((lane >= SUMS_LANE - 128) & (lane < SUMS_LANE - 124), total, tail)
    packed = jnp.concatenate([half_one[0:1], tail[0:1]], axis=1)
    out[...] = jnp.broadcast_to(packed[None], out.shape)


def within_group(place):
    return place - GROUP * lax.shift_right_logical(place * 2731, 16)


def cross(messages, out):
    table = messages[...]
    count = table.shape[0]
    place = lax.broadcasted_iota(jnp.int32, table.shape, 1)
    within = within_group(place)
    following = jnp.where(within < 18, pltpu.roll(table, count - 1, 0), pltpu.roll(table, 1, 0))
    matched = jnp.where(within < 12, table * rolled(following, 0, -12), 0.0)
    packed = jnp.sum(jnp.where(place < SUMS_LANE, matched, table), axis=0, keepdims=True)
    out[...] = jnp.broadcast_to(packed[None], out.shape)


def drives(sums, node_total):
    packed = jnp.sum(sums, axis=0)
    place = lax.broadcasted_iota(jnp.int32, packed.shape, 1)
    within = within_group(place)
    totals = []
    for i in range(4):
        keep = place == SUMS_LANE + i
        for start in range(i - 1, 12 if i else 0, 3):
            keep = keep | ((place < SUMS_LANE) & (within == start))
        totals.append(jnp.sum(jnp.where(keep, packed, 0.0), axis=1, keepdims=True))
    flow, one, count, two = totals
    first = BASE_DRIVE + DRIVE_GAIN * (TARGET_FLOW - flow / node_total)
    later = (one + count * first + two * (first * first)) / node_total
    second = BASE_DRIVE + DRIVE_GAIN * (TARGET_FLOW - later)
    return jnp.broadcast_to(first, (8, 128)), jnp.broadcast_to(second, (8, 128))


HALVES = (slice(0, 8), slice(8, 16))


def pack_columns(pops, solid, inflow, first, second, first_flags, second_flags, after, edges):
    odd = is_odd("gz")
    lane = lax.broadcasted_iota(jnp.int32, (8, 128), 1)
    row = lax.broadcasted_iota(jnp.int32, (8, 128), 0)
    values = slot_values(pops, solid, inflow)
    for tile in range(TILES):
        packed = [jnp.zeros((8, 128), jnp.float32)] * 2
        for slot in range(tile * 32, min(tile * 32 + 32, SLOTS)):
            offset = 4 * (slot % 32)
            start = 2 * (slot % 4)
            if slot in (FLAG_SLOT, FLAG_SLOT + 1):
                one, two = first_flags[...], second_flags[...]
                start = 2 * (slot - FLAG_SLOT)
            else:
                one, two = first[slot // 4], second[slot // 4]
            above, below = jnp.where(odd, two, one), jnp.where(odd, one, two)
            outer = jnp.where(row < 4, rolled(above, -start, 0), rolled(below, 6 - start, 0))
            place = ((lane + (128 - offset + 2)) & 127) < 4
            for half, value in enumerate((values[slot](), outer)):
                packed[half] = jnp.where(place, rolled(value, 0, offset), packed[half])
        edges[tile, 0:8] = packed[0]
        edges[tile, 8:16] = packed[1]


def prepare(
    pops, solid, inflow, first, second, first_flags, second_flags, after, kept, relaxed, state, flags, entry, rows
):
    odd = is_odd("gz")
    for y in range(2):
        pair = slice(2 * y, 2 * y + 2)
        lay_rows(flags.at[y], solid[y].astype(jnp.float32), odd, first_flags[pair], second_flags[pair])
    for i in range(len(INCOMING)):
        lay_rows(entry.at[i], inflow[i], odd, *halo_rows(INFLOW_SLOT + i, first, second))
    for y in range(PLANES):
        for q in range(Q):
            lay_rows(rows.at[y, q], pops[q, y], odd, *halo_rows(q * PLANES + y, first, second))
    kept[...] = rows[0:2]

    def collide(y, carry):
        for half in HALVES:
            result, velocity, inv = relax([rows[y, q, half] for q in range(Q)])
            for q in range(Q):
                relaxed[y, q, half] = result[q]
            for i, value in enumerate(velocity + (inv,)):
                state[y, i, half] = value
        return carry

    lax.fori_loop(0, PLANES, collide, 0)


def advance(
    node_total, kept, relaxed, state, flags, entry, near, far, sums,
    out_hbm, out, moved, now, moved_side, now_side, hits, hits_side, done,
):
    drive, drive_later = drives(sums[...], node_total)
    odd = is_odd("gx")
    lane = lax.broadcasted_iota(jnp.int32, (16, 128), 1)
    edges = []
    for tile in range(TILES):
        one, two = near[tile], far[tile]
        low, high = jnp.where(odd, one, two), jnp.where(odd, two, one)
        edges.append(jnp.where((lane & 3) < 2, high, low))
    for q in range(Q):
        now_side[q] = rolled(edges[q // 4], 0, -32 * (q % 4))
    wall = ((lane + 2) & 127) < 8
    flags_side = jnp.where(wall, rolled(edges[4], 0, -96), 0.0)
    stay_side = flags_side > 0.5

    def sideways(value, q, source):
        cx, _, cz = LATTICE[q]
        lane_to = 0 if cx > 0 else 127
        return lane == lane_to, rolled(value, cz, lane_to - (4 * source - (1 if cx > 0 else 0)))

    def inward(q, source):
        cx, cy, _ = LATTICE[q]
        lane_to = 4 * (source + cy) - (0 if cx > 0 else 1)
        return lane == lane_to % 128, lane_to - (127 if cx > 0 else 0)

    for q in range(Q):
        cx, cy, cz = LATTICE[q]
        for source in range(2):
            hit = rolled(flags[source], cz, cx)
            if cx:
                edge, value = sideways(flags_side, q, source)
                hit = jnp.where(edge, value, hit)
            hits[source, q] = hit
        hit = rolled(flags_side, cz, 4 * cy + cx)
        for source in range(2):
            if cx and 0 <= source + cy:
                edge, shift = inward(q, source)
                hit = jnp.where(edge, rolled(flags[source], cz, shift), hit)
        if cy > 0:
            hit = jnp.where(((lane + 2) & 127) < 4, 1.0, hit)
        hits_side[q] = hit

    def push(y, carry):
        for half in HALVES:
            velocity = tuple(state[y, i, half] for i in range(3))
            result = driven([relaxed[y, q, half] for q in range(Q)], velocity, state[y, 3, half], drive)
            for q in range(Q):
                moved[y, q, half] = result[q]
        return carry

    def collide(y, carry):
        for half in HALVES:
            result = driven(*relax([now[y, q, half] for q in range(Q)]), drive_later)
            for q in range(Q):
                moved[y, q, half] = result[q]
        return carry

    def collide_side(applied):
        for half in HALVES:
            result = driven(*relax([now_side[q, half] for q in range(Q)]), applied)
            for q in range(Q):
                moved_side[q, half] = result[q]

    def arrive(y, q, part):
        cx, cy, cz = LATTICE[q]
        source = y - cy
        if source < 0:
            arrived = moved[y, OPPOSITE[q], part]
        elif source >= PLANES:
            arrived = entry[INCOMING.index(q), part]
        else:
            arrived = rolled(moved[source, q], cz, cx)
            if cx:
                edge, value = sideways(moved_side[q], q, source)
                arrived = jnp.where(edge, value, arrived)
            arrived = arrived[part]
            if source < 2:
                arrived = jnp.where(hits[source, q, part] > 0.5, moved[y, OPPOSITE[q], part], arrived)
        if y < 2:
            before = kept if part == slice(0, 16) else now
            arrived = jnp.where(flags[y, part] > 0.5, before[y, q, part], arrived)
        return arrived

    def arrive_side(q):
        cx, cy, cz = LATTICE[q]
        arrived = rolled(moved_side[q], cz, 4 * cy + cx)
        if cx:
            for source in range(PLANES):
                if 0 <= source + cy < PLANES:
                    edge, shift = inward(q, source)
                    arrived = jnp.where(edge, rolled(moved[source, q], cz, shift), arrived)
        arrived = jnp.where(hits_side[q] > 0.5, moved_side[OPPOSITE[q]], arrived)
        if cy < 0:
            slot = (INFLOW_SLOT + INCOMING.index(q)) % 32
            value = rolled(edges[INFLOW_SLOT // 32], 0, 4 * (PLANES - 1) - 4 * slot)
            arrived = jnp.where(((lane - 26) & 127) < 4, value, arrived)
        return jnp.where(stay_side, now_side[q], arrived)

    lax.fori_loop(0, PLANES, push, 0)
    collide_side(drive)
    for y in range(PLANES):
        for q in range(Q):
            now[y, q] = arrive(y, q, slice(0, 16))
    for q in range(Q):
        now_side[q] = arrive_side(q)
    lax.fori_loop(0, PLANES, collide, 0)
    collide_side(drive_later)
    copies = []
    for y in range(PLANES):
        for q in range(Q):
            out[y, q] = arrive(y, q, slice(0, 8))
        copies.append(pltpu.make_async_copy(out.at[y], out_hbm.at[:, y], done.at[y]))
        copies[-1].start()
    for copy in copies:
        copy.wait()


def kernel_call(body, shapes, scratch, *operands, memory=pltpu.VMEM):
    return pl.pallas_call(
        body,
        in_specs=[pl.BlockSpec(memory_space=memory)] * len(operands),
        out_specs=[pl.BlockSpec(memory_space=pltpu.VMEM)] * len(shapes),
        out_shape=[pltpu.VMEM(item, jnp.float32) if isinstance(item, tuple) else item for item in shapes],
        scratch_shapes=[
            pltpu.VMEM(item, jnp.float32) if isinstance(item, tuple) else item for item in scratch
        ],
        compiler_params=pltpu.CompilerParams(vmem_limit_bytes=20 * 1024 * 1024),
    )(*operands)


def swapped(axis, first, second):
    count = lax.axis_size(axis)
    pairs = [(i, i ^ 1) for i in range(count)]
    others = [(i, (i + 1 if i % 2 else i - 1) % count) for i in range(count)]
    return lax.ppermute(first, axis, pairs), lax.ppermute(second, axis, others)


def local(populations, solid, top_inflow):
    along_x, along_z = lax.axis_size("gx"), lax.axis_size("gz")
    node_total = float(PLANES * 8 * 128 * along_x * along_z)
    fields = (populations, solid, top_inflow)
    *flags, pops, solid, top_inflow = kernel_call(
        load,
        [(8, 128)] * 2 + [pltpu.VMEM(field.shape, field.dtype) for field in fields],
        [pltpu.SemaphoreType.DMA((2 + len(PIECES),))],
        *(pltpu.with_memory_space_constraint(field, pltpu.HBM) for field in fields),
        memory=pltpu.HBM,
    )
    flags = swapped("gz", *flags)
    own = kernel_call(tally, [(8, 128)] * 5, [], pops, solid, top_inflow)
    (sums,) = kernel_call(announce, [(along_x, 1, 256)], [], *flags, *own)
    rows = kernel_call(pack_rows, [(ROW_TILES, 8, 128)] * 2, [], pops, top_inflow, sums)
    sums = lax.all_to_all(sums, "gx", 0, 0, tiled=True)
    halo = swapped("gz", *rows)
    (sums,) = kernel_call(cross, [(along_z, 1, 256)], [], sums.reshape(along_x, 256))
    block = (pops, solid, top_inflow, *halo, *flags)
    (edges,) = kernel_call(pack_columns, [(TILES, 16, 128)], [], *block, sums)
    sums = lax.all_to_all(sums, "gz", 0, 0, tiled=True)
    near, far = swapped("gx", edges, edges)
    prepared = kernel_call(
        prepare,
        [
            (2, Q, 16, 128),
            (PLANES, Q, 16, 128),
            (PLANES, 4, 16, 128),
            (2, 16, 128),
            (len(INCOMING), 16, 128),
        ],
        [(PLANES, Q, 16, 128)],
        *block,
        edges,
    )
    (advanced,) = pl.pallas_call(
        lambda *refs: advance(node_total, *refs),
        in_specs=[pl.BlockSpec(memory_space=pltpu.VMEM)] * 8,
        out_specs=[pl.BlockSpec(memory_space=pltpu.HBM)],
        out_shape=[jax.ShapeDtypeStruct((Q, PLANES, 8, 128), jnp.float32)],
        scratch_shapes=[
            pltpu.VMEM((PLANES, Q, 8, 128), jnp.float32),
            pltpu.VMEM((PLANES, Q, 16, 128), jnp.float32),
            pltpu.VMEM((PLANES, Q, 16, 128), jnp.float32),
            pltpu.VMEM((Q, 16, 128), jnp.float32),
            pltpu.VMEM((Q, 16, 128), jnp.float32),
            pltpu.VMEM((2, Q, 16, 128), jnp.float32),
            pltpu.VMEM((Q, 16, 128), jnp.float32),
            pltpu.SemaphoreType.DMA((PLANES,)),
        ],
        compiler_params=pltpu.CompilerParams(vmem_limit_bytes=20 * 1024 * 1024),
    )(*prepared, near, far, sums)
    return advanced


def solution(mesh):
    placed = (P(None, None, "gz", "gx"), P(None, "gz", "gx"), P(None, "gz", "gx"))
    return jax.shard_map(
        local, mesh=mesh, in_specs=placed, out_specs=P(None, None, "gz", "gx"), check_vma=False
    )
```

```python
import jax
import jax.numpy as jnp
from jax import lax
from jax.experimental import pallas as pl
from jax.experimental.pallas import tpu as pltpu
from jax.sharding import PartitionSpec as P


Q = 19
PLANES = 8
LATTICE = (
    (0, 0, 0),
    (1, 0, 0),
    (-1, 0, 0),
    (0, 1, 0),
    (0, -1, 0),
    (0, 0, 1),
    (0, 0, -1),
    (1, 1, 0),
    (-1, -1, 0),
    (1, -1, 0),
    (-1, 1, 0),
    (1, 0, 1),
    (-1, 0, -1),
    (1, 0, -1),
    (-1, 0, 1),
    (0, 1, 1),
    (0, -1, -1),
    (0, 1, -1),
    (0, -1, 1),
)
OPPOSITE = (0, 2, 1, 4, 3, 6, 5, 8, 7, 10, 9, 12, 11, 14, 13, 16, 15, 18, 17)
INCOMING = (4, 8, 9, 16, 18)
SECOND, THIRD, FOURTH = 1.8, 1.2, 1.1
BASE_DRIVE = 0.0001
DRIVE_GAIN = 1.0
TARGET_FLOW = 0.1

FLAG_SLOT = Q * PLANES
INFLOW_SLOT = FLAG_SLOT + 2
SLOTS = INFLOW_SLOT + len(INCOMING)
TILES = 5
ROW_TILES = 40
PIECES = ((0, 5), (5, 10), (10, 15), (15, 19))
GROUP = 24
SUMS_LANE = 10 * GROUP


def relax(f):
    along = []
    for p in (1, 3, 5):
        along.append((f[p] + f[p + 1], f[p] - f[p + 1]))
    diagonal = []
    for p in (7, 11, 15):
        a, b = f[p] + f[p + 1], f[p + 2] + f[p + 3]
        c, d = f[p] - f[p + 1], f[p + 2] - f[p + 3]
        diagonal.append((a + b, a - b, c + d, c - d))
    (xxyy, xy, xyy, xxy), (xxzz, xz, xzz, xxz), (yyzz, yz, yzz, yyz) = diagonal
    density = f[0] + (along[0][0] + along[1][0] + along[2][0]) + (xxyy + xxzz + yyzz)
    jx = along[0][1] + xyy + xzz
    jy = along[1][1] + xxy + yzz
    jz = along[2][1] + xxz + yyz
    inv = 1.0 / density
    ux, uy, uz = jx * inv, jy * inv, jz * inv
    exx, eyy, ezz = jx * ux, jy * uy, jz * uz
    third = density * (1.0 / 3.0)
    ninth = density * (1.0 / 9.0)
    xx = along[0][0] + xxyy + xxzz
    yy = along[1][0] + xxyy + yyzz
    zz = along[2][0] + xxzz + yyzz
    dxx = SECOND * (xx - third - exx)
    dyy = SECOND * (yy - third - eyy)
    dzz = SECOND * (zz - third - ezz)
    dxy = SECOND * (xy - jx * uy)
    dxz = SECOND * (xz - jx * uz)
    dyz = SECOND * (yz - jy * uz)
    x3, y3, z3 = jx * (1.0 / 3.0), jy * (1.0 / 3.0), jz * (1.0 / 3.0)
    dxyy, dxzz = THIRD * (xyy - x3), THIRD * (xzz - x3)
    dxxy, dyzz = THIRD * (xxy - y3), THIRD * (yzz - y3)
    dxxz, dyyz = THIRD * (xxz - z3), THIRD * (yyz - z3)
    half = 0.5 * (exx + eyy + ezz)
    dxxyy = FOURTH * (xxyy - ninth - (half - 0.5 * ezz) * (2.0 / 3.0) + ezz * (1.0 / 6.0))
    dxxzz = FOURTH * (xxzz - ninth - (half - 0.5 * eyy) * (2.0 / 3.0) + eyy * (1.0 / 6.0))
    dyyzz = FOURTH * (yyzz - ninth - (half - 0.5 * exx) * (2.0 / 3.0) + exx * (1.0 / 6.0))
    out = [None] * Q
    out[0] = f[0] + (dxx + dyy + dzz) - (dxxyy + dxxzz + dyyzz)
    for p, even, odd in (
        (1, dxx - dxxyy - dxxzz, dxyy + dxzz),
        (3, dyy - dxxyy - dyyzz, dxxy + dyzz),
        (5, dzz - dxxzz - dyyzz, dxxz + dyyz),
    ):
        out[p] = f[p] - 0.5 * (even - odd)
        out[p + 1] = f[p + 1] - 0.5 * (even + odd)
    for p, four, cross, first, second in (
        (7, dxxyy, dxy, dxyy, dxxy),
        (11, dxxzz, dxz, dxzz, dxxz),
        (15, dyyzz, dyz, dyzz, dyyz),
    ):
        same, other = 0.25 * (four + cross), 0.25 * (four - cross)
        total, rest = 0.25 * (first + second), 0.25 * (first - second)
        out[p] = f[p] - (same + total)
        out[p + 1] = f[p + 1] - (same - total)
        out[p + 2] = f[p + 2] - (other + rest)
        out[p + 3] = f[p + 3] - (other - rest)
    return out, (ux, uy, uz), inv


def weight(index):
    return 1.0 / 3.0 if index == 0 else (1.0 / 18.0 if index < 7 else 1.0 / 36.0)


def push_parts(index, velocity, inv):
    cx, cy, cz = LATTICE[index]
    along = 9.0 * velocity[0] - 3.0 * velocity[0] + 3.0 * cx
    if cy:
        along = along + (9.0 * cx * cy) * velocity[1]
    if cz:
        along = along + (9.0 * cx * cz) * velocity[2]
    return weight(index) * along, (3.0 * weight(index)) * inv


def driven(relaxed, velocity, inv, drive):
    ux, uy, uz = velocity
    square = drive * drive * inv
    still = -3.0 * drive * ux - 1.5 * square
    moved = still + 9.0 * drive * ux + 4.5 * square
    three = 3.0 * drive
    up, down = moved + three, moved - three
    hy, hz = 9.0 * drive * uy, 9.0 * drive * uz
    calm = still * (1.0 / 36.0)
    out = list(relaxed)
    out[0] = out[0] + still * (1.0 / 3.0)
    out[1] = out[1] + up * (1.0 / 18.0)
    out[2] = out[2] + down * (1.0 / 18.0)
    for index in (3, 4, 5, 6):
        out[index] = out[index] + (calm + calm)
    for p, side in ((7, hy), (11, hz)):
        out[p] = out[p] + (up + side) * (1.0 / 36.0)
        out[p + 1] = out[p + 1] + (down + side) * (1.0 / 36.0)
        out[p + 2] = out[p + 2] + (up - side) * (1.0 / 36.0)
        out[p + 3] = out[p + 3] + (down - side) * (1.0 / 36.0)
    for index in (15, 16, 17, 18):
        out[index] = out[index] + calm
    return out


def rolled(value, step_z, step_x):
    if step_z:
        value = pltpu.roll(value, step_z % value.shape[0], 0)
    if step_x:
        value = pltpu.roll(value, step_x % value.shape[1], 1)
    return value


def slot_values(pops, solid, inflow):
    values = [lambda q=q, y=y: pops[q, y] for q in range(Q) for y in range(PLANES)]
    values += [lambda y=y: solid[y].astype(jnp.float32) for y in range(2)]
    values += [lambda i=i: inflow[i] for i in range(len(INCOMING))]
    return values


def is_odd(axis):
    return lax.axis_index(axis) % 2 == 1


def load(pops_hbm, solid_hbm, inflow_hbm, first, second, pops, solid, inflow, done):
    copies = [(solid_hbm, solid), (inflow_hbm, inflow)]
    copies += [(pops_hbm.at[a:b], pops.at[a:b]) for a, b in PIECES]
    copies = [pltpu.make_async_copy(source, target, done.at[i]) for i, (source, target) in enumerate(copies)]
    for copy in copies:
        copy.start()
    copies[0].wait()
    odd = is_odd("gz")
    first[...] = jnp.zeros(first.shape, jnp.float32)
    second[...] = jnp.zeros(second.shape, jnp.float32)
    for y in range(2):
        tile = solid[y].astype(jnp.float32)
        low, high = tile[0:2], tile[6:8]
        first[2 * y : 2 * y + 2] = jnp.where(odd, low, high)
        second[2 * y : 2 * y + 2] = jnp.where(odd, high, low)
    for copy in copies[1:]:
        copy.wait()


def pack(pops, solid, inflow, first, second, columns):
    odd = is_odd("gz")
    lane = lax.broadcasted_iota(jnp.int32, (8, 128), 1)
    values = slot_values(pops, solid, inflow)
    for tile in range(TILES):
        packed = jnp.zeros((8, 128), jnp.float32)
        for slot in range(tile * 32, min(tile * 32 + 32, SLOTS)):
            value = values[slot]()
            if slot not in (FLAG_SLOT, FLAG_SLOT + 1):
                low, high = value[0:2], value[6:8]
                place = (slot // 4, slice(2 * (slot % 4), 2 * (slot % 4) + 2))
                first[place] = jnp.where(odd, low, high)
                second[place] = jnp.where(odd, high, low)
            packed = jnp.where(in_slot(lane, slot), rolled(value, 0, 4 * (slot % 32)), packed)
        columns[tile] = packed


def in_slot(lane, slot):
    return ((lane + (128 - 4 * (slot % 32) + 2)) & 127) < 4


def lay_rows(target, main, odd, one, two):
    target[0:8] = main
    target[8:10] = jnp.where(odd, two, one)
    target[14:16] = jnp.where(odd, one, two)


def halo_rows(slot, first, second):
    place = (slot // 4, slice(2 * (slot % 4), 2 * (slot % 4) + 2))
    return first[place], second[place]


def tally(pops, solid, inflow, acc, low_rows, high_rows, half_one, half_two):
    lane = lax.broadcasted_iota(jnp.int32, (8, 128), 1)
    row = lax.broadcasted_iota(jnp.int32, (8, 128), 0)
    nothing = jnp.zeros((8, 128), jnp.float32)
    blocked = [solid[y].astype(jnp.float32) for y in range(2)]
    flags = [jnp.concatenate([part, nothing], axis=0) for part in blocked]
    fluid = [1.0 - part for part in blocked]
    flow = nothing
    for y in range(PLANES):
        f = pops
        jx = (
            (f[1, y] - f[2, y])
            + (f[7, y] - f[8, y])
            + (f[9, y] - f[10, y])
            + (f[11, y] - f[12, y])
            + (f[13, y] - f[14, y])
        )
        flow = flow + (jx * fluid[y] if y < 2 else jx)
    one = flow + (inflow[INCOMING.index(9)] - inflow[INCOMING.index(8)])
    count = float(PLANES - 2) + fluid[0] + fluid[1]
    two = nothing
    weights = {}
    outer = {-1: nothing, 1: nothing}
    for y in (0, 1, 2, PLANES - 1):
        relaxed, velocity, inv = relax([pops[q, y] for q in range(Q)])
        for index in range(Q):
            cx, cy, cz = LATTICE[index]
            target = y + cy
            if not cx or 1 < target < PLANES:
                continue
            linear, square = push_parts(index, velocity, inv)
            factor = -float(cx) if target >= PLANES else -2.0 * cx
            parts = [relaxed[index] * factor, linear * factor, square * factor]
            if y < 2:
                parts = [part * fluid[y] for part in parts]
            if 0 <= target < PLANES:
                for i, part in enumerate(parts):
                    key = ((0 if cx > 0 else 6) + 3 * target + i, cz)
                    weights[key] = weights[key] + part if key in weights else part
                    if cz:
                        place = 3 * target + i
                        moved = rolled(part, place - (7 if cz > 0 else 0), cx)
                        keep = (row == place) & (lane != (0 if cx > 0 else 127))
                        outer[cz] = outer[cz] + jnp.where(keep, moved, 0.0)
                hit = rolled(flags[target], -cz, -cx)[0:8]
                hit = jnp.where(lane == (127 if cx > 0 else 0), 0.0, hit)
                parts = [part * hit for part in parts]
            one, count, two = one + parts[0], count + parts[1], two + parts[2]
    low_rows[...] = outer[-1]
    high_rows[...] = outer[1]
    totals = nothing
    for i, part in enumerate((flow, one, count, two)):
        totals = jnp.where(row == i, jnp.sum(part, axis=0, keepdims=True), totals)
    acc[...] = totals

    by_row = {-1: nothing, 0: nothing, 1: nothing}
    for (place, cz), part in weights.items():
        by_row[cz] = jnp.where(lane == place, rolled(part, 0, place - (127 if place < 6 else 0)), by_row[cz])
    table = jnp.zeros((16, 128), jnp.float32)
    for cz, part in by_row.items():
        table = table + rolled(jnp.concatenate([part, nothing], axis=0), cz, 0)
    lanes = lax.broadcasted_iota(jnp.int32, (16, 128), 1)
    for y in range(2):
        for i in range(3):
            place = 12 + 3 * y + i
            table = jnp.where(lanes == place, rolled(flags[y], 0, place), table)
            table = jnp.where(lanes == place + 6, rolled(flags[y], 0, place + 6 - 127), table)
    halves = [nothing, nothing]
    for k in range(10):
        source = k if k < 9 else 15
        spread = rolled(jnp.broadcast_to(table[source : source + 1], (8, 128)), 0, (GROUP * k) % 128)
        for half in range(2):
            start = GROUP * k - 128 * half
            if -GROUP < start < 128:
                halves[half] = jnp.where((lane >= start) & (lane < start + GROUP), spread, halves[half])
    half_one[...] = halves[0]
    half_two[...] = halves[1]


def announce(first, second, acc, low_rows, high_rows, half_one, half_two, out):
    lane = lax.broadcasted_iota(jnp.int32, (8, 128), 1)
    row = lax.broadcasted_iota(jnp.int32, (8, 128), 0)
    odd = is_odd("gz")
    one, two = first[...], second[...]
    below, above = jnp.where(odd, one, two), jnp.where(odd, two, one)
    tail = half_two[...]
    edge = []
    for flags, offset, k in ((below, 1, 9), (above, 0, 8)):
        planes = [jnp.broadcast_to(flags[2 * y + offset : 2 * y + offset + 1], (8, 128)) for y in range(2)]
        edge.append(jnp.where(row < 3, planes[0], jnp.where(row < 6, planes[1], 0.0)))
        for y in range(2):
            start = GROUP * k - 128 + 12 + 3 * y
            for begin, column in ((start, 0), (start + 6, 127)):
                value = jnp.broadcast_to(planes[y][:, column : column + 1], (8, 128))
                tail = jnp.where((lane >= begin) & (lane < begin + 3), value, tail)
    more = low_rows[...] * edge[0] + high_rows[...] * edge[1]
    inside = (row >= 1) & (row < 4)
    total = acc[...] + jnp.where(inside, rolled(more, 1, 0) + rolled(more, -2, 0), 0.0)
    total = jnp.broadcast_to(jnp.sum(total, axis=1, keepdims=True), (8, 128))
    total = jnp.sum(jnp.where(lane == SUMS_LANE - 128 + row, total, 0.0), axis=0, keepdims=True)
    tail = jnp.where((lane >= SUMS_LANE - 128) & (lane < SUMS_LANE - 124), total, tail)
    packed = jnp.concatenate([half_one[0:1], tail[0:1]], axis=1)
    out[...] = jnp.broadcast_to(packed[None], out.shape)


def within_group(place):
    return place - GROUP * lax.shift_right_logical(place * 2731, 16)


def cross(messages, out):
    table = messages[...]
    count = table.shape[0]
    place = lax.broadcasted_iota(jnp.int32, table.shape, 1)
    within = within_group(place)
    following = jnp.where(within < 18, pltpu.roll(table, count - 1, 0), pltpu.roll(table, 1, 0))
    matched = jnp.where(within < 12, table * rolled(following, 0, -12), 0.0)
    packed = jnp.sum(jnp.where(place < SUMS_LANE, matched, table), axis=0, keepdims=True)
    out[...] = jnp.broadcast_to(packed[None], out.shape)


def drives(sums, node_total):
    packed = jnp.sum(sums, axis=0)
    place = lax.broadcasted_iota(jnp.int32, packed.shape, 1)
    within = within_group(place)
    totals = []
    for i in range(4):
        keep = place == SUMS_LANE + i
        for start in range(i - 1, 12 if i else 0, 3):
            keep = keep | ((place < SUMS_LANE) & (within == start))
        totals.append(jnp.sum(jnp.where(keep, packed, 0.0), axis=1, keepdims=True))
    flow, one, count, two = totals
    first = BASE_DRIVE + DRIVE_GAIN * (TARGET_FLOW - flow / node_total)
    later = (one + count * first + two * (first * first)) / node_total
    second = BASE_DRIVE + DRIVE_GAIN * (TARGET_FLOW - later)
    return jnp.broadcast_to(first, (8, 128)), jnp.broadcast_to(second, (8, 128))


HALVES = (slice(0, 8), slice(8, 16))


def lay_out(pops, solid, inflow, first, second, first_flags, second_flags, columns, after, rows, flags, entry, edges):
    odd = is_odd("gz")
    lane = lax.broadcasted_iota(jnp.int32, (8, 128), 1)
    for y in range(2):
        pair = slice(2 * y, 2 * y + 2)
        lay_rows(flags.at[y], solid[y].astype(jnp.float32), odd, first_flags[pair], second_flags[pair])
    for i in range(len(INCOMING)):
        lay_rows(entry.at[i], inflow[i], odd, *halo_rows(INFLOW_SLOT + i, first, second))
    for y in range(PLANES):
        for q in range(Q):
            lay_rows(rows.at[y, q], pops[q, y], odd, *halo_rows(q * PLANES + y, first, second))
    outer = slice(8, 16)
    values = [lambda q=q, y=y: rows[y, q, outer] for q in range(Q) for y in range(PLANES)]
    values += [lambda y=y: flags[y, outer] for y in range(2)]
    values += [lambda i=i: entry[i, outer] for i in range(len(INCOMING))]
    for tile in range(TILES):
        packed = jnp.zeros((8, 128), jnp.float32)
        for slot in range(tile * 32, min(tile * 32 + 32, SLOTS)):
            packed = jnp.where(in_slot(lane, slot), rolled(values[slot](), 0, 4 * (slot % 32)), packed)
        edges[tile, 0:8] = columns[tile]
        edges[tile, outer] = packed


def prepare(rows, after, kept, relaxed, state):
    kept[...] = rows[0:2]

    def collide(y, carry):
        for half in HALVES:
            result, velocity, inv = relax([rows[y, q, half] for q in range(Q)])
            for q in range(Q):
                relaxed[y, q, half] = result[q]
            for i, value in enumerate(velocity + (inv,)):
                state[y, i, half] = value
        return carry

    lax.fori_loop(0, PLANES, collide, 0)


def advance(
    node_total, kept, relaxed, state, flags, entry, near, far, sums,
    out_hbm, out, moved, now, moved_side, now_side, hits, hits_side, done,
):
    drive, drive_later = drives(sums[...], node_total)
    odd = is_odd("gx")
    lane = lax.broadcasted_iota(jnp.int32, (16, 128), 1)
    edges = []
    for tile in range(TILES):
        one, two = near[tile], far[tile]
        low, high = jnp.where(odd, one, two), jnp.where(odd, two, one)
        edges.append(jnp.where((lane & 3) < 2, high, low))
    for q in range(Q):
        now_side[q] = rolled(edges[q // 4], 0, -32 * (q % 4))
    wall = ((lane + 2) & 127) < 8
    flags_side = jnp.where(wall, rolled(edges[4], 0, -96), 0.0)
    stay_side = flags_side > 0.5

    def sideways(value, q, source):
        cx, _, cz = LATTICE[q]
        lane_to = 0 if cx > 0 else 127
        return lane == lane_to, rolled(value, cz, lane_to - (4 * source - (1 if cx > 0 else 0)))

    def inward(q, source):
        cx, cy, _ = LATTICE[q]
        lane_to = 4 * (source + cy) - (0 if cx > 0 else 1)
        return lane == lane_to % 128, lane_to - (127 if cx > 0 else 0)

    for q in range(Q):
        cx, cy, cz = LATTICE[q]
        for source in range(2):
            hit = rolled(flags[source], cz, cx)
            if cx:
                edge, value = sideways(flags_side, q, source)
                hit = jnp.where(edge, value, hit)
            hits[source, q] = hit
        hit = rolled(flags_side, cz, 4 * cy + cx)
        for source in range(2):
            if cx and 0 <= source + cy:
                edge, shift = inward(q, source)
                hit = jnp.where(edge, rolled(flags[source], cz, shift), hit)
        if cy > 0:
            hit = jnp.where(((lane + 2) & 127) < 4, 1.0, hit)
        hits_side[q] = hit

    def push(y, carry):
        for half in HALVES:
            velocity = tuple(state[y, i, half] for i in range(3))
            result = driven([relaxed[y, q, half] for q in range(Q)], velocity, state[y, 3, half], drive)
            for q in range(Q):
                moved[y, q, half] = result[q]
        return carry

    def collide(y, carry):
        for half in HALVES:
            result = driven(*relax([now[y, q, half] for q in range(Q)]), drive_later)
            for q in range(Q):
                moved[y, q, half] = result[q]
        return carry

    def collide_side(applied):
        for half in HALVES:
            result = driven(*relax([now_side[q, half] for q in range(Q)]), applied)
            for q in range(Q):
                moved_side[q, half] = result[q]

    def arrive(y, q, part):
        cx, cy, cz = LATTICE[q]
        source = y - cy
        if source < 0:
            arrived = moved[y, OPPOSITE[q], part]
        elif source >= PLANES:
            arrived = entry[INCOMING.index(q), part]
        else:
            arrived = rolled(moved[source, q], cz, cx)
            if cx:
                edge, value = sideways(moved_side[q], q, source)
                arrived = jnp.where(edge, value, arrived)
            arrived = arrived[part]
            if source < 2:
                arrived = jnp.where(hits[source, q, part] > 0.5, moved[y, OPPOSITE[q], part], arrived)
        if y < 2:
            before = kept if part == slice(0, 16) else now
            arrived = jnp.where(flags[y, part] > 0.5, before[y, q, part], arrived)
        return arrived

    def arrive_side(q):
        cx, cy, cz = LATTICE[q]
        arrived = rolled(moved_side[q], cz, 4 * cy + cx)
        if cx:
            for source in range(PLANES):
                if 0 <= source + cy < PLANES:
                    edge, shift = inward(q, source)
                    arrived = jnp.where(edge, rolled(moved[source, q], cz, shift), arrived)
        arrived = jnp.where(hits_side[q] > 0.5, moved_side[OPPOSITE[q]], arrived)
        if cy < 0:
            slot = (INFLOW_SLOT + INCOMING.index(q)) % 32
            value = rolled(edges[INFLOW_SLOT // 32], 0, 4 * (PLANES - 1) - 4 * slot)
            arrived = jnp.where(((lane - 26) & 127) < 4, value, arrived)
        return jnp.where(stay_side, now_side[q], arrived)

    lax.fori_loop(0, PLANES, push, 0)
    collide_side(drive)
    for y in range(PLANES):
        for q in range(Q):
            now[y, q] = arrive(y, q, slice(0, 16))
    for q in range(Q):
        now_side[q] = arrive_side(q)
    lax.fori_loop(0, PLANES, collide, 0)
    collide_side(drive_later)
    copies = []
    for y in range(PLANES):
        for q in range(Q):
            out[y, q] = arrive(y, q, slice(0, 8))
        copies.append(pltpu.make_async_copy(out.at[y], out_hbm.at[:, y], done.at[y]))
        copies[-1].start()
    for copy in copies:
        copy.wait()


def kernel_call(body, shapes, scratch, *operands, memory=pltpu.VMEM, after=()):
    return pl.pallas_call(
        body,
        in_specs=[pl.BlockSpec(memory_space=memory)] * len(operands) + [pl.BlockSpec(memory_space=pl.ANY)] * len(after),
        out_specs=[pl.BlockSpec(memory_space=pltpu.VMEM)] * len(shapes),
        out_shape=[pltpu.VMEM(item, jnp.float32) if isinstance(item, tuple) else item for item in shapes],
        scratch_shapes=[
            pltpu.VMEM(item, jnp.float32) if isinstance(item, tuple) else item for item in scratch
        ],
        compiler_params=pltpu.CompilerParams(vmem_limit_bytes=20 * 1024 * 1024),
    )(*operands, *after)


def swapped(axis, first, second):
    count = lax.axis_size(axis)
    pairs = [(i, i ^ 1) for i in range(count)]
    others = [(i, (i + 1 if i % 2 else i - 1) % count) for i in range(count)]
    return lax.ppermute(first, axis, pairs), lax.ppermute(second, axis, others)


def local(populations, solid, top_inflow):
    along_x, along_z = lax.axis_size("gx"), lax.axis_size("gz")
    node_total = float(PLANES * 8 * 128 * along_x * along_z)
    fields = (populations, solid, top_inflow)
    *flags, pops, solid, top_inflow = kernel_call(
        load,
        [(8, 128)] * 2 + [pltpu.VMEM(field.shape, field.dtype) for field in fields],
        [pltpu.SemaphoreType.DMA((2 + len(PIECES),))],
        *(pltpu.with_memory_space_constraint(field, pltpu.HBM) for field in fields),
        memory=pltpu.HBM,
    )
    block = (pops, solid, top_inflow)
    flags = swapped("gz", *flags)
    *rows, columns = kernel_call(pack, [(ROW_TILES, 8, 128)] * 2 + [(TILES, 8, 128)], [], *block)
    own = kernel_call(tally, [(8, 128)] * 5, [], *block)
    (sums,) = kernel_call(announce, [(along_x, 1, 256)], [], *flags, *own)
    sums = lax.all_to_all(sums, "gx", 0, 0, tiled=True)
    halo = swapped("gz", *rows)
    (sums,) = kernel_call(cross, [(along_z, 1, 256)], [], sums.reshape(along_x, 256))
    laid, flags, entry, edges = kernel_call(
        lay_out,
        [(PLANES, Q, 16, 128), (2, 16, 128), (len(INCOMING), 16, 128), (TILES, 16, 128)],
        [],
        *block,
        *halo,
        *flags,
        columns,
        after=(sums,),
    )
    sums = lax.all_to_all(sums, "gz", 0, 0, tiled=True)
    near, far = swapped("gx", edges, edges)
    prepared = kernel_call(
        prepare,
        [(2, Q, 16, 128), (PLANES, Q, 16, 128), (PLANES, 4, 16, 128)],
        [],
        laid,
        after=(edges,),
    )
    prepared = (*prepared, flags, entry)
    (advanced,) = pl.pallas_call(
        lambda *refs: advance(node_total, *refs),
        in_specs=[pl.BlockSpec(memory_space=pltpu.VMEM)] * 8,
        out_specs=[pl.BlockSpec(memory_space=pltpu.HBM)],
        out_shape=[jax.ShapeDtypeStruct((Q, PLANES, 8, 128), jnp.float32)],
        scratch_shapes=[
            pltpu.VMEM((PLANES, Q, 8, 128), jnp.float32),
            pltpu.VMEM((PLANES, Q, 16, 128), jnp.float32),
            pltpu.VMEM((PLANES, Q, 16, 128), jnp.float32),
            pltpu.VMEM((Q, 16, 128), jnp.float32),
            pltpu.VMEM((Q, 16, 128), jnp.float32),
            pltpu.VMEM((2, Q, 16, 128), jnp.float32),
            pltpu.VMEM((Q, 16, 128), jnp.float32),
            pltpu.SemaphoreType.DMA((PLANES,)),
        ],
        compiler_params=pltpu.CompilerParams(vmem_limit_bytes=20 * 1024 * 1024),
    )(*prepared, near, far, sums)
    return advanced


def solution(mesh):
    placed = (P(None, None, "gz", "gx"), P(None, "gz", "gx"), P(None, "gz", "gx"))
    return jax.shard_map(
        local, mesh=mesh, in_specs=placed, out_specs=P(None, None, "gz", "gx"), check_vma=False
    )
```

```python
import jax
import jax.numpy as jnp
from jax import lax
from jax.experimental import pallas as pl
from jax.experimental.pallas import tpu as pltpu
from jax.sharding import PartitionSpec as P


Q = 19
PLANES = 8
LATTICE = (
    (0, 0, 0),
    (1, 0, 0),
    (-1, 0, 0),
    (0, 1, 0),
    (0, -1, 0),
    (0, 0, 1),
    (0, 0, -1),
    (1, 1, 0),
    (-1, -1, 0),
    (1, -1, 0),
    (-1, 1, 0),
    (1, 0, 1),
    (-1, 0, -1),
    (1, 0, -1),
    (-1, 0, 1),
    (0, 1, 1),
    (0, -1, -1),
    (0, 1, -1),
    (0, -1, 1),
)
OPPOSITE = (0, 2, 1, 4, 3, 6, 5, 8, 7, 10, 9, 12, 11, 14, 13, 16, 15, 18, 17)
INCOMING = (4, 8, 9, 16, 18)
SECOND, THIRD, FOURTH = 1.8, 1.2, 1.1
BASE_DRIVE = 0.0001
DRIVE_GAIN = 1.0
TARGET_FLOW = 0.1

FLAG_SLOT = Q * PLANES
INFLOW_SLOT = FLAG_SLOT + 2
SLOTS = INFLOW_SLOT + len(INCOMING)
TILES = 5
ROW_TILES = 40
PIECES = ((0, 5), (5, 10), (10, 15), (15, 19))
GROUP = 24
SUMS_LANE = 10 * GROUP


def relax(f):
    along = []
    for p in (1, 3, 5):
        along.append((f[p] + f[p + 1], f[p] - f[p + 1]))
    diagonal = []
    for p in (7, 11, 15):
        a, b = f[p] + f[p + 1], f[p + 2] + f[p + 3]
        c, d = f[p] - f[p + 1], f[p + 2] - f[p + 3]
        diagonal.append((a + b, a - b, c + d, c - d))
    (xxyy, xy, xyy, xxy), (xxzz, xz, xzz, xxz), (yyzz, yz, yzz, yyz) = diagonal
    density = f[0] + (along[0][0] + along[1][0] + along[2][0]) + (xxyy + xxzz + yyzz)
    jx = along[0][1] + xyy + xzz
    jy = along[1][1] + xxy + yzz
    jz = along[2][1] + xxz + yyz
    inv = 1.0 / density
    ux, uy, uz = jx * inv, jy * inv, jz * inv
    exx, eyy, ezz = jx * ux, jy * uy, jz * uz
    third = density * (1.0 / 3.0)
    ninth = density * (1.0 / 9.0)
    xx = along[0][0] + xxyy + xxzz
    yy = along[1][0] + xxyy + yyzz
    zz = along[2][0] + xxzz + yyzz
    dxx = SECOND * (xx - third - exx)
    dyy = SECOND * (yy - third - eyy)
    dzz = SECOND * (zz - third - ezz)
    dxy = SECOND * (xy - jx * uy)
    dxz = SECOND * (xz - jx * uz)
    dyz = SECOND * (yz - jy * uz)
    x3, y3, z3 = jx * (1.0 / 3.0), jy * (1.0 / 3.0), jz * (1.0 / 3.0)
    dxyy, dxzz = THIRD * (xyy - x3), THIRD * (xzz - x3)
    dxxy, dyzz = THIRD * (xxy - y3), THIRD * (yzz - y3)
    dxxz, dyyz = THIRD * (xxz - z3), THIRD * (yyz - z3)
    half = 0.5 * (exx + eyy + ezz)
    dxxyy = FOURTH * (xxyy - ninth - (half - 0.5 * ezz) * (2.0 / 3.0) + ezz * (1.0 / 6.0))
    dxxzz = FOURTH * (xxzz - ninth - (half - 0.5 * eyy) * (2.0 / 3.0) + eyy * (1.0 / 6.0))
    dyyzz = FOURTH * (yyzz - ninth - (half - 0.5 * exx) * (2.0 / 3.0) + exx * (1.0 / 6.0))
    out = [None] * Q
    out[0] = f[0] + (dxx + dyy + dzz) - (dxxyy + dxxzz + dyyzz)
    for p, even, odd in (
        (1, dxx - dxxyy - dxxzz, dxyy + dxzz),
        (3, dyy - dxxyy - dyyzz, dxxy + dyzz),
        (5, dzz - dxxzz - dyyzz, dxxz + dyyz),
    ):
        out[p] = f[p] - 0.5 * (even - odd)
        out[p + 1] = f[p + 1] - 0.5 * (even + odd)
    for p, four, cross, first, second in (
        (7, dxxyy, dxy, dxyy, dxxy),
        (11, dxxzz, dxz, dxzz, dxxz),
        (15, dyyzz, dyz, dyzz, dyyz),
    ):
        same, other = 0.25 * (four + cross), 0.25 * (four - cross)
        total, rest = 0.25 * (first + second), 0.25 * (first - second)
        out[p] = f[p] - (same + total)
        out[p + 1] = f[p + 1] - (same - total)
        out[p + 2] = f[p + 2] - (other + rest)
        out[p + 3] = f[p + 3] - (other - rest)
    return out, (ux, uy, uz), inv


def weight(index):
    return 1.0 / 3.0 if index == 0 else (1.0 / 18.0 if index < 7 else 1.0 / 36.0)


def push_parts(index, velocity, inv):
    cx, cy, cz = LATTICE[index]
    along = 9.0 * velocity[0] - 3.0 * velocity[0] + 3.0 * cx
    if cy:
        along = along + (9.0 * cx * cy) * velocity[1]
    if cz:
        along = along + (9.0 * cx * cz) * velocity[2]
    return weight(index) * along, (3.0 * weight(index)) * inv


def driven(relaxed, velocity, inv, drive):
    ux, uy, uz = velocity
    square = drive * drive * inv
    still = -3.0 * drive * ux - 1.5 * square
    moved = still + 9.0 * drive * ux + 4.5 * square
    three = 3.0 * drive
    up, down = moved + three, moved - three
    hy, hz = 9.0 * drive * uy, 9.0 * drive * uz
    calm = still * (1.0 / 36.0)
    out = list(relaxed)
    out[0] = out[0] + still * (1.0 / 3.0)
    out[1] = out[1] + up * (1.0 / 18.0)
    out[2] = out[2] + down * (1.0 / 18.0)
    for index in (3, 4, 5, 6):
        out[index] = out[index] + (calm + calm)
    for p, side in ((7, hy), (11, hz)):
        out[p] = out[p] + (up + side) * (1.0 / 36.0)
        out[p + 1] = out[p + 1] + (down + side) * (1.0 / 36.0)
        out[p + 2] = out[p + 2] + (up - side) * (1.0 / 36.0)
        out[p + 3] = out[p + 3] + (down - side) * (1.0 / 36.0)
    for index in (15, 16, 17, 18):
        out[index] = out[index] + calm
    return out


def rolled(value, step_z, step_x):
    if step_z:
        value = pltpu.roll(value, step_z % value.shape[0], 0)
    if step_x:
        value = pltpu.roll(value, step_x % value.shape[1], 1)
    return value


def slot_values(pops, solid, inflow):
    values = [lambda q=q, y=y: pops[q, y] for q in range(Q) for y in range(PLANES)]
    values += [lambda y=y: solid[y].astype(jnp.float32) for y in range(2)]
    values += [lambda i=i: inflow[i] for i in range(len(INCOMING))]
    return values


def is_odd(axis):
    return lax.axis_index(axis) % 2 == 1


def load(pops_hbm, solid_hbm, inflow_hbm, first, second, pops, solid, inflow, done):
    copies = [(solid_hbm, solid), (inflow_hbm, inflow)]
    copies += [(pops_hbm.at[a:b], pops.at[a:b]) for a, b in PIECES]
    copies = [pltpu.make_async_copy(source, target, done.at[i]) for i, (source, target) in enumerate(copies)]
    for copy in copies:
        copy.start()
    copies[0].wait()
    odd = is_odd("gz")
    first[...] = jnp.zeros(first.shape, jnp.float32)
    second[...] = jnp.zeros(second.shape, jnp.float32)
    for y in range(2):
        tile = solid[y].astype(jnp.float32)
        low, high = tile[0:2], tile[6:8]
        first[2 * y : 2 * y + 2] = jnp.where(odd, low, high)
        second[2 * y : 2 * y + 2] = jnp.where(odd, high, low)
    for copy in copies[1:]:
        copy.wait()


def pack(pops, solid, inflow, first, second, columns):
    odd = is_odd("gz")
    lane = lax.broadcasted_iota(jnp.int32, (8, 128), 1)
    values = slot_values(pops, solid, inflow)
    for tile in range(TILES):
        packed = jnp.zeros((8, 128), jnp.float32)
        for slot in range(tile * 32, min(tile * 32 + 32, SLOTS)):
            value = values[slot]()
            if slot not in (FLAG_SLOT, FLAG_SLOT + 1):
                low, high = value[0:2], value[6:8]
                place = (slot // 4, slice(2 * (slot % 4), 2 * (slot % 4) + 2))
                first[place] = jnp.where(odd, low, high)
                second[place] = jnp.where(odd, high, low)
            packed = jnp.where(in_slot(lane, slot), rolled(value, 0, 4 * (slot % 32)), packed)
        columns[tile] = packed


def in_slot(lane, slot):
    return ((lane + (128 - 4 * (slot % 32) + 2)) & 127) < 4


def lay_rows(target, main, odd, one, two):
    target[0:8] = main
    target[8:10] = jnp.where(odd, two, one)
    target[14:16] = jnp.where(odd, one, two)


def halo_rows(slot, first, second):
    place = (slot // 4, slice(2 * (slot % 4), 2 * (slot % 4) + 2))
    return first[place], second[place]


def tally(pops, solid, inflow, acc, low_rows, high_rows, half_one, half_two):
    lane = lax.broadcasted_iota(jnp.int32, (8, 128), 1)
    row = lax.broadcasted_iota(jnp.int32, (8, 128), 0)
    nothing = jnp.zeros((8, 128), jnp.float32)
    blocked = [solid[y].astype(jnp.float32) for y in range(2)]
    flags = [jnp.concatenate([part, nothing], axis=0) for part in blocked]
    fluid = [1.0 - part for part in blocked]
    flow = nothing
    for y in range(PLANES):
        f = pops
        jx = (
            (f[1, y] - f[2, y])
            + (f[7, y] - f[8, y])
            + (f[9, y] - f[10, y])
            + (f[11, y] - f[12, y])
            + (f[13, y] - f[14, y])
        )
        flow = flow + (jx * fluid[y] if y < 2 else jx)
    one = flow + (inflow[INCOMING.index(9)] - inflow[INCOMING.index(8)])
    count = float(PLANES - 2) + fluid[0] + fluid[1]
    two = nothing
    weights = {}
    outer = {-1: nothing, 1: nothing}
    for y in (0, 1, 2, PLANES - 1):
        relaxed, velocity, inv = relax([pops[q, y] for q in range(Q)])
        for index in range(Q):
            cx, cy, cz = LATTICE[index]
            target = y + cy
            if not cx or 1 < target < PLANES:
                continue
            linear, square = push_parts(index, velocity, inv)
            factor = -float(cx) if target >= PLANES else -2.0 * cx
            parts = [relaxed[index] * factor, linear * factor, square * factor]
            if y < 2:
                parts = [part * fluid[y] for part in parts]
            if 0 <= target < PLANES:
                for i, part in enumerate(parts):
                    key = ((0 if cx > 0 else 6) + 3 * target + i, cz)
                    weights[key] = weights[key] + part if key in weights else part
                    if cz:
                        place = 3 * target + i
                        moved = rolled(part, place - (7 if cz > 0 else 0), cx)
                        keep = (row == place) & (lane != (0 if cx > 0 else 127))
                        outer[cz] = outer[cz] + jnp.where(keep, moved, 0.0)
                hit = rolled(flags[target], -cz, -cx)[0:8]
                hit = jnp.where(lane == (127 if cx > 0 else 0), 0.0, hit)
                parts = [part * hit for part in parts]
            one, count, two = one + parts[0], count + parts[1], two + parts[2]
    low_rows[...] = outer[-1]
    high_rows[...] = outer[1]
    totals = nothing
    for i, part in enumerate((flow, one, count, two)):
        totals = jnp.where(row == i, jnp.sum(part, axis=0, keepdims=True), totals)
    acc[...] = totals

    by_row = {-1: nothing, 0: nothing, 1: nothing}
    for (place, cz), part in weights.items():
        by_row[cz] = jnp.where(lane == place, rolled(part, 0, place - (127 if place < 6 else 0)), by_row[cz])
    table = jnp.zeros((16, 128), jnp.float32)
    for cz, part in by_row.items():
        table = table + rolled(jnp.concatenate([part, nothing], axis=0), cz, 0)
    lanes = lax.broadcasted_iota(jnp.int32, (16, 128), 1)
    for y in range(2):
        for i in range(3):
            place = 12 + 3 * y + i
            table = jnp.where(lanes == place, rolled(flags[y], 0, place), table)
            table = jnp.where(lanes == place + 6, rolled(flags[y], 0, place + 6 - 127), table)
    halves = [nothing, nothing]
    for k in range(10):
        source = k if k < 9 else 15
        spread = rolled(jnp.broadcast_to(table[source : source + 1], (8, 128)), 0, (GROUP * k) % 128)
        for half in range(2):
            start = GROUP * k - 128 * half
            if -GROUP < start < 128:
                halves[half] = jnp.where((lane >= start) & (lane < start + GROUP), spread, halves[half])
    half_one[...] = halves[0]
    half_two[...] = halves[1]


def announce(first, second, acc, low_rows, high_rows, half_one, half_two, out):
    lane = lax.broadcasted_iota(jnp.int32, (8, 128), 1)
    row = lax.broadcasted_iota(jnp.int32, (8, 128), 0)
    odd = is_odd("gz")
    one, two = first[...], second[...]
    below, above = jnp.where(odd, one, two), jnp.where(odd, two, one)
    tail = half_two[...]
    edge = []
    for flags, offset, k in ((below, 1, 9), (above, 0, 8)):
        planes = [jnp.broadcast_to(flags[2 * y + offset : 2 * y + offset + 1], (8, 128)) for y in range(2)]
        edge.append(jnp.where(row < 3, planes[0], jnp.where(row < 6, planes[1], 0.0)))
        for y in range(2):
            start = GROUP * k - 128 + 12 + 3 * y
            for begin, column in ((start, 0), (start + 6, 127)):
                value = jnp.broadcast_to(planes[y][:, column : column + 1], (8, 128))
                tail = jnp.where((lane >= begin) & (lane < begin + 3), value, tail)
    more = low_rows[...] * edge[0] + high_rows[...] * edge[1]
    inside = (row >= 1) & (row < 4)
    total = acc[...] + jnp.where(inside, rolled(more, 1, 0) + rolled(more, -2, 0), 0.0)
    total = jnp.broadcast_to(jnp.sum(total, axis=1, keepdims=True), (8, 128))
    total = jnp.sum(jnp.where(lane == SUMS_LANE - 128 + row, total, 0.0), axis=0, keepdims=True)
    tail = jnp.where((lane >= SUMS_LANE - 128) & (lane < SUMS_LANE - 124), total, tail)
    packed = jnp.concatenate([half_one[0:1], tail[0:1]], axis=1)
    out[...] = jnp.broadcast_to(packed[None], out.shape)


def within_group(place):
    return place - GROUP * lax.shift_right_logical(place * 2731, 16)


def cross(messages, out):
    table = messages[...]
    count = table.shape[0]
    place = lax.broadcasted_iota(jnp.int32, table.shape, 1)
    within = within_group(place)
    following = jnp.where(within < 18, pltpu.roll(table, count - 1, 0), pltpu.roll(table, 1, 0))
    matched = jnp.where(within < 12, table * rolled(following, 0, -12), 0.0)
    packed = jnp.sum(jnp.where(place < SUMS_LANE, matched, table), axis=0, keepdims=True)
    out[...] = jnp.broadcast_to(packed[None], out.shape)


def drives(sums, node_total):
    packed = jnp.sum(sums, axis=0)
    place = lax.broadcasted_iota(jnp.int32, packed.shape, 1)
    within = within_group(place)
    totals = []
    for i in range(4):
        keep = place == SUMS_LANE + i
        for start in range(i - 1, 12 if i else 0, 3):
            keep = keep | ((place < SUMS_LANE) & (within == start))
        totals.append(jnp.sum(jnp.where(keep, packed, 0.0), axis=1, keepdims=True))
    flow, one, count, two = totals
    first = BASE_DRIVE + DRIVE_GAIN * (TARGET_FLOW - flow / node_total)
    later = (one + count * first + two * (first * first)) / node_total
    second = BASE_DRIVE + DRIVE_GAIN * (TARGET_FLOW - later)
    return jnp.broadcast_to(first, (8, 128)), jnp.broadcast_to(second, (8, 128))


HALVES = (slice(0, 8), slice(8, 16))


def lay_out(pops, solid, inflow, first, second, first_flags, second_flags, columns, after, rows, flags, entry, edges):
    odd = is_odd("gz")
    lane = lax.broadcasted_iota(jnp.int32, (8, 128), 1)
    for y in range(2):
        pair = slice(2 * y, 2 * y + 2)
        lay_rows(flags.at[y], solid[y].astype(jnp.float32), odd, first_flags[pair], second_flags[pair])
    for i in range(len(INCOMING)):
        lay_rows(entry.at[i], inflow[i], odd, *halo_rows(INFLOW_SLOT + i, first, second))
    for y in range(PLANES):
        for q in range(Q):
            lay_rows(rows.at[y, q], pops[q, y], odd, *halo_rows(q * PLANES + y, first, second))
    outer = slice(8, 16)
    values = [lambda q=q, y=y: rows[y, q, outer] for q in range(Q) for y in range(PLANES)]
    values += [lambda y=y: flags[y, outer] for y in range(2)]
    values += [lambda i=i: entry[i, outer] for i in range(len(INCOMING))]
    for tile in range(TILES):
        packed = jnp.zeros((8, 128), jnp.float32)
        for slot in range(tile * 32, min(tile * 32 + 32, SLOTS)):
            packed = jnp.where(in_slot(lane, slot), rolled(values[slot](), 0, 4 * (slot % 32)), packed)
        edges[tile, 0:8] = columns[tile]
        edges[tile, outer] = packed


def prepare(rows, after, kept, relaxed, state):
    kept[...] = rows[0:2]

    def collide(y, carry):
        for half in HALVES:
            result, velocity, inv = relax([rows[y, q, half] for q in range(Q)])
            for q in range(Q):
                relaxed[y, q, half] = result[q]
            for i, value in enumerate(velocity + (inv,)):
                state[y, i, half] = value
        return carry

    lax.fori_loop(0, PLANES, collide, 0)


def sideways(value, q, source):
    cx, _, cz = LATTICE[q]
    lane = lax.broadcasted_iota(jnp.int32, (16, 128), 1)
    lane_to = 0 if cx > 0 else 127
    return lane == lane_to, rolled(value, cz, lane_to - (4 * source - (1 if cx > 0 else 0)))


def inward(q, source):
    cx, cy, _ = LATTICE[q]
    lane = lax.broadcasted_iota(jnp.int32, (16, 128), 1)
    lane_to = 4 * (source + cy) - (0 if cx > 0 else 1)
    return lane == lane_to % 128, lane_to - (127 if cx > 0 else 0)


def lay_side(flags, near, far, hits, hits_side, flags_side_out, now_side, entry_side, relaxed_side, state_side):
    odd = is_odd("gx")
    lane = lax.broadcasted_iota(jnp.int32, (16, 128), 1)
    edges = []
    for tile in range(TILES):
        one, two = near[tile], far[tile]
        low, high = jnp.where(odd, one, two), jnp.where(odd, two, one)
        edges.append(jnp.where((lane & 3) < 2, high, low))
    for q in range(Q):
        now_side[q] = rolled(edges[q // 4], 0, -32 * (q % 4))
    for i in range(len(INCOMING)):
        slot = (INFLOW_SLOT + i) % 32
        entry_side[i] = rolled(edges[INFLOW_SLOT // 32], 0, 4 * (PLANES - 1) - 4 * slot)
    flags_side = jnp.where(((lane + 2) & 127) < 8, rolled(edges[4], 0, -96), 0.0)
    flags_side_out[...] = flags_side
    for q in range(Q):
        cx, cy, cz = LATTICE[q]
        for source in range(2):
            hit = rolled(flags[source], cz, cx)
            if cx:
                edge, value = sideways(flags_side, q, source)
                hit = jnp.where(edge, value, hit)
            hits[source, q] = hit
        hit = rolled(flags_side, cz, 4 * cy + cx)
        for source in range(2):
            if cx and 0 <= source + cy:
                edge, shift = inward(q, source)
                hit = jnp.where(edge, rolled(flags[source], cz, shift), hit)
        if cy > 0:
            hit = jnp.where(((lane + 2) & 127) < 4, 1.0, hit)
        hits_side[q] = hit
    for half in HALVES:
        result, velocity, inv = relax([now_side[q, half] for q in range(Q)])
        for q in range(Q):
            relaxed_side[q, half] = result[q]
        for i, value in enumerate(velocity + (inv,)):
            state_side[i, half] = value


def advance(
    node_total, kept, relaxed, state, flags, entry, hits, hits_side, flags_side, first_side, entry_side,
    relaxed_side, state_side, sums, out_hbm, out, moved, now, moved_side, now_side, done,
):
    drive, drive_later = drives(sums[...], node_total)
    lane = lax.broadcasted_iota(jnp.int32, (16, 128), 1)

    def push(y, carry):
        for half in HALVES:
            velocity = tuple(state[y, i, half] for i in range(3))
            result = driven([relaxed[y, q, half] for q in range(Q)], velocity, state[y, 3, half], drive)
            for q in range(Q):
                moved[y, q, half] = result[q]
        return carry

    def collide(y, carry):
        for half in HALVES:
            result = driven(*relax([now[y, q, half] for q in range(Q)]), drive_later)
            for q in range(Q):
                moved[y, q, half] = result[q]
        return carry

    def push_side():
        for half in HALVES:
            velocity = tuple(state_side[i, half] for i in range(3))
            result = driven([relaxed_side[q, half] for q in range(Q)], velocity, state_side[3, half], drive)
            for q in range(Q):
                moved_side[q, half] = result[q]

    def collide_side():
        for half in HALVES:
            result = driven(*relax([now_side[q, half] for q in range(Q)]), drive_later)
            for q in range(Q):
                moved_side[q, half] = result[q]

    def arrive(y, q, part):
        cx, cy, cz = LATTICE[q]
        source = y - cy
        if source < 0:
            arrived = moved[y, OPPOSITE[q], part]
        elif source >= PLANES:
            arrived = entry[INCOMING.index(q), part]
        else:
            arrived = rolled(moved[source, q], cz, cx)
            if cx:
                edge, value = sideways(moved_side[q], q, source)
                arrived = jnp.where(edge, value, arrived)
            arrived = arrived[part]
            if source < 2:
                arrived = jnp.where(hits[source, q, part] > 0.5, moved[y, OPPOSITE[q], part], arrived)
        if y < 2:
            before = kept if part == slice(0, 16) else now
            arrived = jnp.where(flags[y, part] > 0.5, before[y, q, part], arrived)
        return arrived

    def arrive_side(q):
        cx, cy, cz = LATTICE[q]
        arrived = rolled(moved_side[q], cz, 4 * cy + cx)
        if cx:
            for source in range(PLANES):
                if 0 <= source + cy < PLANES:
                    edge, shift = inward(q, source)
                    arrived = jnp.where(edge, rolled(moved[source, q], cz, shift), arrived)
        arrived = jnp.where(hits_side[q] > 0.5, moved_side[OPPOSITE[q]], arrived)
        if cy < 0:
            arrived = jnp.where(((lane - 26) & 127) < 4, entry_side[INCOMING.index(q)], arrived)
        return jnp.where(flags_side[...] > 0.5, first_side[q], arrived)

    lax.fori_loop(0, PLANES, push, 0)
    push_side()
    for y in range(PLANES):
        for q in range(Q):
            now[y, q] = arrive(y, q, slice(0, 16))
    for q in range(Q):
        now_side[q] = arrive_side(q)
    lax.fori_loop(0, PLANES, collide, 0)
    collide_side()
    copies = []
    for y in range(PLANES):
        for q in range(Q):
            out[y, q] = arrive(y, q, slice(0, 8))
        copies.append(pltpu.make_async_copy(out.at[y], out_hbm.at[:, y], done.at[y]))
        copies[-1].start()
    for copy in copies:
        copy.wait()


def kernel_call(body, shapes, scratch, *operands, memory=pltpu.VMEM, after=()):
    return pl.pallas_call(
        body,
        in_specs=[pl.BlockSpec(memory_space=memory)] * len(operands) + [pl.BlockSpec(memory_space=pl.ANY)] * len(after),
        out_specs=[pl.BlockSpec(memory_space=pltpu.VMEM)] * len(shapes),
        out_shape=[pltpu.VMEM(item, jnp.float32) if isinstance(item, tuple) else item for item in shapes],
        scratch_shapes=[
            pltpu.VMEM(item, jnp.float32) if isinstance(item, tuple) else item for item in scratch
        ],
        compiler_params=pltpu.CompilerParams(vmem_limit_bytes=20 * 1024 * 1024),
    )(*operands, *after)


def swapped(axis, first, second):
    count = lax.axis_size(axis)
    pairs = [(i, i ^ 1) for i in range(count)]
    others = [(i, (i + 1 if i % 2 else i - 1) % count) for i in range(count)]
    return lax.ppermute(first, axis, pairs), lax.ppermute(second, axis, others)


def local(populations, solid, top_inflow):
    along_x, along_z = lax.axis_size("gx"), lax.axis_size("gz")
    node_total = float(PLANES * 8 * 128 * along_x * along_z)
    fields = (populations, solid, top_inflow)
    *flags, pops, solid, top_inflow = kernel_call(
        load,
        [(8, 128)] * 2 + [pltpu.VMEM(field.shape, field.dtype) for field in fields],
        [pltpu.SemaphoreType.DMA((2 + len(PIECES),))],
        *(pltpu.with_memory_space_constraint(field, pltpu.HBM) for field in fields),
        memory=pltpu.HBM,
    )
    block = (pops, solid, top_inflow)
    flags = swapped("gz", *flags)
    *rows, columns = kernel_call(pack, [(ROW_TILES, 8, 128)] * 2 + [(TILES, 8, 128)], [], *block)
    own = kernel_call(tally, [(8, 128)] * 5, [], *block)
    (sums,) = kernel_call(announce, [(along_x, 1, 256)], [], *flags, *own)
    sums = lax.all_to_all(sums, "gx", 0, 0, tiled=True)
    halo = swapped("gz", *rows)
    (sums,) = kernel_call(cross, [(along_z, 1, 256)], [], sums.reshape(along_x, 256))
    laid, flags, entry, edges = kernel_call(
        lay_out,
        [(PLANES, Q, 16, 128), (2, 16, 128), (len(INCOMING), 16, 128), (TILES, 16, 128)],
        [],
        *block,
        *halo,
        *flags,
        columns,
        after=(sums,),
    )
    sums = lax.all_to_all(sums, "gz", 0, 0, tiled=True)
    near, far = swapped("gx", edges, edges)
    prepared = kernel_call(
        prepare,
        [(2, Q, 16, 128), (PLANES, Q, 16, 128), (PLANES, 4, 16, 128)],
        [],
        laid,
        after=(edges,),
    )
    tile = (16, 128)
    side = kernel_call(
        lay_side,
        [(2, Q) + tile, (Q,) + tile, tile, (Q,) + tile, (len(INCOMING),) + tile, (Q,) + tile, (4,) + tile],
        [],
        flags,
        near,
        far,
    )
    operands = (*prepared, flags, entry, *side, sums)
    (advanced,) = pl.pallas_call(
        lambda *refs: advance(node_total, *refs),
        in_specs=[pl.BlockSpec(memory_space=pltpu.VMEM)] * len(operands),
        out_specs=[pl.BlockSpec(memory_space=pltpu.HBM)],
        out_shape=[jax.ShapeDtypeStruct((Q, PLANES, 8, 128), jnp.float32)],
        scratch_shapes=[
            pltpu.VMEM((PLANES, Q, 8, 128), jnp.float32),
            pltpu.VMEM((PLANES, Q) + tile, jnp.float32),
            pltpu.VMEM((PLANES, Q) + tile, jnp.float32),
            pltpu.VMEM((Q,) + tile, jnp.float32),
            pltpu.VMEM((Q,) + tile, jnp.float32),
            pltpu.SemaphoreType.DMA((PLANES,)),
        ],
        compiler_params=pltpu.CompilerParams(vmem_limit_bytes=20 * 1024 * 1024),
    )(*operands)
    return advanced


def solution(mesh):
    placed = (P(None, None, "gz", "gx"), P(None, "gz", "gx"), P(None, "gz", "gx"))
    return jax.shard_map(
        local, mesh=mesh, in_specs=placed, out_specs=P(None, None, "gz", "gx"), check_vma=False
    )
```

```python
import jax
import jax.numpy as jnp
from jax import lax
from jax.experimental import pallas as pl
from jax.experimental.pallas import tpu as pltpu
from jax.sharding import PartitionSpec as P


Q = 19
PLANES = 8
LATTICE = (
    (0, 0, 0),
    (1, 0, 0),
    (-1, 0, 0),
    (0, 1, 0),
    (0, -1, 0),
    (0, 0, 1),
    (0, 0, -1),
    (1, 1, 0),
    (-1, -1, 0),
    (1, -1, 0),
    (-1, 1, 0),
    (1, 0, 1),
    (-1, 0, -1),
    (1, 0, -1),
    (-1, 0, 1),
    (0, 1, 1),
    (0, -1, -1),
    (0, 1, -1),
    (0, -1, 1),
)
OPPOSITE = (0, 2, 1, 4, 3, 6, 5, 8, 7, 10, 9, 12, 11, 14, 13, 16, 15, 18, 17)
INCOMING = (4, 8, 9, 16, 18)
SECOND, THIRD, FOURTH = 1.8, 1.2, 1.1
BASE_DRIVE = 0.0001
DRIVE_GAIN = 1.0
TARGET_FLOW = 0.1

FLAG_SLOT = Q * PLANES
INFLOW_SLOT = FLAG_SLOT + 2
SLOTS = INFLOW_SLOT + len(INCOMING)
TILES = 5
ROW_TILES = 40
PIECES = ((0, 5), (5, 10), (10, 15), (15, 19))
GROUP = 24
SUMS_LANE = 10 * GROUP


def relax(f):
    along = []
    for p in (1, 3, 5):
        along.append((f[p] + f[p + 1], f[p] - f[p + 1]))
    diagonal = []
    for p in (7, 11, 15):
        a, b = f[p] + f[p + 1], f[p + 2] + f[p + 3]
        c, d = f[p] - f[p + 1], f[p + 2] - f[p + 3]
        diagonal.append((a + b, a - b, c + d, c - d))
    (xxyy, xy, xyy, xxy), (xxzz, xz, xzz, xxz), (yyzz, yz, yzz, yyz) = diagonal
    density = f[0] + (along[0][0] + along[1][0] + along[2][0]) + (xxyy + xxzz + yyzz)
    jx = along[0][1] + xyy + xzz
    jy = along[1][1] + xxy + yzz
    jz = along[2][1] + xxz + yyz
    inv = 1.0 / density
    ux, uy, uz = jx * inv, jy * inv, jz * inv
    exx, eyy, ezz = jx * ux, jy * uy, jz * uz
    third = density * (1.0 / 3.0)
    ninth = density * (1.0 / 9.0)
    xx = along[0][0] + xxyy + xxzz
    yy = along[1][0] + xxyy + yyzz
    zz = along[2][0] + xxzz + yyzz
    dxx = SECOND * (xx - third - exx)
    dyy = SECOND * (yy - third - eyy)
    dzz = SECOND * (zz - third - ezz)
    dxy = SECOND * (xy - jx * uy)
    dxz = SECOND * (xz - jx * uz)
    dyz = SECOND * (yz - jy * uz)
    x3, y3, z3 = jx * (1.0 / 3.0), jy * (1.0 / 3.0), jz * (1.0 / 3.0)
    dxyy, dxzz = THIRD * (xyy - x3), THIRD * (xzz - x3)
    dxxy, dyzz = THIRD * (xxy - y3), THIRD * (yzz - y3)
    dxxz, dyyz = THIRD * (xxz - z3), THIRD * (yyz - z3)
    half = 0.5 * (exx + eyy + ezz)
    dxxyy = FOURTH * (xxyy - ninth - (half - 0.5 * ezz) * (2.0 / 3.0) + ezz * (1.0 / 6.0))
    dxxzz = FOURTH * (xxzz - ninth - (half - 0.5 * eyy) * (2.0 / 3.0) + eyy * (1.0 / 6.0))
    dyyzz = FOURTH * (yyzz - ninth - (half - 0.5 * exx) * (2.0 / 3.0) + exx * (1.0 / 6.0))
    out = [None] * Q
    out[0] = f[0] + (dxx + dyy + dzz) - (dxxyy + dxxzz + dyyzz)
    for p, even, odd in (
        (1, dxx - dxxyy - dxxzz, dxyy + dxzz),
        (3, dyy - dxxyy - dyyzz, dxxy + dyzz),
        (5, dzz - dxxzz - dyyzz, dxxz + dyyz),
    ):
        out[p] = f[p] - 0.5 * (even - odd)
        out[p + 1] = f[p + 1] - 0.5 * (even + odd)
    for p, four, cross, first, second in (
        (7, dxxyy, dxy, dxyy, dxxy),
        (11, dxxzz, dxz, dxzz, dxxz),
        (15, dyyzz, dyz, dyzz, dyyz),
    ):
        same, other = 0.25 * (four + cross), 0.25 * (four - cross)
        total, rest = 0.25 * (first + second), 0.25 * (first - second)
        out[p] = f[p] - (same + total)
        out[p + 1] = f[p + 1] - (same - total)
        out[p + 2] = f[p + 2] - (other + rest)
        out[p + 3] = f[p + 3] - (other - rest)
    return out, (ux, uy, uz), inv


def weight(index):
    return 1.0 / 3.0 if index == 0 else (1.0 / 18.0 if index < 7 else 1.0 / 36.0)


def push_parts(index, velocity, inv):
    cx, cy, cz = LATTICE[index]
    along = 9.0 * velocity[0] - 3.0 * velocity[0] + 3.0 * cx
    if cy:
        along = along + (9.0 * cx * cy) * velocity[1]
    if cz:
        along = along + (9.0 * cx * cz) * velocity[2]
    return weight(index) * along, (3.0 * weight(index)) * inv


def driven(relaxed, velocity, inv, drive):
    ux, uy, uz = velocity
    square = drive * drive * inv
    still = -3.0 * drive * ux - 1.5 * square
    moved = still + 9.0 * drive * ux + 4.5 * square
    three = 3.0 * drive
    up, down = moved + three, moved - three
    hy, hz = 9.0 * drive * uy, 9.0 * drive * uz
    calm = still * (1.0 / 36.0)
    out = list(relaxed)
    out[0] = out[0] + still * (1.0 / 3.0)
    out[1] = out[1] + up * (1.0 / 18.0)
    out[2] = out[2] + down * (1.0 / 18.0)
    for index in (3, 4, 5, 6):
        out[index] = out[index] + (calm + calm)
    for p, side in ((7, hy), (11, hz)):
        out[p] = out[p] + (up + side) * (1.0 / 36.0)
        out[p + 1] = out[p + 1] + (down + side) * (1.0 / 36.0)
        out[p + 2] = out[p + 2] + (up - side) * (1.0 / 36.0)
        out[p + 3] = out[p + 3] + (down - side) * (1.0 / 36.0)
    for index in (15, 16, 17, 18):
        out[index] = out[index] + calm
    return out


def rolled(value, step_z, step_x):
    if step_z:
        value = pltpu.roll(value, step_z % value.shape[0], 0)
    if step_x:
        value = pltpu.roll(value, step_x % value.shape[1], 1)
    return value


def slot_values(pops, solid, inflow):
    values = [lambda q=q, y=y: pops[q, y] for q in range(Q) for y in range(PLANES)]
    values += [lambda y=y: solid[y].astype(jnp.float32) for y in range(2)]
    values += [lambda i=i: inflow[i] for i in range(len(INCOMING))]
    return values


def is_odd(axis):
    return lax.axis_index(axis) % 2 == 1


def load(pops_hbm, solid_hbm, inflow_hbm, first, second, pops, solid, inflow, done):
    copies = [(solid_hbm, solid), (inflow_hbm, inflow)]
    copies += [(pops_hbm.at[a:b], pops.at[a:b]) for a, b in PIECES]
    copies = [pltpu.make_async_copy(source, target, done.at[i]) for i, (source, target) in enumerate(copies)]
    for copy in copies:
        copy.start()
    copies[0].wait()
    odd = is_odd("gz")
    first[...] = jnp.zeros(first.shape, jnp.float32)
    second[...] = jnp.zeros(second.shape, jnp.float32)
    for y in range(2):
        tile = solid[y].astype(jnp.float32)
        low, high = tile[0:2], tile[6:8]
        first[2 * y : 2 * y + 2] = jnp.where(odd, low, high)
        second[2 * y : 2 * y + 2] = jnp.where(odd, high, low)
    for copy in copies[1:]:
        copy.wait()


def pack(pops, solid, inflow, first, second, columns):
    odd = is_odd("gz")
    lane = lax.broadcasted_iota(jnp.int32, (8, 128), 1)
    values = slot_values(pops, solid, inflow)
    for tile in range(TILES):
        packed = jnp.zeros((8, 128), jnp.float32)
        for slot in range(tile * 32, min(tile * 32 + 32, SLOTS)):
            value = values[slot]()
            if slot not in (FLAG_SLOT, FLAG_SLOT + 1):
                low, high = value[0:2], value[6:8]
                place = (slot // 4, slice(2 * (slot % 4), 2 * (slot % 4) + 2))
                first[place] = jnp.where(odd, low, high)
                second[place] = jnp.where(odd, high, low)
            packed = jnp.where(in_slot(lane, slot), rolled(value, 0, 4 * (slot % 32)), packed)
        columns[tile] = packed


def in_slot(lane, slot):
    return ((lane + (128 - 4 * (slot % 32) + 2)) & 127) < 4


def lay_rows(target, main, odd, one, two):
    target[0:8] = main
    target[8:10] = jnp.where(odd, two, one)
    target[14:16] = jnp.where(odd, one, two)


def halo_rows(slot, first, second):
    place = (slot // 4, slice(2 * (slot % 4), 2 * (slot % 4) + 2))
    return first[place], second[place]


def tally(pops, solid, inflow, acc, low_rows, high_rows, half_one, half_two):
    lane = lax.broadcasted_iota(jnp.int32, (8, 128), 1)
    row = lax.broadcasted_iota(jnp.int32, (8, 128), 0)
    nothing = jnp.zeros((8, 128), jnp.float32)
    blocked = [solid[y].astype(jnp.float32) for y in range(2)]
    flags = [jnp.concatenate([part, nothing], axis=0) for part in blocked]
    fluid = [1.0 - part for part in blocked]
    flow = nothing
    for y in range(PLANES):
        f = pops
        jx = (
            (f[1, y] - f[2, y])
            + (f[7, y] - f[8, y])
            + (f[9, y] - f[10, y])
            + (f[11, y] - f[12, y])
            + (f[13, y] - f[14, y])
        )
        flow = flow + (jx * fluid[y] if y < 2 else jx)
    one = flow + (inflow[INCOMING.index(9)] - inflow[INCOMING.index(8)])
    count = float(PLANES - 2) + fluid[0] + fluid[1]
    two = nothing
    weights = {}
    outer = {-1: nothing, 1: nothing}
    for y in (0, 1, 2, PLANES - 1):
        relaxed, velocity, inv = relax([pops[q, y] for q in range(Q)])
        for index in range(Q):
            cx, cy, cz = LATTICE[index]
            target = y + cy
            if not cx or 1 < target < PLANES:
                continue
            linear, square = push_parts(index, velocity, inv)
            factor = -float(cx) if target >= PLANES else -2.0 * cx
            parts = [relaxed[index] * factor, linear * factor, square * factor]
            if y < 2:
                parts = [part * fluid[y] for part in parts]
            if 0 <= target < PLANES:
                for i, part in enumerate(parts):
                    key = ((0 if cx > 0 else 6) + 3 * target + i, cz)
                    weights[key] = weights[key] + part if key in weights else part
                    if cz:
                        place = 3 * target + i
                        moved = rolled(part, place - (7 if cz > 0 else 0), cx)
                        keep = (row == place) & (lane != (0 if cx > 0 else 127))
                        outer[cz] = outer[cz] + jnp.where(keep, moved, 0.0)
                hit = rolled(flags[target], -cz, -cx)[0:8]
                hit = jnp.where(lane == (127 if cx > 0 else 0), 0.0, hit)
                parts = [part * hit for part in parts]
            one, count, two = one + parts[0], count + parts[1], two + parts[2]
    low_rows[...] = outer[-1]
    high_rows[...] = outer[1]
    totals = nothing
    for i, part in enumerate((flow, one, count, two)):
        totals = jnp.where(row == i, jnp.sum(part, axis=0, keepdims=True), totals)
    acc[...] = totals

    by_row = {-1: nothing, 0: nothing, 1: nothing}
    for (place, cz), part in weights.items():
        by_row[cz] = jnp.where(lane == place, rolled(part, 0, place - (127 if place < 6 else 0)), by_row[cz])
    table = jnp.zeros((16, 128), jnp.float32)
    for cz, part in by_row.items():
        table = table + rolled(jnp.concatenate([part, nothing], axis=0), cz, 0)
    lanes = lax.broadcasted_iota(jnp.int32, (16, 128), 1)
    for y in range(2):
        for i in range(3):
            place = 12 + 3 * y + i
            table = jnp.where(lanes == place, rolled(flags[y], 0, place), table)
            table = jnp.where(lanes == place + 6, rolled(flags[y], 0, place + 6 - 127), table)
    halves = [nothing, nothing]
    for k in range(10):
        source = k if k < 9 else 15
        spread = rolled(jnp.broadcast_to(table[source : source + 1], (8, 128)), 0, (GROUP * k) % 128)
        for half in range(2):
            start = GROUP * k - 128 * half
            if -GROUP < start < 128:
                halves[half] = jnp.where((lane >= start) & (lane < start + GROUP), spread, halves[half])
    half_one[...] = halves[0]
    half_two[...] = halves[1]


def announce(first, second, acc, low_rows, high_rows, half_one, half_two, out):
    lane = lax.broadcasted_iota(jnp.int32, (8, 128), 1)
    row = lax.broadcasted_iota(jnp.int32, (8, 128), 0)
    odd = is_odd("gz")
    one, two = first[...], second[...]
    below, above = jnp.where(odd, one, two), jnp.where(odd, two, one)
    tail = half_two[...]
    edge = []
    for flags, offset, k in ((below, 1, 9), (above, 0, 8)):
        planes = [jnp.broadcast_to(flags[2 * y + offset : 2 * y + offset + 1], (8, 128)) for y in range(2)]
        edge.append(jnp.where(row < 3, planes[0], jnp.where(row < 6, planes[1], 0.0)))
        for y in range(2):
            start = GROUP * k - 128 + 12 + 3 * y
            for begin, column in ((start, 0), (start + 6, 127)):
                value = jnp.broadcast_to(planes[y][:, column : column + 1], (8, 128))
                tail = jnp.where((lane >= begin) & (lane < begin + 3), value, tail)
    more = low_rows[...] * edge[0] + high_rows[...] * edge[1]
    inside = (row >= 1) & (row < 4)
    total = acc[...] + jnp.where(inside, rolled(more, 1, 0) + rolled(more, -2, 0), 0.0)
    total = jnp.broadcast_to(jnp.sum(total, axis=1, keepdims=True), (8, 128))
    total = jnp.sum(jnp.where(lane == SUMS_LANE - 128 + row, total, 0.0), axis=0, keepdims=True)
    tail = jnp.where((lane >= SUMS_LANE - 128) & (lane < SUMS_LANE - 124), total, tail)
    packed = jnp.concatenate([half_one[0:1], tail[0:1]], axis=1)
    out[...] = jnp.broadcast_to(packed[None], out.shape)


def within_group(place):
    return place - GROUP * lax.shift_right_logical(place * 2731, 16)


def cross(messages, out):
    table = messages[...]
    count = table.shape[0]
    place = lax.broadcasted_iota(jnp.int32, table.shape, 1)
    within = within_group(place)
    following = jnp.where(within < 18, pltpu.roll(table, count - 1, 0), pltpu.roll(table, 1, 0))
    matched = jnp.where(within < 12, table * rolled(following, 0, -12), 0.0)
    packed = jnp.sum(jnp.where(place < SUMS_LANE, matched, table), axis=0, keepdims=True)
    out[...] = jnp.broadcast_to(packed[None], out.shape)


def drives(sums, node_total):
    packed = jnp.sum(sums, axis=0)
    place = lax.broadcasted_iota(jnp.int32, packed.shape, 1)
    within = within_group(place)
    totals = []
    for i in range(4):
        keep = place == SUMS_LANE + i
        for start in range(i - 1, 12 if i else 0, 3):
            keep = keep | ((place < SUMS_LANE) & (within == start))
        totals.append(jnp.sum(jnp.where(keep, packed, 0.0), axis=1, keepdims=True))
    flow, one, count, two = totals
    first = BASE_DRIVE + DRIVE_GAIN * (TARGET_FLOW - flow / node_total)
    later = (one + count * first + two * (first * first)) / node_total
    second = BASE_DRIVE + DRIVE_GAIN * (TARGET_FLOW - later)
    return jnp.broadcast_to(first, (8, 128)), jnp.broadcast_to(second, (8, 128))


HALVES = (slice(0, 8), slice(8, 16))


def lay_out(pops, solid, inflow, first, second, first_flags, second_flags, columns, after, rows, flags, entry, edges):
    odd = is_odd("gz")
    lane = lax.broadcasted_iota(jnp.int32, (8, 128), 1)
    for y in range(2):
        pair = slice(2 * y, 2 * y + 2)
        lay_rows(flags.at[y], solid[y].astype(jnp.float32), odd, first_flags[pair], second_flags[pair])
    for i in range(len(INCOMING)):
        lay_rows(entry.at[i], inflow[i], odd, *halo_rows(INFLOW_SLOT + i, first, second))
    for y in range(PLANES):
        for q in range(Q):
            lay_rows(rows.at[y, q], pops[q, y], odd, *halo_rows(q * PLANES + y, first, second))
    outer = slice(8, 16)
    values = [lambda q=q, y=y: rows[y, q, outer] for q in range(Q) for y in range(PLANES)]
    values += [lambda y=y: flags[y, outer] for y in range(2)]
    values += [lambda i=i: entry[i, outer] for i in range(len(INCOMING))]
    for tile in range(TILES):
        packed = jnp.zeros((8, 128), jnp.float32)
        for slot in range(tile * 32, min(tile * 32 + 32, SLOTS)):
            packed = jnp.where(in_slot(lane, slot), rolled(values[slot](), 0, 4 * (slot % 32)), packed)
        edges[tile, 0:8] = columns[tile]
        edges[tile, outer] = packed


def prepare(rows, after, kept, relaxed, state):
    kept[...] = rows[0:2]

    def collide(y, carry):
        for half in HALVES:
            result, velocity, inv = relax([rows[y, q, half] for q in range(Q)])
            for q in range(Q):
                relaxed[y, q, half] = result[q]
            for i, value in enumerate(velocity + (inv,)):
                state[y, i, half] = value
        return carry

    lax.fori_loop(0, PLANES, collide, 0, unroll=8)


def sideways(value, q, source):
    cx, _, cz = LATTICE[q]
    lane = lax.broadcasted_iota(jnp.int32, (16, 128), 1)
    lane_to = 0 if cx > 0 else 127
    return lane == lane_to, rolled(value, cz, lane_to - (4 * source - (1 if cx > 0 else 0)))


def inward(q, source):
    cx, cy, _ = LATTICE[q]
    lane = lax.broadcasted_iota(jnp.int32, (16, 128), 1)
    lane_to = 4 * (source + cy) - (0 if cx > 0 else 1)
    return lane == lane_to % 128, lane_to - (127 if cx > 0 else 0)


def lay_side(flags, near, far, hits, hits_side, flags_side_out, now_side, entry_side, relaxed_side, state_side):
    odd = is_odd("gx")
    lane = lax.broadcasted_iota(jnp.int32, (16, 128), 1)
    edges = []
    for tile in range(TILES):
        one, two = near[tile], far[tile]
        low, high = jnp.where(odd, one, two), jnp.where(odd, two, one)
        edges.append(jnp.where((lane & 3) < 2, high, low))
    for q in range(Q):
        now_side[q] = rolled(edges[q // 4], 0, -32 * (q % 4))
    for i in range(len(INCOMING)):
        slot = (INFLOW_SLOT + i) % 32
        entry_side[i] = rolled(edges[INFLOW_SLOT // 32], 0, 4 * (PLANES - 1) - 4 * slot)
    flags_side = jnp.where(((lane + 2) & 127) < 8, rolled(edges[4], 0, -96), 0.0)
    flags_side_out[...] = flags_side
    for q in range(Q):
        cx, cy, cz = LATTICE[q]
        for source in range(2):
            hit = rolled(flags[source], cz, cx)
            if cx:
                edge, value = sideways(flags_side, q, source)
                hit = jnp.where(edge, value, hit)
            hits[source, q] = hit
        hit = rolled(flags_side, cz, 4 * cy + cx)
        for source in range(2):
            if cx and 0 <= source + cy:
                edge, shift = inward(q, source)
                hit = jnp.where(edge, rolled(flags[source], cz, shift), hit)
        if cy > 0:
            hit = jnp.where(((lane + 2) & 127) < 4, 1.0, hit)
        hits_side[q] = hit
    for half in HALVES:
        result, velocity, inv = relax([now_side[q, half] for q in range(Q)])
        for q in range(Q):
            relaxed_side[q, half] = result[q]
        for i, value in enumerate(velocity + (inv,)):
            state_side[i, half] = value


def advance(
    node_total, kept, relaxed, state, flags, entry, hits, hits_side, flags_side, first_side, entry_side,
    relaxed_side, state_side, sums, out_hbm, out, moved, now, moved_side, now_side, done,
):
    drive, drive_later = drives(sums[...], node_total)
    lane = lax.broadcasted_iota(jnp.int32, (16, 128), 1)

    def push(y, carry):
        for half in HALVES:
            velocity = tuple(state[y, i, half] for i in range(3))
            result = driven([relaxed[y, q, half] for q in range(Q)], velocity, state[y, 3, half], drive)
            for q in range(Q):
                moved[y, q, half] = result[q]
        return carry

    def collide(y, carry):
        for half in HALVES:
            result = driven(*relax([now[y, q, half] for q in range(Q)]), drive_later)
            for q in range(Q):
                moved[y, q, half] = result[q]
        return carry

    def push_side():
        for half in HALVES:
            velocity = tuple(state_side[i, half] for i in range(3))
            result = driven([relaxed_side[q, half] for q in range(Q)], velocity, state_side[3, half], drive)
            for q in range(Q):
                moved_side[q, half] = result[q]

    def collide_side():
        for half in HALVES:
            result = driven(*relax([now_side[q, half] for q in range(Q)]), drive_later)
            for q in range(Q):
                moved_side[q, half] = result[q]

    def arrive(y, q, part):
        cx, cy, cz = LATTICE[q]
        source = y - cy
        if source < 0:
            arrived = moved[y, OPPOSITE[q], part]
        elif source >= PLANES:
            arrived = entry[INCOMING.index(q), part]
        else:
            arrived = rolled(rolled(moved[source, q], cz, 0)[part], 0, cx)
            if cx:
                lane_to = 0 if cx > 0 else 127
                value = rolled(moved_side[q], cz, 0)[part]
                value = rolled(value, 0, lane_to - (4 * source - (1 if cx > 0 else 0)))
                arrived = jnp.where(lane[part] == lane_to, value, arrived)
            if source < 2:
                arrived = jnp.where(hits[source, q, part] > 0.5, moved[y, OPPOSITE[q], part], arrived)
        if y < 2:
            before = kept if part == slice(0, 16) else now
            arrived = jnp.where(flags[y, part] > 0.5, before[y, q, part], arrived)
        return arrived

    def arrive_side(q):
        cx, cy, cz = LATTICE[q]
        arrived = rolled(moved_side[q], cz, 4 * cy + cx)
        if cx:
            for source in range(PLANES):
                if 0 <= source + cy < PLANES:
                    edge, shift = inward(q, source)
                    arrived = jnp.where(edge, rolled(moved[source, q], cz, shift), arrived)
        arrived = jnp.where(hits_side[q] > 0.5, moved_side[OPPOSITE[q]], arrived)
        if cy < 0:
            arrived = jnp.where(((lane - 26) & 127) < 4, entry_side[INCOMING.index(q)], arrived)
        return jnp.where(flags_side[...] > 0.5, first_side[q], arrived)

    lax.fori_loop(0, PLANES, push, 0, unroll=8)
    push_side()
    for y in range(PLANES):
        for q in range(Q):
            now[y, q] = arrive(y, q, slice(0, 16))
    for q in range(Q):
        now_side[q] = arrive_side(q)
    lax.fori_loop(0, PLANES, collide, 0, unroll=8)
    collide_side()
    copies = []
    for y in range(PLANES):
        for q in range(Q):
            out[y, q] = arrive(y, q, slice(0, 8))
        copies.append(pltpu.make_async_copy(out.at[y], out_hbm.at[:, y], done.at[y]))
        copies[-1].start()
    for copy in copies:
        copy.wait()


def kernel_call(body, shapes, scratch, *operands, memory=pltpu.VMEM, after=()):
    return pl.pallas_call(
        body,
        in_specs=[pl.BlockSpec(memory_space=memory)] * len(operands) + [pl.BlockSpec(memory_space=pl.ANY)] * len(after),
        out_specs=[pl.BlockSpec(memory_space=pltpu.VMEM)] * len(shapes),
        out_shape=[pltpu.VMEM(item, jnp.float32) if isinstance(item, tuple) else item for item in shapes],
        scratch_shapes=[
            pltpu.VMEM(item, jnp.float32) if isinstance(item, tuple) else item for item in scratch
        ],
        compiler_params=pltpu.CompilerParams(vmem_limit_bytes=20 * 1024 * 1024),
    )(*operands, *after)


def swapped(axis, first, second):
    count = lax.axis_size(axis)
    pairs = [(i, i ^ 1) for i in range(count)]
    others = [(i, (i + 1 if i % 2 else i - 1) % count) for i in range(count)]
    return lax.ppermute(first, axis, pairs), lax.ppermute(second, axis, others)


def local(populations, solid, top_inflow):
    along_x, along_z = lax.axis_size("gx"), lax.axis_size("gz")
    node_total = float(PLANES * 8 * 128 * along_x * along_z)
    fields = (populations, solid, top_inflow)
    *flags, pops, solid, top_inflow = kernel_call(
        load,
        [(8, 128)] * 2 + [pltpu.VMEM(field.shape, field.dtype) for field in fields],
        [pltpu.SemaphoreType.DMA((2 + len(PIECES),))],
        *(pltpu.with_memory_space_constraint(field, pltpu.HBM) for field in fields),
        memory=pltpu.HBM,
    )
    block = (pops, solid, top_inflow)
    flags = swapped("gz", *flags)
    *rows, columns = kernel_call(pack, [(ROW_TILES, 8, 128)] * 2 + [(TILES, 8, 128)], [], *block)
    own = kernel_call(tally, [(8, 128)] * 5, [], *block)
    (sums,) = kernel_call(announce, [(along_x, 1, 256)], [], *flags, *own)
    sums = lax.all_to_all(sums, "gx", 0, 0, tiled=True)
    halo = swapped("gz", *rows)
    (sums,) = kernel_call(cross, [(along_z, 1, 256)], [], sums.reshape(along_x, 256))
    laid, flags, entry, edges = kernel_call(
        lay_out,
        [(PLANES, Q, 16, 128), (2, 16, 128), (len(INCOMING), 16, 128), (TILES, 16, 128)],
        [],
        *block,
        *halo,
        *flags,
        columns,
        after=(sums,),
    )
    sums = lax.all_to_all(sums, "gz", 0, 0, tiled=True)
    near, far = swapped("gx", edges, edges)
    prepared = kernel_call(
        prepare,
        [(2, Q, 16, 128), (PLANES, Q, 16, 128), (PLANES, 4, 16, 128)],
        [],
        laid,
        after=(edges,),
    )
    tile = (16, 128)
    side = kernel_call(
        lay_side,
        [(2, Q) + tile, (Q,) + tile, tile, (Q,) + tile, (len(INCOMING),) + tile, (Q,) + tile, (4,) + tile],
        [],
        flags,
        near,
        far,
    )
    operands = (*prepared, flags, entry, *side, sums)
    (advanced,) = pl.pallas_call(
        lambda *refs: advance(node_total, *refs),
        in_specs=[pl.BlockSpec(memory_space=pltpu.VMEM)] * len(operands),
        out_specs=[pl.BlockSpec(memory_space=pltpu.HBM)],
        out_shape=[jax.ShapeDtypeStruct((Q, PLANES, 8, 128), jnp.float32)],
        scratch_shapes=[
            pltpu.VMEM((PLANES, Q, 8, 128), jnp.float32),
            pltpu.VMEM((PLANES, Q) + tile, jnp.float32),
            pltpu.VMEM((PLANES, Q) + tile, jnp.float32),
            pltpu.VMEM((Q,) + tile, jnp.float32),
            pltpu.VMEM((Q,) + tile, jnp.float32),
            pltpu.SemaphoreType.DMA((PLANES,)),
        ],
        compiler_params=pltpu.CompilerParams(vmem_limit_bytes=20 * 1024 * 1024),
    )(*operands)
    return advanced


def solution(mesh):
    placed = (P(None, None, "gz", "gx"), P(None, "gz", "gx"), P(None, "gz", "gx"))
    return jax.shard_map(
        local, mesh=mesh, in_specs=placed, out_specs=P(None, None, "gz", "gx"), check_vma=False
    )
```

```python
import jax
import jax.numpy as jnp
from jax import lax
from jax.experimental import pallas as pl
from jax.experimental.pallas import tpu as pltpu
from jax.sharding import PartitionSpec as P


Q = 19
PLANES = 8
LATTICE = (
    (0, 0, 0),
    (1, 0, 0),
    (-1, 0, 0),
    (0, 1, 0),
    (0, -1, 0),
    (0, 0, 1),
    (0, 0, -1),
    (1, 1, 0),
    (-1, -1, 0),
    (1, -1, 0),
    (-1, 1, 0),
    (1, 0, 1),
    (-1, 0, -1),
    (1, 0, -1),
    (-1, 0, 1),
    (0, 1, 1),
    (0, -1, -1),
    (0, 1, -1),
    (0, -1, 1),
)
OPPOSITE = (0, 2, 1, 4, 3, 6, 5, 8, 7, 10, 9, 12, 11, 14, 13, 16, 15, 18, 17)
INCOMING = (4, 8, 9, 16, 18)
SECOND, THIRD, FOURTH = 1.8, 1.2, 1.1
BASE_DRIVE = 0.0001
DRIVE_GAIN = 1.0
TARGET_FLOW = 0.1

FLAG_SLOT = Q * PLANES
INFLOW_SLOT = FLAG_SLOT + 2
SLOTS = INFLOW_SLOT + len(INCOMING)
TILES = 5
ROW_TILES = 40
PIECES = ((0, 5), (5, 10), (10, 15), (15, 19))
GROUP = 24
SUMS_LANE = 10 * GROUP


def relax(f):
    along = []
    for p in (1, 3, 5):
        along.append((f[p] + f[p + 1], f[p] - f[p + 1]))
    diagonal = []
    for p in (7, 11, 15):
        a, b = f[p] + f[p + 1], f[p + 2] + f[p + 3]
        c, d = f[p] - f[p + 1], f[p + 2] - f[p + 3]
        diagonal.append((a + b, a - b, c + d, c - d))
    (xxyy, xy, xyy, xxy), (xxzz, xz, xzz, xxz), (yyzz, yz, yzz, yyz) = diagonal
    density = f[0] + (along[0][0] + along[1][0] + along[2][0]) + (xxyy + xxzz + yyzz)
    jx = along[0][1] + xyy + xzz
    jy = along[1][1] + xxy + yzz
    jz = along[2][1] + xxz + yyz
    inv = 1.0 / density
    ux, uy, uz = jx * inv, jy * inv, jz * inv
    exx, eyy, ezz = jx * ux, jy * uy, jz * uz
    third = density * (1.0 / 3.0)
    ninth = density * (1.0 / 9.0)
    xx = along[0][0] + xxyy + xxzz
    yy = along[1][0] + xxyy + yyzz
    zz = along[2][0] + xxzz + yyzz
    dxx = SECOND * (xx - third - exx)
    dyy = SECOND * (yy - third - eyy)
    dzz = SECOND * (zz - third - ezz)
    dxy = SECOND * (xy - jx * uy)
    dxz = SECOND * (xz - jx * uz)
    dyz = SECOND * (yz - jy * uz)
    x3, y3, z3 = jx * (1.0 / 3.0), jy * (1.0 / 3.0), jz * (1.0 / 3.0)
    dxyy, dxzz = THIRD * (xyy - x3), THIRD * (xzz - x3)
    dxxy, dyzz = THIRD * (xxy - y3), THIRD * (yzz - y3)
    dxxz, dyyz = THIRD * (xxz - z3), THIRD * (yyz - z3)
    half = 0.5 * (exx + eyy + ezz)
    dxxyy = FOURTH * (xxyy - ninth - (half - 0.5 * ezz) * (2.0 / 3.0) + ezz * (1.0 / 6.0))
    dxxzz = FOURTH * (xxzz - ninth - (half - 0.5 * eyy) * (2.0 / 3.0) + eyy * (1.0 / 6.0))
    dyyzz = FOURTH * (yyzz - ninth - (half - 0.5 * exx) * (2.0 / 3.0) + exx * (1.0 / 6.0))
    out = [None] * Q
    out[0] = f[0] + (dxx + dyy + dzz) - (dxxyy + dxxzz + dyyzz)
    for p, even, odd in (
        (1, dxx - dxxyy - dxxzz, dxyy + dxzz),
        (3, dyy - dxxyy - dyyzz, dxxy + dyzz),
        (5, dzz - dxxzz - dyyzz, dxxz + dyyz),
    ):
        out[p] = f[p] - 0.5 * (even - odd)
        out[p + 1] = f[p + 1] - 0.5 * (even + odd)
    for p, four, cross, first, second in (
        (7, dxxyy, dxy, dxyy, dxxy),
        (11, dxxzz, dxz, dxzz, dxxz),
        (15, dyyzz, dyz, dyzz, dyyz),
    ):
        same, other = 0.25 * (four + cross), 0.25 * (four - cross)
        total, rest = 0.25 * (first + second), 0.25 * (first - second)
        out[p] = f[p] - (same + total)
        out[p + 1] = f[p + 1] - (same - total)
        out[p + 2] = f[p + 2] - (other + rest)
        out[p + 3] = f[p + 3] - (other - rest)
    return out, (ux, uy, uz), inv


def weight(index):
    return 1.0 / 3.0 if index == 0 else (1.0 / 18.0 if index < 7 else 1.0 / 36.0)


def push_parts(index, velocity, inv):
    cx, cy, cz = LATTICE[index]
    along = 9.0 * velocity[0] - 3.0 * velocity[0] + 3.0 * cx
    if cy:
        along = along + (9.0 * cx * cy) * velocity[1]
    if cz:
        along = along + (9.0 * cx * cz) * velocity[2]
    return weight(index) * along, (3.0 * weight(index)) * inv


def driven(relaxed, velocity, inv, drive):
    ux, uy, uz = velocity
    square = drive * drive * inv
    still = -3.0 * drive * ux - 1.5 * square
    moved = still + 9.0 * drive * ux + 4.5 * square
    three = 3.0 * drive
    up, down = moved + three, moved - three
    hy, hz = 9.0 * drive * uy, 9.0 * drive * uz
    calm = still * (1.0 / 36.0)
    out = list(relaxed)
    out[0] = out[0] + still * (1.0 / 3.0)
    out[1] = out[1] + up * (1.0 / 18.0)
    out[2] = out[2] + down * (1.0 / 18.0)
    for index in (3, 4, 5, 6):
        out[index] = out[index] + (calm + calm)
    for p, side in ((7, hy), (11, hz)):
        out[p] = out[p] + (up + side) * (1.0 / 36.0)
        out[p + 1] = out[p + 1] + (down + side) * (1.0 / 36.0)
        out[p + 2] = out[p + 2] + (up - side) * (1.0 / 36.0)
        out[p + 3] = out[p + 3] + (down - side) * (1.0 / 36.0)
    for index in (15, 16, 17, 18):
        out[index] = out[index] + calm
    return out


def rolled(value, step_z, step_x):
    if step_z:
        value = pltpu.roll(value, step_z % value.shape[0], 0)
    if step_x:
        value = pltpu.roll(value, step_x % value.shape[1], 1)
    return value


def slot_values(pops, solid, inflow):
    values = [lambda q=q, y=y: pops[q, y] for q in range(Q) for y in range(PLANES)]
    values += [lambda y=y: solid[y].astype(jnp.float32) for y in range(2)]
    values += [lambda i=i: inflow[i] for i in range(len(INCOMING))]
    return values


def is_odd(axis):
    return lax.axis_index(axis) % 2 == 1


def load(pops_hbm, solid_hbm, inflow_hbm, first, second, pops, solid, inflow, done):
    copies = [(solid_hbm, solid), (inflow_hbm, inflow)]
    copies += [(pops_hbm.at[a:b], pops.at[a:b]) for a, b in PIECES]
    copies = [pltpu.make_async_copy(source, target, done.at[i]) for i, (source, target) in enumerate(copies)]
    for copy in copies:
        copy.start()
    copies[0].wait()
    odd = is_odd("gz")
    first[...] = jnp.zeros(first.shape, jnp.float32)
    second[...] = jnp.zeros(second.shape, jnp.float32)
    for y in range(2):
        tile = solid[y].astype(jnp.float32)
        low, high = tile[0:2], tile[6:8]
        first[2 * y : 2 * y + 2] = jnp.where(odd, low, high)
        second[2 * y : 2 * y + 2] = jnp.where(odd, high, low)
    for copy in copies[1:]:
        copy.wait()


def pack(pops, solid, inflow, first, second, columns):
    odd = is_odd("gz")
    lane = lax.broadcasted_iota(jnp.int32, (8, 128), 1)
    values = slot_values(pops, solid, inflow)
    for tile in range(TILES):
        packed = jnp.zeros((8, 128), jnp.float32)
        for slot in range(tile * 32, min(tile * 32 + 32, SLOTS)):
            value = values[slot]()
            if slot not in (FLAG_SLOT, FLAG_SLOT + 1):
                low, high = value[0:2], value[6:8]
                place = (slot // 4, slice(2 * (slot % 4), 2 * (slot % 4) + 2))
                first[place] = jnp.where(odd, low, high)
                second[place] = jnp.where(odd, high, low)
            packed = jnp.where(in_slot(lane, slot), rolled(value, 0, 4 * (slot % 32)), packed)
        columns[tile] = packed


def in_slot(lane, slot):
    return ((lane + (128 - 4 * (slot % 32) + 2)) & 127) < 4


def lay_rows(target, main, odd, one, two):
    target[0:8] = main
    target[8:10] = jnp.where(odd, two, one)
    target[14:16] = jnp.where(odd, one, two)


def halo_rows(slot, first, second):
    place = (slot // 4, slice(2 * (slot % 4), 2 * (slot % 4) + 2))
    return first[place], second[place]


def tally(pops, solid, inflow, acc, low_rows, high_rows, half_one, half_two):
    lane = lax.broadcasted_iota(jnp.int32, (8, 128), 1)
    row = lax.broadcasted_iota(jnp.int32, (8, 128), 0)
    nothing = jnp.zeros((8, 128), jnp.float32)
    blocked = [solid[y].astype(jnp.float32) for y in range(2)]
    flags = [jnp.concatenate([part, nothing], axis=0) for part in blocked]
    fluid = [1.0 - part for part in blocked]
    flow = nothing
    for y in range(PLANES):
        f = pops
        jx = (
            (f[1, y] - f[2, y])
            + (f[7, y] - f[8, y])
            + (f[9, y] - f[10, y])
            + (f[11, y] - f[12, y])
            + (f[13, y] - f[14, y])
        )
        flow = flow + (jx * fluid[y] if y < 2 else jx)
    one = flow + (inflow[INCOMING.index(9)] - inflow[INCOMING.index(8)])
    count = float(PLANES - 2) + fluid[0] + fluid[1]
    two = nothing
    weights = {}
    outer = {-1: nothing, 1: nothing}
    for y in (0, 1, 2, PLANES - 1):
        relaxed, velocity, inv = relax([pops[q, y] for q in range(Q)])
        for index in range(Q):
            cx, cy, cz = LATTICE[index]
            target = y + cy
            if not cx or 1 < target < PLANES:
                continue
            linear, square = push_parts(index, velocity, inv)
            factor = -float(cx) if target >= PLANES else -2.0 * cx
            parts = [relaxed[index] * factor, linear * factor, square * factor]
            if y < 2:
                parts = [part * fluid[y] for part in parts]
            if 0 <= target < PLANES:
                for i, part in enumerate(parts):
                    key = ((0 if cx > 0 else 6) + 3 * target + i, cz)
                    weights[key] = weights[key] + part if key in weights else part
                    if cz:
                        place = 3 * target + i
                        moved = rolled(part, place - (7 if cz > 0 else 0), cx)
                        keep = (row == place) & (lane != (0 if cx > 0 else 127))
                        outer[cz] = outer[cz] + jnp.where(keep, moved, 0.0)
                hit = rolled(flags[target], -cz, -cx)[0:8]
                hit = jnp.where(lane == (127 if cx > 0 else 0), 0.0, hit)
                parts = [part * hit for part in parts]
            one, count, two = one + parts[0], count + parts[1], two + parts[2]
    low_rows[...] = outer[-1]
    high_rows[...] = outer[1]
    totals = nothing
    for i, part in enumerate((flow, one, count, two)):
        totals = jnp.where(row == i, jnp.sum(part, axis=0, keepdims=True), totals)
    acc[...] = totals

    by_row = {-1: nothing, 0: nothing, 1: nothing}
    for (place, cz), part in weights.items():
        by_row[cz] = jnp.where(lane == place, rolled(part, 0, place - (127 if place < 6 else 0)), by_row[cz])
    table = jnp.zeros((16, 128), jnp.float32)
    for cz, part in by_row.items():
        table = table + rolled(jnp.concatenate([part, nothing], axis=0), cz, 0)
    lanes = lax.broadcasted_iota(jnp.int32, (16, 128), 1)
    for y in range(2):
        for i in range(3):
            place = 12 + 3 * y + i
            table = jnp.where(lanes == place, rolled(flags[y], 0, place), table)
            table = jnp.where(lanes == place + 6, rolled(flags[y], 0, place + 6 - 127), table)
    halves = [nothing, nothing]
    for k in range(10):
        source = k if k < 9 else 15
        spread = rolled(jnp.broadcast_to(table[source : source + 1], (8, 128)), 0, (GROUP * k) % 128)
        for half in range(2):
            start = GROUP * k - 128 * half
            if -GROUP < start < 128:
                halves[half] = jnp.where((lane >= start) & (lane < start + GROUP), spread, halves[half])
    half_one[...] = halves[0]
    half_two[...] = halves[1]


def announce(first, second, acc, low_rows, high_rows, half_one, half_two, out):
    lane = lax.broadcasted_iota(jnp.int32, (8, 128), 1)
    row = lax.broadcasted_iota(jnp.int32, (8, 128), 0)
    odd = is_odd("gz")
    one, two = first[...], second[...]
    below, above = jnp.where(odd, one, two), jnp.where(odd, two, one)
    tail = half_two[...]
    edge = []
    for flags, offset, k in ((below, 1, 9), (above, 0, 8)):
        planes = [jnp.broadcast_to(flags[2 * y + offset : 2 * y + offset + 1], (8, 128)) for y in range(2)]
        edge.append(jnp.where(row < 3, planes[0], jnp.where(row < 6, planes[1], 0.0)))
        for y in range(2):
            start = GROUP * k - 128 + 12 + 3 * y
            for begin, column in ((start, 0), (start + 6, 127)):
                value = jnp.broadcast_to(planes[y][:, column : column + 1], (8, 128))
                tail = jnp.where((lane >= begin) & (lane < begin + 3), value, tail)
    more = low_rows[...] * edge[0] + high_rows[...] * edge[1]
    inside = (row >= 1) & (row < 4)
    total = acc[...] + jnp.where(inside, rolled(more, 1, 0) + rolled(more, -2, 0), 0.0)
    total = jnp.broadcast_to(jnp.sum(total, axis=1, keepdims=True), (8, 128))
    total = jnp.sum(jnp.where(lane == SUMS_LANE - 128 + row, total, 0.0), axis=0, keepdims=True)
    tail = jnp.where((lane >= SUMS_LANE - 128) & (lane < SUMS_LANE - 124), total, tail)
    packed = jnp.concatenate([half_one[0:1], tail[0:1]], axis=1)
    out[...] = jnp.broadcast_to(packed[None], out.shape)


def within_group(place):
    return place - GROUP * lax.shift_right_logical(place * 2731, 16)


def cross(messages, out):
    table = messages[...]
    count = table.shape[0]
    place = lax.broadcasted_iota(jnp.int32, table.shape, 1)
    within = within_group(place)
    following = jnp.where(within < 18, pltpu.roll(table, count - 1, 0), pltpu.roll(table, 1, 0))
    matched = jnp.where(within < 12, table * rolled(following, 0, -12), 0.0)
    packed = jnp.sum(jnp.where(place < SUMS_LANE, matched, table), axis=0, keepdims=True)
    out[...] = jnp.broadcast_to(packed[None], out.shape)


def drives(sums, node_total):
    packed = jnp.sum(sums, axis=0)
    place = lax.broadcasted_iota(jnp.int32, packed.shape, 1)
    within = within_group(place)
    totals = []
    for i in range(4):
        keep = place == SUMS_LANE + i
        for start in range(i - 1, 12 if i else 0, 3):
            keep = keep | ((place < SUMS_LANE) & (within == start))
        totals.append(jnp.sum(jnp.where(keep, packed, 0.0), axis=1, keepdims=True))
    flow, one, count, two = totals
    first = BASE_DRIVE + DRIVE_GAIN * (TARGET_FLOW - flow / node_total)
    later = (one + count * first + two * (first * first)) / node_total
    second = BASE_DRIVE + DRIVE_GAIN * (TARGET_FLOW - later)
    return jnp.broadcast_to(first, (8, 128)), jnp.broadcast_to(second, (8, 128))


HALVES = (slice(0, 8), slice(8, 16))


def lay_out(pops, solid, inflow, first, second, first_flags, second_flags, columns, after, rows, flags, entry, edges):
    odd = is_odd("gz")
    lane = lax.broadcasted_iota(jnp.int32, (8, 128), 1)
    for y in range(2):
        pair = slice(2 * y, 2 * y + 2)
        lay_rows(flags.at[y], solid[y].astype(jnp.float32), odd, first_flags[pair], second_flags[pair])
    for i in range(len(INCOMING)):
        lay_rows(entry.at[i], inflow[i], odd, *halo_rows(INFLOW_SLOT + i, first, second))
    for y in range(PLANES):
        for q in range(Q):
            lay_rows(rows.at[y, q], pops[q, y], odd, *halo_rows(q * PLANES + y, first, second))
    outer = slice(8, 16)
    values = [lambda q=q, y=y: rows[y, q, outer] for q in range(Q) for y in range(PLANES)]
    values += [lambda y=y: flags[y, outer] for y in range(2)]
    values += [lambda i=i: entry[i, outer] for i in range(len(INCOMING))]
    for tile in range(TILES):
        packed = jnp.zeros((8, 128), jnp.float32)
        for slot in range(tile * 32, min(tile * 32 + 32, SLOTS)):
            packed = jnp.where(in_slot(lane, slot), rolled(values[slot](), 0, 4 * (slot % 32)), packed)
        edges[tile, 0:8] = columns[tile]
        edges[tile, outer] = packed


def prepare(rows, after, kept, relaxed, state):
    kept[...] = rows[0:2]

    def collide(y, carry):
        for half in HALVES:
            result, velocity, inv = relax([rows[y, q, half] for q in range(Q)])
            for q in range(Q):
                relaxed[y, q, half] = result[q]
            for i, value in enumerate(velocity + (inv,)):
                state[y, i, half] = value
        return carry

    lax.fori_loop(0, PLANES, collide, 0, unroll=8)


def sideways(value, q, source):
    cx, _, cz = LATTICE[q]
    lane = lax.broadcasted_iota(jnp.int32, (16, 128), 1)
    lane_to = 0 if cx > 0 else 127
    return lane == lane_to, rolled(value, cz, lane_to - (4 * source - (1 if cx > 0 else 0)))


def inward(q, source):
    cx, cy, _ = LATTICE[q]
    lane = lax.broadcasted_iota(jnp.int32, (16, 128), 1)
    lane_to = 4 * (source + cy) - (0 if cx > 0 else 1)
    return lane == lane_to % 128, lane_to - (127 if cx > 0 else 0)


def lay_side(flags, near, far, hits, hits_side, flags_side_out, now_side, entry_side, relaxed_side, state_side):
    odd = is_odd("gx")
    lane = lax.broadcasted_iota(jnp.int32, (16, 128), 1)
    edges = []
    for tile in range(TILES):
        one, two = near[tile], far[tile]
        low, high = jnp.where(odd, one, two), jnp.where(odd, two, one)
        edges.append(jnp.where((lane & 3) < 2, high, low))
    for q in range(Q):
        now_side[q] = rolled(edges[q // 4], 0, -32 * (q % 4))
    for i in range(len(INCOMING)):
        slot = (INFLOW_SLOT + i) % 32
        entry_side[i] = rolled(edges[INFLOW_SLOT // 32], 0, 4 * (PLANES - 1) - 4 * slot)
    flags_side = jnp.where(((lane + 2) & 127) < 8, rolled(edges[4], 0, -96), 0.0)
    flags_side_out[...] = flags_side
    for q in range(Q):
        cx, cy, cz = LATTICE[q]
        for source in range(2):
            hit = rolled(flags[source], cz, cx)
            if cx:
                edge, value = sideways(flags_side, q, source)
                hit = jnp.where(edge, value, hit)
            hits[source, q] = hit
        hit = rolled(flags_side, cz, 4 * cy + cx)
        for source in range(2):
            if cx and 0 <= source + cy:
                edge, shift = inward(q, source)
                hit = jnp.where(edge, rolled(flags[source], cz, shift), hit)
        if cy > 0:
            hit = jnp.where(((lane + 2) & 127) < 4, 1.0, hit)
        hits_side[q] = hit
    for half in HALVES:
        result, velocity, inv = relax([now_side[q, half] for q in range(Q)])
        for q in range(Q):
            relaxed_side[q, half] = result[q]
        for i, value in enumerate(velocity + (inv,)):
            state_side[i, half] = value


def advance(
    node_total, kept, relaxed, state, flags, entry, hits, hits_side, flags_side, first_side, entry_side,
    relaxed_side, state_side, sums, out_hbm, out, moved, now, moved_side, now_side, done,
):
    drive, drive_later = drives(sums[...], node_total)
    lane = lax.broadcasted_iota(jnp.int32, (16, 128), 1)

    def push(y, carry):
        for half in HALVES:
            velocity = tuple(state[y, i, half] for i in range(3))
            result = driven([relaxed[y, q, half] for q in range(Q)], velocity, state[y, 3, half], drive)
            for q in range(Q):
                moved[y, q, half] = result[q]
        return carry

    def collide(y, carry):
        for half in HALVES:
            result = driven(*relax([now[y, q, half] for q in range(Q)]), drive_later)
            for q in range(Q):
                moved[y, q, half] = result[q]
        return carry

    def push_side():
        for half in HALVES:
            velocity = tuple(state_side[i, half] for i in range(3))
            result = driven([relaxed_side[q, half] for q in range(Q)], velocity, state_side[3, half], drive)
            for q in range(Q):
                moved_side[q, half] = result[q]

    def collide_side():
        for half in HALVES:
            result = driven(*relax([now_side[q, half] for q in range(Q)]), drive_later)
            for q in range(Q):
                moved_side[q, half] = result[q]

    def arrive(y, q, part):
        cx, cy, cz = LATTICE[q]
        source = y - cy
        if source < 0:
            arrived = moved[y, OPPOSITE[q], part]
        elif source >= PLANES:
            arrived = entry[INCOMING.index(q), part]
        else:
            arrived = rolled(rolled(moved[source, q], cz, 0)[part], 0, cx)
            if cx:
                lane_to = 0 if cx > 0 else 127
                value = rolled(moved_side[q], cz, 0)[part]
                value = rolled(value, 0, lane_to - (4 * source - (1 if cx > 0 else 0)))
                arrived = jnp.where(lane[part] == lane_to, value, arrived)
            if source < 2:
                arrived = jnp.where(hits[source, q, part] > 0.5, moved[y, OPPOSITE[q], part], arrived)
        if y < 2:
            before = kept if part == slice(0, 16) else now
            arrived = jnp.where(flags[y, part] > 0.5, before[y, q, part], arrived)
        return arrived

    def arrive_side(q):
        cx, cy, cz = LATTICE[q]
        arrived = rolled(moved_side[q], cz, 4 * cy + cx)
        if cx:
            for source in range(PLANES):
                if 0 <= source + cy < PLANES:
                    edge, shift = inward(q, source)
                    arrived = jnp.where(edge, rolled(moved[source, q], cz, shift), arrived)
        arrived = jnp.where(hits_side[q] > 0.5, moved_side[OPPOSITE[q]], arrived)
        if cy < 0:
            arrived = jnp.where(((lane - 26) & 127) < 4, entry_side[INCOMING.index(q)], arrived)
        return jnp.where(flags_side[...] > 0.5, first_side[q], arrived)

    lax.fori_loop(0, PLANES, push, 0, unroll=8)
    push_side()
    for y in range(PLANES):
        for q in range(Q):
            now[y, q] = arrive(y, q, slice(0, 16))
    for q in range(Q):
        now_side[q] = arrive_side(q)
    lax.fori_loop(0, PLANES, collide, 0, unroll=8)
    collide_side()
    copies = []
    for y in range(PLANES):
        for q in range(Q):
            out[y, q] = arrive(y, q, slice(0, 8))
        copies.append(pltpu.make_async_copy(out.at[y], out_hbm.at[:, y], done.at[y]))
        copies[-1].start()
    for copy in copies:
        copy.wait()


def kernel_call(body, shapes, scratch, *operands, memory=pltpu.VMEM, after=()):
    return pl.pallas_call(
        body,
        in_specs=[pl.BlockSpec(memory_space=memory)] * len(operands) + [pl.BlockSpec(memory_space=pl.ANY)] * len(after),
        out_specs=[pl.BlockSpec(memory_space=pltpu.VMEM)] * len(shapes),
        out_shape=[pltpu.VMEM(item, jnp.float32) if isinstance(item, tuple) else item for item in shapes],
        scratch_shapes=[
            pltpu.VMEM(item, jnp.float32) if isinstance(item, tuple) else item for item in scratch
        ],
        compiler_params=pltpu.CompilerParams(vmem_limit_bytes=20 * 1024 * 1024),
    )(*operands, *after)


def pairings(axis):
    count = lax.axis_size(axis)
    pairs = [(i, i ^ 1) for i in range(count)]
    return pairs, [(i, (i + 1 if i % 2 else i - 1) % count) for i in range(count)]


def swapped(axis, first, second):
    pairs, others = pairings(axis)
    return lax.ppermute(first, axis, pairs), lax.ppermute(second, axis, others)


def local(populations, solid, top_inflow):
    along_x, along_z = lax.axis_size("gx"), lax.axis_size("gz")
    node_total = float(PLANES * 8 * 128 * along_x * along_z)
    fields = (populations, solid, top_inflow)
    *flags, pops, solid, top_inflow = kernel_call(
        load,
        [(8, 128)] * 2 + [pltpu.VMEM(field.shape, field.dtype) for field in fields],
        [pltpu.SemaphoreType.DMA((2 + len(PIECES),))],
        *(pltpu.with_memory_space_constraint(field, pltpu.HBM) for field in fields),
        memory=pltpu.HBM,
    )
    block = (pops, solid, top_inflow)
    flags = swapped("gz", *flags)
    *rows, columns = kernel_call(pack, [(ROW_TILES, 8, 128)] * 2 + [(TILES, 8, 128)], [], *block)
    own = kernel_call(tally, [(8, 128)] * 5, [], *block)
    (sums,) = kernel_call(announce, [(along_x, 1, 256)], [], *flags, *own)
    sums = lax.all_to_all(sums, "gx", 0, 0, tiled=True)
    pairs, others = pairings("gz")
    near_rows = lax.ppermute(rows[0], "gz", pairs)
    halo = near_rows, lax.ppermute(rows[1], "gz", others)
    (sums,) = kernel_call(cross, [(along_z, 1, 256)], [], sums.reshape(along_x, 256))
    laid, flags, entry, edges = kernel_call(
        lay_out,
        [(PLANES, Q, 16, 128), (2, 16, 128), (len(INCOMING), 16, 128), (TILES, 16, 128)],
        [],
        *block,
        *halo,
        *flags,
        columns,
        after=(sums,),
    )
    sums = lax.all_to_all(sums, "gz", 0, 0, tiled=True)
    near, far = swapped("gx", edges, edges)
    prepared = kernel_call(
        prepare,
        [(2, Q, 16, 128), (PLANES, Q, 16, 128), (PLANES, 4, 16, 128)],
        [],
        laid,
        after=(edges,),
    )
    tile = (16, 128)
    side = kernel_call(
        lay_side,
        [(2, Q) + tile, (Q,) + tile, tile, (Q,) + tile, (len(INCOMING),) + tile, (Q,) + tile, (4,) + tile],
        [],
        flags,
        near,
        far,
    )
    operands = (*prepared, flags, entry, *side, sums)
    (advanced,) = pl.pallas_call(
        lambda *refs: advance(node_total, *refs),
        in_specs=[pl.BlockSpec(memory_space=pltpu.VMEM)] * len(operands),
        out_specs=[pl.BlockSpec(memory_space=pltpu.HBM)],
        out_shape=[jax.ShapeDtypeStruct((Q, PLANES, 8, 128), jnp.float32)],
        scratch_shapes=[
            pltpu.VMEM((PLANES, Q, 8, 128), jnp.float32),
            pltpu.VMEM((PLANES, Q) + tile, jnp.float32),
            pltpu.VMEM((PLANES, Q) + tile, jnp.float32),
            pltpu.VMEM((Q,) + tile, jnp.float32),
            pltpu.VMEM((Q,) + tile, jnp.float32),
            pltpu.SemaphoreType.DMA((PLANES,)),
        ],
        compiler_params=pltpu.CompilerParams(vmem_limit_bytes=20 * 1024 * 1024),
    )(*operands)
    return advanced


def solution(mesh):
    placed = (P(None, None, "gz", "gx"), P(None, "gz", "gx"), P(None, "gz", "gx"))
    return jax.shard_map(
        local, mesh=mesh, in_specs=placed, out_specs=P(None, None, "gz", "gx"), check_vma=False
    )
```
